32 devices in a mesh: phi: 16 (over z, x, core), eta: 2 (over y).
Axes of the slice: x: 2, y: 2, z: 4, core: 2. Of those that a mesh axis runs over, the one named last changes fastest.
Arguments:
- features: bfloat16 [32, 256, 256], P(None, 'phi', 'eta'), may hold values from -6 to 6
- cotangent: bfloat16 [32, 256, 256], P(None, 'phi', 'eta'), may hold values from -6 to 6
- kernel_a: bfloat16 [27, 32, 32], replicated, may hold values from -0.21875 to 0.21875
- kernel_b: bfloat16 [27, 64, 32], replicated, may hold values from -0.21875 to 0.21875
- mixing: bfloat16 [32, 64], replicated, may hold values from -0.75 to 0.75
Outputs:
- output: bfloat16 [32, 256, 256], P(None, 'phi', 'eta')
- grad_input: bfloat16 [32, 256, 256], P(None, 'phi', 'eta')
- grad_kernel_a: float32 [27, 32, 32], replicated
- grad_kernel_b: float32 [27, 64, 32], replicated
- grad_mixing: float32 [32, 64], replicated
The draws below stay inside these ranges and needn't reach their ends.
All inputs are finite; a program needn't handle non-finite values.
Results may differ from the reference program's by a relative error of at most 0.012.
Values may be sent and summed in bfloat16 or wider, within the bound.
No kernel may reach another device: no remote copies, remote signals or barrier semaphores. Data moves between devices by JAX's collectives and lax.ppermute only.
A program may use at most 128 MiB of HBM per device.

```python
import jax
import jax.numpy as jnp
from jax import lax

C1 = 32
C2 = 64
LAYERS = 32
PHI = 256
ETA = 8


def block_levels(stream_key, dims, cuts, smallest, top_value):
    def one(position, shards_of):
        steps = jax.random.uniform(jax.random.fold_in(jax.random.fold_in(stream_key, 6), position), (shards_of,), jnp.float32, smallest / len(cuts), top_value / len(cuts))
        return jnp.repeat(jnp.exp(steps), dims[position] // shards_of).reshape((-1,) + (1,) * (len(dims) - position - 1))

    factor_of = one(*cuts[0])
    for cut in cuts[1:]:
        factor_of = factor_of * one(*cut)
    return factor_of


def noise(stream_key, shape, scale, bound, split=(), dtype=jnp.bfloat16):
    result = scale * jax.random.normal(stream_key, shape, jnp.float32)
    if split:
        result = result * block_levels(stream_key, shape, split, -0.22, 0.18)
    return jnp.clip(result, -bound, bound).astype(dtype)


def setup_inputs(seed: int = 0) -> dict:
    arg_keys = jax.random.split(jax.random.key(seed), 6)
    features = noise(arg_keys[0], (C1, PHI, ETA * LAYERS), 1.0, 6.0, ((1, 16), (2, 2)))
    cotangent = noise(arg_keys[1], (C1, PHI, ETA * LAYERS), 1.0, 6.0, ((1, 16), (2, 2)))
    kernel_a = noise(arg_keys[2], (27, C1, C1), (27 * C1) ** -0.5, 0.21875)
    kernel_b = noise(arg_keys[3], (27, C2, C1), (27 * C1) ** -0.5, 0.21875)
    mixing = noise(arg_keys[4], (C1, C2), C2 ** -0.5, 0.75)
    return {"features": features, "cotangent": cotangent, "kernel_a": kernel_a, "kernel_b": kernel_b, "mixing": mixing}


def wrap_pad(values):
    looped = jnp.concatenate([values[:, -1:], values, values[:, :1]], axis=1)
    return jnp.pad(looped, ((0, 0), (0, 0), (1, 1), (1, 1)))

def shifted(padded, offset, extent):
    step_phi = offset // 9
    step_eta = offset // 3 % 3
    step_layer = offset % 3
    window = padded[:, step_phi:step_phi + extent[0], step_eta:step_eta + extent[1], step_layer:step_layer + extent[2]]
    return window.reshape(padded.shape[0], -1)

def convolve(padded, weight):
    extent = (padded.shape[1] - 2, padded.shape[2] - 2, padded.shape[3] - 2)
    summed = jnp.zeros((weight.shape[1], extent[0] * extent[1] * extent[2]), jnp.float32)
    for offset in range(27):
        summed = summed + jnp.dot(weight[offset], shifted(padded, offset, extent), preferred_element_type=jnp.float32)
    return summed.reshape((weight.shape[1],) + extent)

def kernel_grad(padded, upstream):
    extent = upstream.shape[1:]
    flat_up = upstream.reshape(upstream.shape[0], -1)
    kernel_terms = [lax.dot_general(flat_up, shifted(padded, offset, extent), (((1,), (1,)), ((), ())), preferred_element_type=jnp.float32) for offset in range(27)]
    return jnp.stack(kernel_terms)

def flipped(weight):
    return jnp.transpose(weight[::-1], (0, 2, 1))

def block_view(fine_grid):
    chans, rows_phi, rows_eta, layer_count = fine_grid.shape
    return fine_grid.astype(jnp.float32).reshape(chans, rows_phi // 2, 2, rows_eta // 2, 2, layer_count)

def widened(coarse):
    return jnp.repeat(jnp.repeat(coarse, 2, axis=1), 2, axis=2)

def silu_slope(linear):
    logistic = jax.nn.sigmoid(linear)
    return logistic * (1.0 + linear * (1.0 - logistic))

def mix_channels(mixing, gated):
    flat_gated = gated.reshape(gated.shape[0], -1)
    mixed = jnp.dot(mixing, flat_gated, preferred_element_type=jnp.float32)
    return mixed.reshape((mixing.shape[0],) + gated.shape[1:])

def unfold(field):
    return field.reshape(field.shape[0], field.shape[1], -1, LAYERS)

def refold(field):
    return field.reshape(field.shape[0], field.shape[1], -1)

def reference(features, cotangent, kernel_a, kernel_b, mixing):
    features = unfold(features)
    cotangent = unfold(cotangent)
    fine_pad = wrap_pad(features)
    linear_a = convolve(fine_pad, kernel_a)
    hidden = jax.nn.silu(linear_a).astype(jnp.bfloat16)
    coarse = block_view(hidden).mean(axis=(2, 4)).astype(jnp.bfloat16)
    coarse_pad = wrap_pad(coarse)
    linear_b = convolve(coarse_pad, kernel_b)
    gated = jax.nn.silu(linear_b).astype(jnp.bfloat16)
    projected = mix_channels(mixing, gated).astype(jnp.bfloat16)
    output = (hidden.astype(jnp.float32) + widened(projected.astype(jnp.float32))).astype(jnp.bfloat16)
    folded = block_view(cotangent).sum(axis=(2, 4)).astype(jnp.bfloat16)
    flat_folded = folded.reshape(folded.shape[0], -1)
    mix_sum = lax.dot_general(flat_folded, gated.reshape(gated.shape[0], -1), (((1,), (1,)), ((), ())), preferred_element_type=jnp.float32)
    grad_gated = lax.dot_general(mixing, flat_folded, (((0,), (0,)), ((), ())), preferred_element_type=jnp.float32).reshape(linear_b.shape)
    grad_linear_b = (grad_gated * silu_slope(linear_b)).astype(jnp.bfloat16)
    kernel_b_sum = kernel_grad(coarse_pad, grad_linear_b)
    grad_coarse = convolve(wrap_pad(grad_linear_b), flipped(kernel_b)).astype(jnp.bfloat16)
    grad_hidden = cotangent.astype(jnp.float32) + 0.25 * widened(grad_coarse.astype(jnp.float32))
    grad_linear_a = (grad_hidden * silu_slope(linear_a)).astype(jnp.bfloat16)
    kernel_a_sum = kernel_grad(fine_pad, grad_linear_a)
    grad_input = convolve(wrap_pad(grad_linear_a), flipped(kernel_a)).astype(jnp.bfloat16)
    factor = 1.0 / jnp.sqrt(jnp.float32(features.shape[1] * features.shape[2] * features.shape[3]))
    return (refold(output), refold(grad_input), kernel_a_sum * factor, kernel_b_sum * factor, mix_sum * factor)
```

```python
import functools
import math

import jax
import jax.numpy as jnp
from jax import lax
from jax.experimental import pallas as pl
from jax.experimental.pallas import tpu as pltpu
from jax.sharding import PartitionSpec as P

LAYERS = 32
PB = 4
BF = jnp.bfloat16
F32 = jnp.float32


def iota(shape, dim):
    return lax.broadcasted_iota(jnp.int32, shape, dim)


def dot(a, b):
    return jnp.dot(a, b, preferred_element_type=F32)


def dot_rows(a, b):
    return lax.dot_general(a, b, (((0,), (0,)), ((), ())), preferred_element_type=F32)


def pre_kernel(f_ref, c_ref, own_ref, lo_ref, hi_ref):
    nb = own_ref.shape[0] // 2
    for k, ref in enumerate((f_ref, c_ref)):
        ch, rows, cells = ref.shape
        swapped = jnp.swapaxes(ref[...].astype(F32), 0, 1)
        for j in range(nb):
            block = swapped[PB * j : PB * (j + 1)].reshape(PB * ch, cells)
            block = block.T.astype(BF)
            own_ref[k * nb + j] = block
            if k == 0:
                if j < 2:
                    lo_ref[j] = block
                if j >= nb - 2:
                    hi_ref[j - nb + 2] = block
            else:
                if j == 0:
                    lo_ref[2] = block
                if j == nb - 1:
                    hi_ref[2] = block


def tiles(block, down, across):
    wide = jnp.concatenate([block] * across, axis=1)
    return jnp.concatenate([wide] * down, axis=0)


def weights_kernel(ka, kat, kb, kbt, mix, mixt, wa, waf, wb, wbf, mp, mt, pool, up):
    c1 = ka.shape[1]
    c2 = kb.shape[1]

    def toeplitz(out, source, order, rows_per, cols_per, row_blocks):
        height = len(row_blocks) * rows_per
        width = PB * cols_per
        shape = (height, width)
        r = iota(shape, 0) // rows_per
        q = r
        for place, value in enumerate(row_blocks):
            if value != place:
                q = jnp.where(r == place, value, q)
        a = q - iota(shape, 1) // cols_per + 1
        for b in range(3):
            for c in range(3):
                acc = jnp.zeros(shape, F32)
                for tap in range(3):
                    block = source[order(9 * tap + 3 * b + c)].astype(F32)
                    acc = jnp.where(a == tap, tiles(block, len(row_blocks), PB), acc)
                out[b * height : (b + 1) * height, c * width : (c + 1) * width] = acc.astype(BF)

    ring = (0, 1, 2, 3, 4, 100, 100, -1)
    toeplitz(wa, kat, lambda t: t, c1, c1, ring)
    toeplitz(waf, ka, lambda t: 26 - t, c1, c1, ring)
    toeplitz(wb, kbt, lambda t: t, c1, c2, ring)
    toeplitz(wbf, kb, lambda t: 26 - t, c2, c1, (0, 1, 2, 3, 4, -1))
    same = iota(mp.shape, 0) // c2 == iota(mp.shape, 1) // c1
    mp[...] = jnp.where(same, tiles(mixt[...].astype(F32), PB, PB), 0.0).astype(BF)
    same = iota(mt.shape, 0) // c1 == iota(mt.shape, 1) // c2
    mt[...] = jnp.where(same, tiles(mix[...].astype(F32), PB, PB), 0.0).astype(BF)
    width = PB * c1
    r = iota(pool.shape, 0)
    l = iota(pool.shape, 1)
    hit = (r % c1 == l % c1) & (r // (2 * width) * 2 + r % width // c1 // 2 == l // c1)
    pool[...] = jnp.where(hit, 1.0, 0.0).astype(BF)
    r = iota(up.shape, 0)
    l = iota(up.shape, 1)
    hit = (r % c1 == l % c1) & (l // width * 2 + l % width // c1 // 2 == r // c1)
    up[...] = jnp.where(hit, 1.0, 0.0).astype(BF)


def combine(summed, width):
    rows = summed.shape[0]
    layer = iota((rows, width), 0) % LAYERS
    below = pltpu.roll(summed[:, :width], 1, 0)
    above = pltpu.roll(summed[:, 2 * width :], rows - 1, 0)
    return (
        summed[:, width : 2 * width]
        + jnp.where(layer == 0, 0.0, below)
        + jnp.where(layer == LAYERS - 1, 0.0, above)
    )


def layer_shifts(block):
    rows, width = block.shape
    layer = iota((rows, width), 0) % LAYERS
    wide = block.astype(F32)
    first = jnp.where(layer == LAYERS - 1, 0.0, pltpu.roll(wide, rows - 1, 0))
    last = jnp.where(layer == 0, 0.0, pltpu.roll(wide, 1, 0))
    return jnp.concatenate([first.astype(BF), block, last.astype(BF)], axis=1)


def taps(ref, j, start, rows):
    parts = []
    for b in range(3):
        at = start + b * LAYERS
        if not isinstance(at, int):
            at = pl.multiple_of(at, LAYERS)
        parts.append(ref[j, pl.ds(at, rows), :])
    return jnp.concatenate(parts, axis=1)


def every_other(block, which):
    count = block.shape[0] // (2 * LAYERS)
    return [block[(2 * i + which) * LAYERS : (2 * i + which + 1) * LAYERS] for i in range(count)]


def paired_rows(first, second):
    parts = []
    for block in (first, second):
        for which in range(2):
            parts.append(jnp.concatenate(every_other(block, which), axis=0))
    return jnp.concatenate(parts, axis=1)


def widen_rows(block):
    parts = []
    for i in range(block.shape[0] // LAYERS):
        part = block[i * LAYERS : (i + 1) * LAYERS]
        parts += [part, part]
    return jnp.concatenate(parts, axis=0)


def sigmoid(v):
    return 1.0 / (1.0 + jnp.exp(-v))


def main_kernel(shards, full, meta, *refs):
    pieces = refs[: 3 * shards]
    wa, waf, wb, wbf, mp, mt, pool, up = refs[3 * shards : 3 * shards + 8]
    out_ref, gin_ref, pk_ref = refs[3 * shards + 8 : 3 * shards + 11]
    fz, cot, hid, slope, cz, fold, gb, proj, gat, gz, acc_a, acc_b, packed = refs[3 * shards + 11 :]
    nbx = fz.shape[0]
    nb = nbx - 4
    nc = nbx // 2
    rows = hid.shape[1]
    rows_c = rows // 2
    own = pieces[0].shape[1]
    own_c = own // 2
    width = hid.shape[2]
    c1 = width // PB
    c2 = gb.shape[2] - 2 * width
    c2 = (gb.shape[2] - width) // PB
    wide = PB * c2

    def keep(value, scale):
        if full:
            return value
        r = iota(value.shape, 0)
        inside = (r >= meta[shards] // scale) & (r < meta[shards + 1] // scale)
        return jnp.where(inside, value, jnp.zeros_like(value))

    zero_pad = jnp.zeros((LAYERS, 1), BF)
    for ref in (fz, cz, gb, gz):
        for j in range(ref.shape[0]):
            pad = jnp.zeros((LAYERS, ref.shape[2]), BF)
            ref[j, :LAYERS, :] = pad
            ref[j, ref.shape[1] - LAYERS :, :] = pad
    del zero_pad
    zeros = jnp.zeros((rows, width), BF)
    for j in (0, nbx - 1):
        cot[j] = zeros
    for s in range(shards):
        middle, before, after = pieces[3 * s : 3 * s + 3]
        at = pl.multiple_of(meta[s] * own, own)
        for j in range(2):
            fz[j, pl.ds(LAYERS + at, own), :width] = before[j]
            fz[nbx - 2 + j, pl.ds(LAYERS + at, own), :width] = after[j]
        cot[1, pl.ds(at, own), :] = before[2]
        cot[nbx - 2, pl.ds(at, own), :] = after[2]
        for j in range(nb):
            fz[2 + j, pl.ds(LAYERS + at, own), :width] = middle[j]
            cot[2 + j, pl.ds(at, own), :] = middle[nb + j]
    own_at = pl.multiple_of(meta[0] * own, own)
    own_at_c = pl.multiple_of(meta[0] * own_c, own_c)

    def edges(ref, count, inner):
        lane = iota((inner, width), 1)
        at = slice(LAYERS, LAYERS + inner)
        for j in range(count):
            nxt = ref[j + 1, at, :width] if j + 1 < count else jnp.zeros((inner, width), BF)
            prv = ref[j - 1, at, :width] if j > 0 else jnp.zeros((inner, width), BF)
            ref[j, at, width:] = jnp.where(lane < 3 * c1, nxt, prv)

    edges(fz, nbx, rows)

    def forward(j, carry):
        linear = combine(dot(taps(fz, j, 0, rows), wa[...]), width)
        logistic = sigmoid(linear)
        hid[j] = (linear * logistic).astype(BF)
        slope[j] = logistic * (1.0 + linear * (1.0 - logistic))
        return carry

    lax.fori_loop(0, nbx, forward, 0)

    def pooling(j, carry):
        pooled = dot(paired_rows(hid[2 * j], hid[2 * j + 1]), pool[...]) * 0.25
        cz[j, LAYERS : LAYERS + rows_c, :width] = keep(pooled.astype(BF), 2)
        fold[j] = dot(paired_rows(cot[2 * j], cot[2 * j + 1]), pool[...]).astype(BF)
        return carry

    lax.fori_loop(0, nc, pooling, 0)
    edges(cz, nc, rows_c)

    def middle_level(j, carry):
        linear = combine(dot(taps(cz, j, 0, rows_c), wb[...]), wide)
        logistic = sigmoid(linear)
        gated = (linear * logistic).astype(BF)
        gat[j] = gated
        grad = dot(fold[j], mt[...]) * (logistic * (1.0 + linear * (1.0 - logistic)))
        gb[j, LAYERS : LAYERS + rows_c, :wide] = keep(grad.astype(BF), 2)
        proj[j] = dot(gated, mp[...]).astype(BF)
        return carry

    lax.fori_loop(0, nc, middle_level, 0)
    lane = iota((rows_c, width), 1)
    at_c = slice(LAYERS, LAYERS + rows_c)
    for j in range(nc):
        nxt = gb[j + 1, at_c, :width] if j + 1 < nc else jnp.zeros((rows_c, width), BF)
        prv = gb[j - 1, at_c, wide - width : wide] if j > 0 else jnp.zeros((rows_c, width), BF)
        gb[j, at_c, wide:] = jnp.where(lane < c2, nxt, prv)

    def back_coarse(j, carry):
        grad = combine(dot(taps(gb, j, 0, rows_c), wbf[...]), width).astype(BF)
        spread = 0.25 * dot(grad, up[...])
        for k in range(2):
            total = cot[2 * j + k].astype(F32) + widen_rows(spread[:, k * width : (k + 1) * width])
            gz[2 * j + k, LAYERS : LAYERS + rows, :width] = keep((total * slope[2 * j + k]).astype(BF), 1)
        return carry

    lax.fori_loop(0, nc, back_coarse, 0)
    edges(gz, nbx, rows)

    lhs = jnp.concatenate(
        [layer_shifts(gz[2 + j, pl.ds(LAYERS + own_at, own), :width]) for j in range(nb)], axis=0
    )
    rhs = jnp.concatenate([taps(fz, 2 + j, own_at, own) for j in range(nb)], axis=0)
    acc_a[...] = dot_rows(lhs, rhs)
    lhs = jnp.concatenate(
        [layer_shifts(gb[j, pl.ds(LAYERS + own_at_c, own_c), :wide]) for j in range(1, nc - 1)], axis=0
    )
    rhs = jnp.concatenate([taps(cz, j, own_at_c, own_c) for j in range(1, nc - 1)], axis=0)
    acc_b[...] = dot_rows(lhs, rhs)
    lhs = jnp.concatenate([gat[j, pl.ds(own_at_c, own_c), :] for j in range(1, nc - 1)], axis=0)
    rhs = jnp.concatenate([fold[j, pl.ds(own_at_c, own_c), :] for j in range(1, nc - 1)], axis=0)
    mixed = dot_rows(lhs, rhs)
    mix_sum = mixed[:c2, :c1]
    for p in range(1, PB):
        mix_sum = mix_sum + mixed[p * c2 : (p + 1) * c2, p * c1 : (p + 1) * c1]
    packed[c1:, 27 * c1 : 28 * c1] = mix_sum
    packed[:c1, 27 * c1 : 28 * c1] = jnp.zeros((c1, c1), F32)
    span = 2 * width
    for acc, outs, first in ((acc_a, c1, 0), (acc_b, c2, c1)):
        for b in range(3):
            for c in range(3):
                total = None
                for p in range(PB):
                    at = (c * PB + p) * outs
                    part = acc[at : at + outs, b * span : (b + 1) * span]
                    part = pltpu.roll(part, (span - (p - 1) * c1) % span, 1)
                    total = part if total is None else total + part
                for a in range(3):
                    t = 9 * a + 3 * b + c
                    packed[first : first + outs, t * c1 : (t + 1) * c1] = total[:, a * c1 : (a + 1) * c1]
    chunk = pk_ref.shape[1]
    per = packed.shape[0] // chunk
    used = packed.shape[1] // 128 * per
    for v in range(packed.shape[1] // 128):
        for r in range(per):
            pk_ref[v * per + r] = packed[r * chunk : (r + 1) * chunk, v * 128 : (v + 1) * 128].astype(BF)
    for v in range(used, pk_ref.shape[0]):
        pk_ref[v] = jnp.zeros(pk_ref.shape[1:], BF)

    def finish(j, carry):
        spread = dot(proj[j + 1, pl.ds(own_at_c, own_c), :], up[...])
        for k in range(2):
            near = hid[2 * j + 2 + k, pl.ds(own_at, own), :].astype(F32)
            total = near + widen_rows(spread[:, k * width : (k + 1) * width])
            out_ref[2 * j + k] = total.T.astype(BF)
            grad = combine(dot(taps(gz, 2 * j + 2 + k, own_at, own), waf[...]), width)
            gin_ref[2 * j + k] = grad.T.astype(BF)
        return carry

    lax.fori_loop(0, nb // 2, finish, 0)


def sum_kernel(x_ref, o_ref):
    total = jnp.sum(x_ref[...].astype(F32), axis=0).astype(BF)
    o_ref[...] = jnp.broadcast_to(total[None], o_ref.shape)


def post_kernel(factor, x_ref, ga_ref, gb_ref, gm_ref, buf):
    chunk = x_ref.shape[1]
    per = buf.shape[0] // chunk
    c1 = ga_ref.shape[1]
    for v in range(buf.shape[1] // 128):
        for r in range(per):
            buf[r * chunk : (r + 1) * chunk, v * 128 : (v + 1) * 128] = x_ref[v * per + r].astype(F32) * factor
    for t in range(27):
        ga_ref[t] = buf[:c1, t * c1 : (t + 1) * c1]
        gb_ref[t] = buf[c1:, t * c1 : (t + 1) * c1]
    gm_ref[...] = buf[c1:, 27 * c1 : 28 * c1].T


def call(kernel, outs, *args, scratch=(), smem=0, name=None):
    specs = [pl.BlockSpec(memory_space=pltpu.SMEM)] * smem
    specs += [pl.BlockSpec(memory_space=pltpu.VMEM)] * (len(args) - smem)
    return pl.pallas_call(
        kernel,
        out_shape=outs,
        in_specs=specs,
        out_specs=jax.tree.map(lambda _: pl.BlockSpec(memory_space=pltpu.VMEM), outs),
        scratch_shapes=list(scratch),
        compiler_params=pltpu.CompilerParams(vmem_limit_bytes=56 * 1024 * 1024),
        name=name,
    )(*args)


def shape(dims, dtype=BF):
    return jax.ShapeDtypeStruct(tuple(dims), dtype)


def gather_shards(own, low, high):
    n_phi = lax.axis_size("phi")
    n_eta = lax.axis_size("eta")
    e = lax.axis_index("eta")
    steps = [0] + ([] if n_eta == 1 else [1, -1] if n_eta == 2 else [-1, 1, -2, 2])
    if n_eta == 2:
        steps = [0, None]
    pieces = []
    for step in steps:
        def pairs(move):
            found = []
            for p in range(n_phi):
                for s in range(n_eta):
                    t = 1 - s if step is None else s - step
                    if 0 <= t < n_eta:
                        found.append((p * n_eta + s, (p + move) % n_phi * n_eta + t))
            return found

        pieces.append(own if step == 0 else lax.ppermute(own, ("phi", "eta"), pairs(0)))
        pieces.append(lax.ppermute(high, ("phi", "eta"), pairs(1)))
        pieces.append(lax.ppermute(low, ("phi", "eta"), pairs(-1)))
    if n_eta <= 2:
        places = [e, 1 - e][:n_eta]
        bounds = [0, 0]
    else:
        places = [2 + step for step in steps]
        bounds = [jnp.maximum(0, 2 - e), jnp.minimum(5, n_eta + 2 - e)]
    return pieces, places, bounds


def shards(features, cotangent, kernel_a, kernel_b, mixing):
    c1, n_rows, cells = features.shape
    c2 = kernel_b.shape[1]
    nb = n_rows // PB
    width = PB * c1
    own, low, high = call(
        pre_kernel,
        (shape((2 * nb, cells, width)), shape((3, cells, width)), shape((3, cells, width))),
        features,
        cotangent,
        name="pre",
    )
    pieces, places, bounds = gather_shards(own, low, high)
    count = len(places)
    full = lax.axis_size("eta") <= 2
    meta = jnp.stack([jnp.asarray(v, jnp.int32) for v in places] + [jnp.asarray(v * cells, jnp.int32) for v in bounds])
    weights = call(
        weights_kernel,
        (
            shape((3 * 2 * width, 3 * width)),
            shape((3 * 2 * width, 3 * width)),
            shape((3 * 2 * width, 3 * PB * c2)),
            shape((3 * 6 * c2, 3 * width)),
            shape((PB * c2, width)),
            shape((width, PB * c2)),
            shape((4 * width, width)),
            shape((width, 2 * width)),
        ),
        kernel_a,
        jnp.swapaxes(kernel_a, 1, 2),
        kernel_b,
        jnp.swapaxes(kernel_b, 1, 2),
        mixing,
        mixing.T,
        name="weights",
    )
    nbx = nb + 4
    nc = nbx // 2
    rows = count * cells
    rows_c = rows // 2
    devices = lax.axis_size("phi") * lax.axis_size("eta")
    lanes = 28 * c1
    total_rows = (c1 + c2) * lanes // 128
    chunk = next(d for d in range(8, c1 + c2 + 1, 8) if (c1 + c2) % d == 0 and total_rows <= d * devices)
    scratch = (
        pltpu.VMEM((nbx, rows + 2 * LAYERS, 2 * width), BF),
        pltpu.VMEM((nbx, rows, width), BF),
        pltpu.VMEM((nbx, rows, width), BF),
        pltpu.VMEM((nbx, rows, width), F32),
        pltpu.VMEM((nc, rows_c + 2 * LAYERS, 2 * width), BF),
        pltpu.VMEM((nc, rows_c, width), BF),
        pltpu.VMEM((nc, rows_c + 2 * LAYERS, PB * c2 + width), BF),
        pltpu.VMEM((nc, rows_c, width), BF),
        pltpu.VMEM((nc, rows_c, PB * c2), BF),
        pltpu.VMEM((nbx, rows + 2 * LAYERS, 2 * width), BF),
        pltpu.VMEM((3 * width, 6 * width), F32),
        pltpu.VMEM((3 * PB * c2, 6 * width), F32),
        pltpu.VMEM((c1 + c2, lanes), F32),
    )
    output, grad_input, terms = call(
        functools.partial(main_kernel, count, full),
        (shape((nb, width, cells)), shape((nb, width, cells)), shape((devices, chunk, 128))),
        meta,
        *pieces,
        *weights,
        scratch=scratch,
        smem=1,
        name="main",
    )
    axes = ("phi", "eta")
    terms = lax.all_to_all(terms, axes, 0, 0, tiled=True)
    sums = call(sum_kernel, shape(terms.shape), terms, name="sum")
    sums = lax.all_to_all(sums, axes, 0, 0, tiled=True)
    cell_count = n_rows * cells * devices
    grads = call(
        functools.partial(post_kernel, 1.0 / math.sqrt(cell_count)),
        (shape((27, c1, c1), F32), shape((27, c2, c1), F32), shape((c1, c2), F32)),
        sums,
        scratch=(pltpu.VMEM((c1 + c2, lanes), F32),),
        name="post",
    )

    def restore(blocks):
        return jnp.transpose(blocks.reshape(n_rows, c1, cells), (1, 0, 2))

    return (restore(output), restore(grad_input)) + tuple(grads)


def solution(mesh):
    in_specs = (P(None, "phi", "eta"), P(None, "phi", "eta"), P(), P(), P())
    out_specs = (P(None, "phi", "eta"), P(None, "phi", "eta"), P(), P(), P())
    return jax.shard_map(shards, mesh=mesh, in_specs=in_specs, out_specs=out_specs, check_vma=False)
```

```python
import functools
import math

import jax
import jax.numpy as jnp
from jax import lax
from jax.experimental import pallas as pl
from jax.experimental.pallas import tpu as pltpu
from jax.sharding import PartitionSpec as P

LAYERS = 32
PB = 4
BF = jnp.bfloat16
F32 = jnp.float32


def iota(shape, dim):
    return lax.broadcasted_iota(jnp.int32, shape, dim)


def dot(a, b):
    return jnp.dot(a, b, preferred_element_type=F32)


def dot_rows(a, b):
    return lax.dot_general(a, b, (((0,), (0,)), ((), ())), preferred_element_type=F32)


def pre_kernel(f_ref, c_ref, own_ref, lo_ref, hi_ref):
    nb = own_ref.shape[0] // 2
    for k, ref in enumerate((f_ref, c_ref)):
        ch, rows, cells = ref.shape
        swapped = jnp.swapaxes(ref[...].astype(F32), 0, 1)
        for j in range(nb):
            block = swapped[PB * j : PB * (j + 1)].reshape(PB * ch, cells)
            block = block.T.astype(BF)
            own_ref[k * nb + j] = block
            if k == 0:
                if j < 2:
                    lo_ref[j] = block
                if j >= nb - 2:
                    hi_ref[j - nb + 2] = block
            else:
                if j == 0:
                    lo_ref[2] = block
                if j == nb - 1:
                    hi_ref[2] = block


def copies(size, times):
    shape = (size, size * times)
    return jnp.where(iota(shape, 0) == iota(shape, 1) % size, 1.0, 0.0).astype(BF)


def weights_kernel(ka, kbt, mix, wa, waf, wb, wbf, mp, mt, pool, up, ta, taf, tb, tbf):
    c1 = ka.shape[1]
    c2 = kbt.shape[2]
    width = PB * c1
    wide = PB * c2

    def flat(block):
        return block.reshape(-1, block.shape[2])

    def turned(ref):
        return jnp.swapaxes(ref[...].astype(F32), 1, 2).astype(BF)

    few = copies(c1, PB)
    many = copies(c2, PB)
    ta[...] = dot(flat(turned(ka)), few)
    taf[...] = dot(flat(ka[...]), few)
    tb[...] = dot(flat(kbt[...]), many)
    tbf[...] = dot(flat(turned(kbt)), few)

    def toeplitz(out, source, order, rows_per, cols_per, row_blocks):
        height = len(row_blocks) * rows_per
        across = PB * cols_per
        place = iota((rows_per, across), 1) // cols_per
        for b in range(3):
            for c in range(3):
                for at, q in enumerate(row_blocks):
                    value = jnp.zeros((rows_per, across), F32)
                    for a in range(3):
                        if 0 <= q + 1 - a < PB:
                            t = order(9 * a + 3 * b + c) * rows_per
                            value = jnp.where(place == q + 1 - a, source[t : t + rows_per], value)
                    first = b * height + at * rows_per
                    out[first : first + rows_per, c * across : (c + 1) * across] = value.astype(BF)

    ring = (0, 1, 2, 3, 4, 100, 100, -1)
    toeplitz(wa, ta, lambda t: t, c1, c1, ring)
    toeplitz(wb, tb, lambda t: t, c1, c2, ring)
    toeplitz(wbf, tbf, lambda t: 26 - t, c2, c1, (0, 1, 2, 3, 4, -1))
    toeplitz(waf, taf, lambda t: 26 - t, c1, c1, ring)
    mixing = mix[...]
    spread = dot(mixing, many)
    spread_t = dot(mixing.astype(F32).T.astype(BF), few)
    for p in range(PB):
        inside = iota((c1, wide), 1) // c2 == p
        mt[p * c1 : (p + 1) * c1] = jnp.where(inside, spread, 0.0).astype(BF)
        inside = iota((c2, width), 1) // c1 == p
        mp[p * c2 : (p + 1) * c2] = jnp.where(inside, spread_t, 0.0).astype(BF)
    r = iota(pool.shape, 0)
    l = iota(pool.shape, 1)
    hit = (r % c1 == l % c1) & (r // (2 * width) * 2 + r % width // c1 // 2 == l // c1)
    pool[...] = jnp.where(hit, 1.0, 0.0).astype(BF)
    r = iota(up.shape, 0)
    l = iota(up.shape, 1)
    hit = (r % c1 == l % c1) & (l // width * 2 + l % width // c1 // 2 == r // c1)
    up[...] = jnp.where(hit, 1.0, 0.0).astype(BF)


def combine(summed, width):
    rows = summed.shape[0]
    layer = iota((rows, width), 0) % LAYERS
    below = pltpu.roll(summed[:, :width], 1, 0)
    above = pltpu.roll(summed[:, 2 * width :], rows - 1, 0)
    return (
        summed[:, width : 2 * width]
        + jnp.where(layer == 0, 0.0, below)
        + jnp.where(layer == LAYERS - 1, 0.0, above)
    )


def layer_shifts(block):
    rows, width = block.shape
    layer = iota((rows, width), 0) % LAYERS
    wide = block.astype(F32)
    first = jnp.where(layer == LAYERS - 1, 0.0, pltpu.roll(wide, rows - 1, 0))
    last = jnp.where(layer == 0, 0.0, pltpu.roll(wide, 1, 0))
    return jnp.concatenate([first.astype(BF), block, last.astype(BF)], axis=1)


def taps(ref, j, start, rows):
    parts = []
    for b in range(3):
        at = start + b * LAYERS
        if not isinstance(at, int):
            at = pl.multiple_of(at, LAYERS)
        parts.append(ref[j, pl.ds(at, rows), :])
    return jnp.concatenate(parts, axis=1)


def every_other(block, which):
    count = block.shape[0] // (2 * LAYERS)
    return [block[(2 * i + which) * LAYERS : (2 * i + which + 1) * LAYERS] for i in range(count)]


def paired_rows(first, second):
    parts = []
    for block in (first, second):
        for which in range(2):
            parts.append(jnp.concatenate(every_other(block, which), axis=0))
    return jnp.concatenate(parts, axis=1)


def widen_rows(block):
    parts = []
    for i in range(block.shape[0] // LAYERS):
        part = block[i * LAYERS : (i + 1) * LAYERS]
        parts += [part, part]
    return jnp.concatenate(parts, axis=0)


def sigmoid(v):
    return 1.0 / (1.0 + jnp.exp(-v))


def main_kernel(shards, full, meta, *refs):
    pieces = refs[: 3 * shards]
    wa, waf, wb, wbf, mp, mt, pool, up = refs[3 * shards : 3 * shards + 8]
    out_ref, gin_ref, pk_ref = refs[3 * shards + 8 : 3 * shards + 11]
    fz, cot, hid, slope, cz, fold, gb, proj, gat, gz, acc_a, acc_b, packed = refs[3 * shards + 11 :]
    nbx = fz.shape[0]
    nb = nbx - 4
    nc = nbx // 2
    rows = hid.shape[1]
    rows_c = rows // 2
    own = pieces[0].shape[1]
    own_c = own // 2
    width = hid.shape[2]
    c1 = width // PB
    c2 = (gb.shape[2] - width) // PB
    wide = PB * c2

    def keep(value, scale):
        if full:
            return value
        r = iota(value.shape, 0)
        inside = (r >= meta[shards] // scale) & (r < meta[shards + 1] // scale)
        return jnp.where(inside, value, jnp.zeros_like(value))

    for ref in (fz, cz, gb, gz):
        for j in range(ref.shape[0]):
            pad = jnp.zeros((LAYERS, ref.shape[2]), BF)
            ref[j, :LAYERS, :] = pad
            ref[j, ref.shape[1] - LAYERS :, :] = pad
    zeros = jnp.zeros((rows, width), BF)
    for j in (0, nbx - 1):
        cot[j] = zeros
    for s in range(shards):
        middle, before, after = pieces[3 * s : 3 * s + 3]
        at = pl.multiple_of(meta[s] * own, own)
        for j in range(2):
            fz[j, pl.ds(LAYERS + at, own), :width] = before[j]
            fz[nbx - 2 + j, pl.ds(LAYERS + at, own), :width] = after[j]
        cot[1, pl.ds(at, own), :] = before[2]
        cot[nbx - 2, pl.ds(at, own), :] = after[2]
        for j in range(nb):
            fz[2 + j, pl.ds(LAYERS + at, own), :width] = middle[j]
            cot[2 + j, pl.ds(at, own), :] = middle[nb + j]
    own_at = pl.multiple_of(meta[0] * own, own)
    own_at_c = pl.multiple_of(meta[0] * own_c, own_c)

    def edges(ref, count, inner):
        lane = iota((inner, width), 1)
        at = slice(LAYERS, LAYERS + inner)
        for j in range(count):
            nxt = ref[j + 1, at, :width] if j + 1 < count else jnp.zeros((inner, width), BF)
            prv = ref[j - 1, at, :width] if j > 0 else jnp.zeros((inner, width), BF)
            ref[j, at, width:] = jnp.where(lane < 3 * c1, nxt, prv)

    edges(fz, nbx, rows)

    def forward(j, carry):
        linear = combine(dot(taps(fz, j, 0, rows), wa[...]), width)
        logistic = sigmoid(linear)
        hid[j] = (linear * logistic).astype(BF)
        slope[j] = logistic * (1.0 + linear * (1.0 - logistic))
        return carry

    lax.fori_loop(0, nbx, forward, 0)

    def pooling(j, carry):
        pooled = dot(paired_rows(hid[2 * j], hid[2 * j + 1]), pool[...]) * 0.25
        cz[j, LAYERS : LAYERS + rows_c, :width] = keep(pooled.astype(BF), 2)
        fold[j] = dot(paired_rows(cot[2 * j], cot[2 * j + 1]), pool[...]).astype(BF)
        return carry

    lax.fori_loop(0, nc, pooling, 0)
    edges(cz, nc, rows_c)

    def middle_level(j, carry):
        linear = combine(dot(taps(cz, j, 0, rows_c), wb[...]), wide)
        logistic = sigmoid(linear)
        gated = (linear * logistic).astype(BF)
        gat[j] = gated
        grad = dot(fold[j], mt[...]) * (logistic * (1.0 + linear * (1.0 - logistic)))
        gb[j, LAYERS : LAYERS + rows_c, :wide] = keep(grad.astype(BF), 2)
        proj[j] = dot(gated, mp[...]).astype(BF)
        return carry

    lax.fori_loop(0, nc, middle_level, 0)
    lane = iota((rows_c, width), 1)
    at_c = slice(LAYERS, LAYERS + rows_c)
    for j in range(nc):
        nxt = gb[j + 1, at_c, :width] if j + 1 < nc else jnp.zeros((rows_c, width), BF)
        prv = gb[j - 1, at_c, wide - width : wide] if j > 0 else jnp.zeros((rows_c, width), BF)
        gb[j, at_c, wide:] = jnp.where(lane < c2, nxt, prv)

    def back_coarse(j, carry):
        grad = combine(dot(taps(gb, j, 0, rows_c), wbf[...]), width).astype(BF)
        spread = 0.25 * dot(grad, up[...])
        for k in range(2):
            total = cot[2 * j + k].astype(F32) + widen_rows(spread[:, k * width : (k + 1) * width])
            gz[2 * j + k, LAYERS : LAYERS + rows, :width] = keep((total * slope[2 * j + k]).astype(BF), 1)
        return carry

    lax.fori_loop(0, nc, back_coarse, 0)
    edges(gz, nbx, rows)

    lhs = jnp.concatenate(
        [layer_shifts(gz[2 + j, pl.ds(LAYERS + own_at, own), :width]) for j in range(nb)], axis=0
    )
    rhs = jnp.concatenate([taps(fz, 2 + j, own_at, own) for j in range(nb)], axis=0)
    acc_a[...] = dot_rows(lhs, rhs)
    lhs = jnp.concatenate(
        [layer_shifts(gb[j, pl.ds(LAYERS + own_at_c, own_c), :wide]) for j in range(1, nc - 1)], axis=0
    )
    rhs = jnp.concatenate([taps(cz, j, own_at_c, own_c) for j in range(1, nc - 1)], axis=0)
    acc_b[...] = dot_rows(lhs, rhs)
    lhs = jnp.concatenate([gat[j, pl.ds(own_at_c, own_c), :] for j in range(1, nc - 1)], axis=0)
    rhs = jnp.concatenate([fold[j, pl.ds(own_at_c, own_c), :] for j in range(1, nc - 1)], axis=0)
    mixed = dot_rows(lhs, rhs)
    mix_sum = mixed[:c2, :c1]
    for p in range(1, PB):
        mix_sum = mix_sum + mixed[p * c2 : (p + 1) * c2, p * c1 : (p + 1) * c1]
    packed[c1:, 27 * c1 : 28 * c1] = mix_sum
    packed[:c1, 27 * c1 : 28 * c1] = jnp.zeros((c1, c1), F32)
    span = 2 * width
    for acc, outs, first in ((acc_a, c1, 0), (acc_b, c2, c1)):
        for b in range(3):
            for c in range(3):
                total = None
                for p in range(PB):
                    at = (c * PB + p) * outs
                    part = acc[at : at + outs, b * span : (b + 1) * span]
                    part = pltpu.roll(part, (span - (p - 1) * c1) % span, 1)
                    total = part if total is None else total + part
                for a in range(3):
                    t = 9 * a + 3 * b + c
                    packed[first : first + outs, t * c1 : (t + 1) * c1] = total[:, a * c1 : (a + 1) * c1]
    chunk = pk_ref.shape[1]
    per = packed.shape[0] // chunk
    used = packed.shape[1] // 128 * per
    for v in range(packed.shape[1] // 128):
        for r in range(per):
            pk_ref[v * per + r] = packed[r * chunk : (r + 1) * chunk, v * 128 : (v + 1) * 128].astype(BF)
    for v in range(used, pk_ref.shape[0]):
        pk_ref[v] = jnp.zeros(pk_ref.shape[1:], BF)

    def finish(j, carry):
        spread = dot(proj[j + 1, pl.ds(own_at_c, own_c), :], up[...])
        for k in range(2):
            near = hid[2 * j + 2 + k, pl.ds(own_at, own), :].astype(F32)
            total = near + widen_rows(spread[:, k * width : (k + 1) * width])
            out_ref[2 * j + k] = total.T.astype(BF)
            grad = combine(dot(taps(gz, 2 * j + 2 + k, own_at, own), waf[...]), width)
            gin_ref[2 * j + k] = grad.T.astype(BF)
        return carry

    lax.fori_loop(0, nb // 2, finish, 0)


def sum_kernel(x_ref, o_ref):
    total = jnp.sum(x_ref[...].astype(F32), axis=0).astype(BF)
    o_ref[...] = jnp.broadcast_to(total[None], o_ref.shape)


def post_kernel(factor, x_ref, ga_ref, gb_ref, gm_ref, buf):
    chunk = x_ref.shape[1]
    per = buf.shape[0] // chunk
    c1 = ga_ref.shape[1]
    for v in range(buf.shape[1] // 128):
        for r in range(per):
            buf[r * chunk : (r + 1) * chunk, v * 128 : (v + 1) * 128] = x_ref[v * per + r].astype(F32) * factor
    for t in range(27):
        ga_ref[t] = buf[:c1, t * c1 : (t + 1) * c1]
        gb_ref[t] = buf[c1:, t * c1 : (t + 1) * c1].T
    gm_ref[...] = buf[c1:, 27 * c1 : 28 * c1].T


def call(kernel, outs, *args, scratch=(), smem=0, near=(), name=None):
    args = [
        pltpu.with_memory_space_constraint(arg, pltpu.VMEM) if place in near else arg
        for place, arg in enumerate(args)
    ]
    specs = [pl.BlockSpec(memory_space=pltpu.SMEM)] * smem
    specs += [pl.BlockSpec(memory_space=pltpu.VMEM)] * (len(args) - smem)
    return pl.pallas_call(
        kernel,
        out_shape=outs,
        in_specs=specs,
        out_specs=tuple(pl.BlockSpec(memory_space=pltpu.VMEM) for _ in outs),
        scratch_shapes=list(scratch),
        compiler_params=pltpu.CompilerParams(vmem_limit_bytes=40 * 1024 * 1024),
        name=name,
    )(*args)


def shape(dims, dtype=BF):
    return jax.ShapeDtypeStruct(tuple(dims), dtype)


def gather_shards(own, low, high):
    n_phi = lax.axis_size("phi")
    n_eta = lax.axis_size("eta")
    e = lax.axis_index("eta")
    steps = [0] + ([] if n_eta == 1 else [1, -1] if n_eta == 2 else [-1, 1, -2, 2])
    if n_eta == 2:
        steps = [0, None]
    pieces = []
    for step in steps:
        def pairs(move):
            found = []
            for p in range(n_phi):
                for s in range(n_eta):
                    t = 1 - s if step is None else s - step
                    if 0 <= t < n_eta:
                        found.append((p * n_eta + s, (p + move) % n_phi * n_eta + t))
            return found

        pieces.append(own if step == 0 else lax.ppermute(own, ("phi", "eta"), pairs(0)))
        pieces.append(lax.ppermute(high, ("phi", "eta"), pairs(1)))
        pieces.append(lax.ppermute(low, ("phi", "eta"), pairs(-1)))
    if n_eta <= 2:
        places = [e, 1 - e][:n_eta]
        bounds = [0, 0]
    else:
        places = [2 + step for step in steps]
        bounds = [jnp.maximum(0, 2 - e), jnp.minimum(5, n_eta + 2 - e)]
    return pieces, places, bounds


def shards(features, cotangent, kernel_a, kernel_b, mixing):
    c1, n_rows, cells = features.shape
    c2 = kernel_b.shape[1]
    nb = n_rows // PB
    width = PB * c1
    own, low, high = call(
        pre_kernel,
        (shape((2 * nb, cells, width)), shape((3, cells, width)), shape((3, cells, width))),
        features,
        cotangent,
        name="pre",
    )
    pieces, places, bounds = gather_shards(own, low, high)
    count = len(places)
    full = lax.axis_size("eta") <= 2
    meta = jnp.stack([jnp.asarray(v, jnp.int32) for v in places] + [jnp.asarray(v * cells, jnp.int32) for v in bounds])
    weights = call(
        weights_kernel,
        (
            pltpu.VMEM((3 * 2 * width, 3 * width), BF),
            pltpu.VMEM((3 * 2 * width, 3 * width), BF),
            pltpu.VMEM((3 * 2 * width, 3 * PB * c2), BF),
            pltpu.VMEM((3 * 6 * c2, 3 * width), BF),
            pltpu.VMEM((PB * c2, width), BF),
            pltpu.VMEM((width, PB * c2), BF),
            pltpu.VMEM((4 * width, width), BF),
            pltpu.VMEM((width, 2 * width), BF),
        ),
        kernel_a,
        jnp.swapaxes(kernel_b, 1, 2),
        mixing,
        scratch=(
            pltpu.VMEM((27 * c1, width), F32),
            pltpu.VMEM((27 * c1, width), F32),
            pltpu.VMEM((27 * c1, PB * c2), F32),
            pltpu.VMEM((27 * c2, width), F32),
        ),
        name="weights",
    )
    nbx = nb + 4
    nc = nbx // 2
    rows = count * cells
    rows_c = rows // 2
    devices = lax.axis_size("phi") * lax.axis_size("eta")
    lanes = 28 * c1
    total_rows = (c1 + c2) * lanes // 128
    chunk = next(d for d in range(8, c1 + c2 + 1, 8) if (c1 + c2) % d == 0 and total_rows <= d * devices)
    scratch = (
        pltpu.VMEM((nbx, rows + 2 * LAYERS, 2 * width), BF),
        pltpu.VMEM((nbx, rows, width), BF),
        pltpu.VMEM((nbx, rows, width), BF),
        pltpu.VMEM((nbx, rows, width), F32),
        pltpu.VMEM((nc, rows_c + 2 * LAYERS, 2 * width), BF),
        pltpu.VMEM((nc, rows_c, width), BF),
        pltpu.VMEM((nc, rows_c + 2 * LAYERS, PB * c2 + width), BF),
        pltpu.VMEM((nc, rows_c, width), BF),
        pltpu.VMEM((nc, rows_c, PB * c2), BF),
        pltpu.VMEM((nbx, rows + 2 * LAYERS, 2 * width), BF),
        pltpu.VMEM((3 * width, 6 * width), F32),
        pltpu.VMEM((3 * PB * c2, 6 * width), F32),
        pltpu.VMEM((c1 + c2, lanes), F32),
    )
    output, grad_input, terms = call(
        functools.partial(main_kernel, count, full),
        (shape((nb, width, cells)), shape((nb, width, cells)), shape((devices, chunk, 128))),
        meta,
        *pieces,
        *weights,
        scratch=scratch,
        smem=1,
        near=range(2, 1 + len(pieces) + len(weights)),
        name="main",
    )
    axes = ("phi", "eta")
    terms = lax.all_to_all(terms, axes, 0, 0, tiled=True)
    (sums,) = call(sum_kernel, (shape(terms.shape),), terms, name="sum")
    sums = lax.all_to_all(sums, axes, 0, 0, tiled=True)
    cell_count = n_rows * cells * devices
    grad_a, grad_b, grad_mix = call(
        functools.partial(post_kernel, 1.0 / math.sqrt(cell_count)),
        (shape((27, c1, c1), F32), shape((27, c1, c2), F32), shape((c1, c2), F32)),
        sums,
        scratch=(pltpu.VMEM((c1 + c2, lanes), F32),),
        name="post",
    )

    def restore(blocks):
        return jnp.transpose(blocks.reshape(n_rows, c1, cells), (1, 0, 2))

    return restore(output), restore(grad_input), grad_a, jnp.swapaxes(grad_b, 1, 2), grad_mix


def solution(mesh):
    in_specs = (P(None, "phi", "eta"), P(None, "phi", "eta"), P(), P(), P())
    out_specs = (P(None, "phi", "eta"), P(None, "phi", "eta"), P(), P(), P())
    return jax.shard_map(shards, mesh=mesh, in_specs=in_specs, out_specs=out_specs, check_vma=False)
```

```python
import functools
import math

import jax
import jax.numpy as jnp
from jax import lax
from jax.experimental import pallas as pl
from jax.experimental.pallas import tpu as pltpu
from jax.sharding import PartitionSpec as P

LAYERS = 32
PB = 4
BF = jnp.bfloat16
F32 = jnp.float32


def iota(shape, dim):
    return lax.broadcasted_iota(jnp.int32, shape, dim)


def dot(a, b):
    return jnp.dot(a, b, preferred_element_type=F32)


def dot_rows(a, b):
    return lax.dot_general(a, b, (((0,), (0,)), ((), ())), preferred_element_type=F32)


def fetch(sources, places, sems):
    moves = [pltpu.make_async_copy(src, dst, sems.at[i]) for i, (src, dst) in enumerate(zip(sources, places))]
    for move in moves:
        move.start()
    return moves


def pre_kernel(paired, f_hbm, c_hbm, f_own, f_first, f_second, c_own, c_first, c_second, *rest):
    f_ref, c_ref, sems = rest[-3:]
    nb = f_own.shape[0]
    moves = fetch((f_hbm, c_hbm), (f_ref, c_ref), sems)
    e = lax.axis_index("eta") if paired else 1
    for move, ref, own, rims in zip(moves, (f_ref, c_ref), (f_own, c_own), ((f_first, f_second), (c_first, c_second))):
        move.wait()
        ch, rows, cells = ref.shape
        swapped = jnp.swapaxes(ref[...].astype(F32), 0, 1)
        for j in range(nb):
            own[j] = swapped[PB * j : PB * (j + 1)].reshape(PB * ch, cells).T.astype(BF)
        for rim, low in zip(rims, (e, 1 - e)):
            for j in range(rim.shape[0]):
                rim[j] = own[(nb - rim.shape[0]) * (1 - low) + j]
    if paired:
        partner = rest[0]
        for j in range(partner.shape[0]):
            partner[j] = c_own[(1 - e) * (nb // 2 - 1) + j]


def copies(size, times):
    shape = (size, size * times)
    return jnp.where(iota(shape, 0) == iota(shape, 1) % size, 1.0, 0.0).astype(BF)


def weights_kernel(
    ka_hbm, kbt_hbm, mix_hbm, wa, waf, wb, wbf, mp, mt, pool, up, ta, taf, tb, tbf, ka, kbt, mix, sems
):
    for move in fetch((ka_hbm, kbt_hbm, mix_hbm), (ka, kbt, mix), sems):
        move.wait()
    c1 = ka.shape[1]
    c2 = kbt.shape[2]
    width = PB * c1
    wide = PB * c2

    def flat(block):
        return block.reshape(-1, block.shape[2])

    def turned(ref):
        return jnp.swapaxes(ref[...].astype(F32), 1, 2).astype(BF)

    few = copies(c1, PB)
    many = copies(c2, PB)
    ta[...] = dot(flat(turned(ka)), few)
    taf[...] = dot(flat(ka[...]), few)
    tb[...] = dot(flat(kbt[...]), many)
    tbf[...] = dot(flat(turned(kbt)), few)

    def toeplitz(out, source, order, rows_per, cols_per, row_blocks):
        height = len(row_blocks) * rows_per
        across = PB * cols_per
        place = iota((rows_per, across), 1) // cols_per
        for b in range(3):
            for c in range(3):
                for at, q in enumerate(row_blocks):
                    value = jnp.zeros((rows_per, across), F32)
                    for a in range(3):
                        if 0 <= q + 1 - a < PB:
                            t = order(9 * a + 3 * b + c) * rows_per
                            value = jnp.where(place == q + 1 - a, source[t : t + rows_per], value)
                    first = b * height + at * rows_per
                    out[first : first + rows_per, c * across : (c + 1) * across] = value.astype(BF)

    ring = (0, 1, 2, 3, 4, 100, 100, -1)
    toeplitz(wa, ta, lambda t: t, c1, c1, ring)
    toeplitz(wb, tb, lambda t: t, c1, c2, ring)
    toeplitz(wbf, tbf, lambda t: 26 - t, c2, c1, (0, 1, 2, 3, 4, -1))
    toeplitz(waf, taf, lambda t: 26 - t, c1, c1, ring)
    mixing = mix[...]
    spread = dot(mixing, many)
    spread_t = dot(mixing.astype(F32).T.astype(BF), few)
    for p in range(PB):
        inside = iota((c1, wide), 1) // c2 == p
        mt[p * c1 : (p + 1) * c1] = jnp.where(inside, spread, 0.0).astype(BF)
        inside = iota((c2, width), 1) // c1 == p
        mp[p * c2 : (p + 1) * c2] = jnp.where(inside, spread_t, 0.0).astype(BF)
    r = iota(pool.shape, 0)
    l = iota(pool.shape, 1)
    hit = (r % c1 == l % c1) & (r // (2 * width) * 2 + r % width // c1 // 2 == l // c1)
    pool[...] = jnp.where(hit, 1.0, 0.0).astype(BF)
    r = iota(up.shape, 0)
    l = iota(up.shape, 1)
    hit = (r % c1 == l % c1) & (l // width * 2 + l % width // c1 // 2 == r // c1)
    up[...] = jnp.where(hit, 1.0, 0.0).astype(BF)


def combine(summed, width):
    rows = summed.shape[0]
    layer = iota((rows, width), 0) % LAYERS
    below = pltpu.roll(summed[:, :width], 1, 0)
    above = pltpu.roll(summed[:, 2 * width :], rows - 1, 0)
    return (
        summed[:, width : 2 * width]
        + jnp.where(layer == 0, 0.0, below)
        + jnp.where(layer == LAYERS - 1, 0.0, above)
    )


def layer_shifts(block):
    rows, width = block.shape
    layer = iota((rows, width), 0) % LAYERS
    wide = block.astype(F32)
    first = jnp.where(layer == LAYERS - 1, 0.0, pltpu.roll(wide, rows - 1, 0))
    last = jnp.where(layer == 0, 0.0, pltpu.roll(wide, 1, 0))
    return jnp.concatenate([first.astype(BF), block, last.astype(BF)], axis=1)


def taps(ref, j, start, rows):
    parts = []
    for b in range(3):
        at = start + b * LAYERS
        if not isinstance(at, int):
            at = pl.multiple_of(at, LAYERS)
        parts.append(ref[j, pl.ds(at, rows), :])
    return jnp.concatenate(parts, axis=1)


def every_other(block, which):
    count = block.shape[0] // (2 * LAYERS)
    return [block[(2 * i + which) * LAYERS : (2 * i + which + 1) * LAYERS] for i in range(count)]


def paired_rows(first, second):
    parts = []
    for block in (first, second):
        for which in range(2):
            parts.append(jnp.concatenate(every_other(block, which), axis=0))
    return jnp.concatenate(parts, axis=1)


def widen_rows(block):
    parts = []
    for i in range(block.shape[0] // LAYERS):
        part = block[i * LAYERS : (i + 1) * LAYERS]
        parts += [part, part]
    return jnp.concatenate(parts, axis=0)


def sigmoid(v):
    return 1.0 / (1.0 + jnp.exp(-v))


def edges(ref, first, last, inner, width, split):
    lane = iota((inner, width), 1)
    at = slice(LAYERS, LAYERS + inner)
    main = ref.shape[2] - width
    for j in range(first, last):
        nxt = ref[j + 1, at, :width] if j + 1 < ref.shape[0] else jnp.zeros((inner, width), BF)
        prv = ref[j - 1, at, main - width : main] if j > 0 else jnp.zeros((inner, width), BF)
        ref[j, at, main:] = jnp.where(lane < split, nxt, prv)


def blank_rims(ref):
    pad = jnp.zeros((LAYERS, ref.shape[2]), BF)
    for j in range(ref.shape[0]):
        ref[j, :LAYERS, :] = pad
        ref[j, ref.shape[1] - LAYERS :, :] = pad


def keep_inside(meta, shards_seen, value, scale):
    if meta is None or shards_seen == 1:
        return value
    r = iota(value.shape, 0)
    inside = (r >= meta[shards_seen] // scale) & (r < meta[shards_seen + 1] // scale)
    return jnp.where(inside, value, jnp.zeros_like(value))


def forward_kernel(paired, count, *refs):
    meta = None
    if not paired:
        meta, refs = refs[0], refs[1:]
    pieces, refs = refs[:count], refs[count:]
    wa, wb, mp, pool = refs[:4]
    fz, hid, slope, cz, gat, slope_b, proj = refs[4:]
    nbx = fz.shape[0]
    nc = gat.shape[0]
    rows = hid.shape[1]
    rows_c = rows // 2
    width = hid.shape[2]
    c1 = width // PB
    wide = gat.shape[2]
    blank_rims(fz)
    blank_rims(cz)
    cells = pieces[0].shape[1]
    if paired:
        own, partner, near, far = pieces
        nb = own.shape[0]
        e = lax.axis_index("eta")
        for chunk, rim, shard in ((own, near, e), (partner, far, 1 - e)):
            at = pl.multiple_of(LAYERS + shard * cells, LAYERS)
            for j in range(nb // 2 + 2):
                fz[j + 2 * (1 - e), pl.ds(at, cells), :width] = chunk[j + e * (nb // 2 - 2)]
            for j in range(2):
                fz[e * (nbx - 2) + j, pl.ds(at, cells), :width] = rim[j]
    else:
        for s in range(count // 3):
            middle, before, after = pieces[3 * s : 3 * s + 3]
            at = pl.multiple_of(LAYERS + meta[s] * cells, LAYERS)
            for j in range(2):
                fz[j, pl.ds(at, cells), :width] = before[j]
                fz[nbx - 2 + j, pl.ds(at, cells), :width] = after[j]
            for j in range(nbx - 4):
                fz[2 + j, pl.ds(at, cells), :width] = middle[j]
    edges(fz, 0, nbx, rows, width, 3 * c1)
    for j in range(nbx):
        linear = combine(dot(taps(fz, j, 0, rows), wa[...]), width)
        logistic = sigmoid(linear)
        hid[j] = (linear * logistic).astype(BF)
        slope[j] = logistic * (1.0 + linear * (1.0 - logistic))
    for j in range(nc + 2):
        first, second = max(2 * j - 1, 0), min(2 * j, nbx - 1)
        pooled = dot(paired_rows(hid[first], hid[second]), pool[...]) * 0.25
        cz[j, LAYERS : LAYERS + rows_c, :width] = keep_inside(meta, count // 3, pooled.astype(BF), 2)
    edges(cz, 1, nc + 1, rows_c, width, 3 * c1)
    for j in range(nc):
        linear = combine(dot(taps(cz, j + 1, 0, rows_c), wb[...]), wide)
        logistic = sigmoid(linear)
        gated = (linear * logistic).astype(BF)
        gat[j] = gated
        slope_b[j] = logistic * (1.0 + linear * (1.0 - logistic))
        proj[j] = dot(gated, mp[...]).astype(BF)


def backward_kernel(paired, count, *refs):
    meta = None
    if not paired:
        meta, refs = refs[0], refs[1:]
    pieces, refs = refs[:count], refs[count:]
    fz, slope, cz, gat, slope_b, wbf, mt, pool, up = refs[:9]
    gz, pk_ref = refs[9:11]
    cot, gb, fold, acc_a, acc_b, packed = refs[11:]
    nbx = fz.shape[0]
    nb = nbx - 4
    nc = gat.shape[0]
    rows = cot.shape[1]
    rows_c = rows // 2
    width = cot.shape[2]
    wide = gat.shape[2]
    c1 = width // PB
    c2 = wide // PB
    cells = pieces[0].shape[1]
    blank_rims(gz)
    blank_rims(gb)
    if paired:
        own, partner, near, far = pieces
        e = lax.axis_index("eta")
        for rim, shard in ((near, e), (far, 1 - e)):
            at = pl.multiple_of(shard * cells, cells)
            cot[1 + e * (nbx - 3), pl.ds(at, cells), :] = rim[0]
            for j in range(partner.shape[0]):
                if rim is near:
                    block = own[j + e * (own.shape[0] // 2 - 1)]
                else:
                    block = partner[j]
                cot[j + 2 - e, pl.ds(at, cells), :] = block
        own, own_at, own_at_c = rows, 0, 0
    else:
        for s in range(count // 3):
            middle, before, after = pieces[3 * s : 3 * s + 3]
            at = pl.multiple_of(meta[s] * cells, cells)
            cot[1, pl.ds(at, cells), :] = before[0]
            cot[nbx - 2, pl.ds(at, cells), :] = after[0]
            for j in range(nb):
                cot[2 + j, pl.ds(at, cells), :] = middle[j]
        own = cells
        own_at = pl.multiple_of(meta[0] * own, own)
        own_at_c = pl.multiple_of(meta[0] * (own // 2), own // 2)
    own_c = own // 2

    for j in range(nc):
        fold[j] = dot(paired_rows(cot[2 * j + 1], cot[2 * j + 2]), pool[...]).astype(BF)
        grad = dot(fold[j], mt[...]) * slope_b[j]
        gb[j, LAYERS : LAYERS + rows_c, :wide] = keep_inside(meta, count // 3, grad.astype(BF), 2)
    edges(gb, 0, nc, rows_c, width, c2)
    for j in range(nc):
        grad = combine(dot(taps(gb, j, 0, rows_c), wbf[...]), width).astype(BF)
        spread = 0.25 * dot(grad, up[...])
        for k in range(2):
            f = 2 * j + 1 + k
            total = cot[f].astype(F32) + widen_rows(spread[:, k * width : (k + 1) * width])
            value = (total * slope[f]).astype(BF)
            gz[f, LAYERS : LAYERS + rows, :width] = keep_inside(meta, count // 3, value, 1)
    edges(gz, 2, nbx - 2, rows, width, 3 * c1)

    def own_half(value, j):
        p = iota(value.shape, 1) // (value.shape[1] // PB)
        if j == 0:
            value = jnp.where(p >= PB // 2, value, jnp.zeros_like(value))
        if j == nc - 1:
            value = jnp.where(p < PB // 2, value, jnp.zeros_like(value))
        return value

    lhs = jnp.concatenate(
        [layer_shifts(gz[2 + j, pl.ds(LAYERS + own_at, own), :width]) for j in range(nb)], axis=0
    )
    rhs = jnp.concatenate([taps(fz, 2 + j, own_at, own) for j in range(nb)], axis=0)
    acc_a[...] = dot_rows(lhs, rhs)
    lhs = jnp.concatenate(
        [layer_shifts(own_half(gb[j, pl.ds(LAYERS + own_at_c, own_c), :wide], j)) for j in range(nc)], axis=0
    )
    rhs = jnp.concatenate([taps(cz, j + 1, own_at_c, own_c) for j in range(nc)], axis=0)
    acc_b[...] = dot_rows(lhs, rhs)
    lhs = jnp.concatenate([gat[j, pl.ds(own_at_c, own_c), :] for j in range(nc)], axis=0)
    rhs = jnp.concatenate([own_half(fold[j, pl.ds(own_at_c, own_c), :], j) for j in range(nc)], axis=0)
    mixed = dot_rows(lhs, rhs)
    mix_sum = mixed[:c2, :c1]
    for p in range(1, PB):
        mix_sum = mix_sum + mixed[p * c2 : (p + 1) * c2, p * c1 : (p + 1) * c1]
    packed[c1:, 27 * c1 : 28 * c1] = mix_sum
    packed[:c1, 27 * c1 : 28 * c1] = jnp.zeros((c1, c1), F32)
    span = 2 * width
    for acc, outs, first in ((acc_a, c1, 0), (acc_b, c2, c1)):
        for b in range(3):
            for c in range(3):
                total = None
                for p in range(PB):
                    at = (c * PB + p) * outs
                    part = acc[at : at + outs, b * span : (b + 1) * span]
                    part = pltpu.roll(part, (span - (p - 1) * c1) % span, 1)
                    total = part if total is None else total + part
                for a in range(3):
                    t = 9 * a + 3 * b + c
                    packed[first : first + outs, t * c1 : (t + 1) * c1] = total[:, a * c1 : (a + 1) * c1]
    chunk = pk_ref.shape[1]
    per = packed.shape[0] // chunk
    used = packed.shape[1] // 128 * per
    for v in range(packed.shape[1] // 128):
        for r in range(per):
            pk_ref[v * per + r] = packed[r * chunk : (r + 1) * chunk, v * 128 : (v + 1) * 128].astype(BF)
    for v in range(used, pk_ref.shape[0]):
        pk_ref[v] = jnp.zeros(pk_ref.shape[1:], BF)


def finish_kernel(paired, *refs):
    meta = None
    if not paired:
        meta, refs = refs[0], refs[1:]
    gz, hid, proj, waf, up = refs[:5]
    outs = refs[5:-1]
    buf = refs[-1]
    nb = gz.shape[0] - 4
    width = hid.shape[2]
    cells = outs[0].shape[2]
    if paired:
        own, own_at, own_at_c = hid.shape[1], 0, 0
        e = lax.axis_index("eta")
        starts = [pl.multiple_of(e * cells, cells), pl.multiple_of((1 - e) * cells, cells)]
    else:
        own = cells
        own_at = pl.multiple_of(meta[0] * own, own)
        own_at_c = pl.multiple_of(meta[0] * (own // 2), own // 2)
        starts = [0]

    def write(value, place):
        buf[place] = value
        for out, start in zip(outs, starts):
            out[place] = buf[place, pl.ds(start, cells), :].T.astype(BF)

    for j in range(nb):
        grad = combine(dot(taps(gz, 2 + j, own_at, own), waf[...]), width)
        write(grad, nb + j)
    for j in range(nb):
        k = (j + 1) % 2
        spread = dot(proj[(j + 1) // 2, pl.ds(own_at_c, own // 2), :], up[:, k * width : (k + 1) * width])
        write(hid[2 + j, pl.ds(own_at, own), :].astype(F32) + widen_rows(spread), j)


def restore_kernel(kept, received, out_ref, gin_ref):
    ch, rows, cells = out_ref.shape
    half = rows // 2
    e = lax.axis_index("eta")
    for k, ref in enumerate((out_ref, gin_ref)):
        at = k * half // PB
        mine = kept[at : at + half // PB].astype(F32)
        other = received[at : at + half // PB].astype(F32)
        first = jnp.where(e == 0, mine, other).reshape(half, ch, cells)
        second = jnp.where(e == 0, other, mine).reshape(half, ch, cells)
        ref[...] = jnp.swapaxes(jnp.concatenate([first, second], axis=0), 0, 1).astype(BF)


def sum_kernel(x_ref, o_ref):
    total = jnp.sum(x_ref[...].astype(F32), axis=0).astype(BF)
    o_ref[...] = jnp.broadcast_to(total[None], o_ref.shape)


def post_kernel(factor, x_ref, ga_ref, gb_ref, gm_ref, buf):
    chunk = x_ref.shape[1]
    per = buf.shape[0] // chunk
    c1 = ga_ref.shape[1]
    for v in range(buf.shape[1] // 128):
        for r in range(per):
            buf[r * chunk : (r + 1) * chunk, v * 128 : (v + 1) * 128] = x_ref[v * per + r].astype(F32) * factor
    for t in range(27):
        ga_ref[t] = buf[:c1, t * c1 : (t + 1) * c1]
        gb_ref[t] = buf[c1:, t * c1 : (t + 1) * c1].T
    gm_ref[...] = buf[c1:, 27 * c1 : 28 * c1].T


def call(kernel, outs, *args, scratch=(), smem=0, near=(), far=(), name=None):
    args = list(args)
    specs = []
    for place in range(len(args)):
        if place < smem:
            specs.append(pl.BlockSpec(memory_space=pltpu.SMEM))
        elif place in far:
            specs.append(pl.BlockSpec(memory_space=pl.ANY))
            args[place] = pltpu.with_memory_space_constraint(args[place], pltpu.HBM)
        else:
            specs.append(pl.BlockSpec(memory_space=pltpu.VMEM))
            if place in near:
                args[place] = pltpu.with_memory_space_constraint(args[place], pltpu.VMEM)
    return pl.pallas_call(
        kernel,
        out_shape=outs,
        in_specs=specs,
        out_specs=tuple(pl.BlockSpec(memory_space=pltpu.VMEM) for _ in outs),
        scratch_shapes=list(scratch),
        compiler_params=pltpu.CompilerParams(vmem_limit_bytes=32 * 1024 * 1024),
        name=name,
    )(*args)


def shape(dims, dtype=BF):
    return jax.ShapeDtypeStruct(tuple(dims), dtype)


AXES = ("phi", "eta")


def moves(n_phi, n_eta, rule):
    found = []
    for p in range(n_phi):
        for s in range(n_eta):
            step, t = rule(p, s)
            if 0 <= t < n_eta:
                found.append((p * n_eta + s, (p + step) % n_phi * n_eta + t))
    return found


def gather_pair(own, sent, near, far):
    n_phi = lax.axis_size("phi")
    send = lambda value, rule: lax.ppermute(value, AXES, moves(n_phi, 2, rule))
    return [
        own,
        send(sent, lambda p, s: (0, 1 - s)),
        send(near, lambda p, s: (1 - 2 * s, s)),
        send(far, lambda p, s: (2 * s - 1, 1 - s)),
    ]


def gather_window(own, low, high):
    n_phi = lax.axis_size("phi")
    n_eta = lax.axis_size("eta")
    pieces = []
    for step in window_steps(n_eta):
        send = lambda value, move: lax.ppermute(value, AXES, moves(n_phi, n_eta, lambda p, s: (move, s - step)))
        pieces.append(own if step == 0 else send(own, 0))
        pieces.append(send(high, 1))
        pieces.append(send(low, -1))
    return pieces


def window_steps(n_eta):
    return [0] if n_eta == 1 else [0, -1, 1, -2, 2]


def window_meta(n_eta, cells):
    e = lax.axis_index("eta")
    steps = window_steps(n_eta)
    middle = len(steps) // 2
    values = [middle + step for step in steps]
    values += [jnp.maximum(0, middle - e) * cells, jnp.minimum(len(steps), n_eta + middle - e) * cells]
    return jnp.stack([jnp.asarray(v, jnp.int32) for v in values])


def shards(features, cotangent, kernel_a, kernel_b, mixing):
    c1, n_rows, cells = features.shape
    c2 = kernel_b.shape[1]
    nb = n_rows // PB
    width = PB * c1
    n_eta = lax.axis_size("eta")
    paired = n_eta == 2 and nb % 4 == 0
    block = (cells, width)
    f_own, f_first, f_second, c_own, c_first, c_second, *c_sent = call(
        functools.partial(pre_kernel, paired),
        tuple(shape((n,) + block) for n in (nb, 2, 2, nb, 1, 1) + ((nb // 2 + 1,) if paired else ())),
        features,
        cotangent,
        scratch=(
            pltpu.VMEM(features.shape, BF),
            pltpu.VMEM(features.shape, BF),
            pltpu.SemaphoreType.DMA((2,)),
        ),
        far=(0, 1),
        name="pre",
    )
    if paired:
        f_pieces = gather_pair(f_own, f_own, f_first, f_second)
        c_pieces = gather_pair(c_own, c_sent[0], c_first, c_second)
        meta = []
        nbx = nb // 2 + 4
        rows = 2 * cells
    else:
        f_pieces = gather_window(f_own, f_first, f_second)
        c_pieces = gather_window(c_own, c_first, c_second)
        meta = [window_meta(n_eta, cells)]
        nbx = nb + 4
        rows = len(window_steps(n_eta)) * cells
    wa, waf, wb, wbf, mp, mt, pool, up = call(
        weights_kernel,
        (
            pltpu.VMEM((3 * 2 * width, 3 * width), BF),
            pltpu.VMEM((3 * 2 * width, 3 * width), BF),
            pltpu.VMEM((3 * 2 * width, 3 * PB * c2), BF),
            pltpu.VMEM((3 * 6 * c2, 3 * width), BF),
            pltpu.VMEM((PB * c2, width), BF),
            pltpu.VMEM((width, PB * c2), BF),
            pltpu.VMEM((4 * width, width), BF),
            pltpu.VMEM((width, 2 * width), BF),
        ),
        kernel_a,
        jnp.swapaxes(kernel_b, 1, 2),
        mixing,
        scratch=(
            pltpu.VMEM((27 * c1, width), F32),
            pltpu.VMEM((27 * c1, width), F32),
            pltpu.VMEM((27 * c1, PB * c2), F32),
            pltpu.VMEM((27 * c2, width), F32),
            pltpu.VMEM(kernel_a.shape, BF),
            pltpu.VMEM((27, c1, c2), BF),
            pltpu.VMEM(mixing.shape, BF),
            pltpu.SemaphoreType.DMA((3,)),
        ),
        far=(0, 1, 2),
        name="weights",
    )
    nc = nbx // 2 - 1
    rows_c = rows // 2
    devices = lax.axis_size("phi") * n_eta
    lanes = 28 * c1
    total_rows = (c1 + c2) * lanes // 128
    chunk = next(d for d in range(8, c1 + c2 + 1, 8) if (c1 + c2) % d == 0 and total_rows <= d * devices)
    tall = rows + 2 * LAYERS
    tall_c = rows_c + 2 * LAYERS
    skip = len(meta)
    count = len(f_pieces)
    matrices = (wa, wb, mp, pool)
    fz, hid, slope, cz, gat, slope_b, proj = call(
        functools.partial(forward_kernel, paired, count),
        (
            pltpu.VMEM((nbx, tall, 2 * width), BF),
            pltpu.VMEM((nbx, rows, width), BF),
            pltpu.VMEM((nbx, rows, width), F32),
            pltpu.VMEM((nc + 2, tall_c, 2 * width), BF),
            pltpu.VMEM((nc, rows_c, PB * c2), BF),
            pltpu.VMEM((nc, rows_c, PB * c2), F32),
            pltpu.VMEM((nc, rows_c, width), BF),
        ),
        *meta,
        *f_pieces,
        *matrices,
        smem=skip,
        near=range(skip + 1, skip + count + len(matrices)),
        name="forward",
    )
    inner = (fz, slope, cz, gat, slope_b, wbf, mt, pool, up)
    gz, terms = call(
        functools.partial(backward_kernel, paired, count),
        (pltpu.VMEM((nbx, tall, 2 * width), BF), shape((devices, chunk, 128))),
        *meta,
        *c_pieces,
        *inner,
        scratch=(
            pltpu.VMEM((nbx, rows, width), BF),
            pltpu.VMEM((nc, tall_c, PB * c2 + width), BF),
            pltpu.VMEM((nc, rows_c, width), BF),
            pltpu.VMEM((3 * width, 6 * width), F32),
            pltpu.VMEM((3 * PB * c2, 6 * width), F32),
            pltpu.VMEM((c1 + c2, lanes), F32),
        ),
        smem=skip,
        near=range(skip + 1, skip + count + len(inner)),
        name="backward",
    )
    terms = lax.all_to_all(terms, AXES, 0, 0, tiled=True)
    blocks = 2 * (nbx - 4)
    results = call(
        functools.partial(finish_kernel, paired),
        (shape((blocks, width, cells)),) * (2 if paired else 1),
        *meta,
        gz,
        hid,
        proj,
        waf,
        up,
        scratch=(pltpu.VMEM((blocks, rows if paired else cells, width), F32),),
        smem=skip,
        near=range(skip, skip + 5),
        name="finish",
    )
    if paired:
        kept, sent = results
        received = lax.ppermute(sent, AXES, moves(lax.axis_size("phi"), 2, lambda p, s: (0, 1 - s)))
        terms, received = lax.optimization_barrier((terms, received))
        output, grad_input = call(
            restore_kernel, (shape(features.shape), shape(features.shape)), kept, received, name="restore"
        )
    else:
        output, grad_input = (
            jnp.transpose(part.reshape(n_rows, c1, cells), (1, 0, 2)) for part in (results[0][:nb], results[0][nb:])
        )
    (sums,) = call(sum_kernel, (shape(terms.shape),), terms, name="sum")
    sums = lax.all_to_all(sums, AXES, 0, 0, tiled=True)
    cell_count = n_rows * cells * devices
    grad_a, grad_b, grad_mix = call(
        functools.partial(post_kernel, 1.0 / math.sqrt(cell_count)),
        (shape((27, c1, c1), F32), shape((27, c1, c2), F32), shape((c1, c2), F32)),
        sums,
        scratch=(pltpu.VMEM((c1 + c2, lanes), F32),),
        name="post",
    )
    return output, grad_input, grad_a, jnp.swapaxes(grad_b, 1, 2), grad_mix


def solution(mesh):
    in_specs = (P(None, "phi", "eta"), P(None, "phi", "eta"), P(), P(), P())
    out_specs = (P(None, "phi", "eta"), P(None, "phi", "eta"), P(), P(), P())
    return jax.shard_map(shards, mesh=mesh, in_specs=in_specs, out_specs=out_specs, check_vma=False)
```

```python
import functools
import math

import jax
import jax.numpy as jnp
from jax import lax
from jax.experimental import pallas as pl
from jax.experimental.pallas import tpu as pltpu
from jax.sharding import PartitionSpec as P


LAYERS = 32
PB = 4
BF = jnp.bfloat16
F32 = jnp.float32


def iota(shape, dim):
    return lax.broadcasted_iota(jnp.int32, shape, dim)


def dot(a, b):
    return jnp.dot(a, b, preferred_element_type=F32)


def dot_rows(a, b):
    return lax.dot_general(a, b, (((0,), (0,)), ((), ())), preferred_element_type=F32)


def fetch(sources, places, sems):
    moves = [pltpu.make_async_copy(src, dst, sems.at[i]) for i, (src, dst) in enumerate(zip(sources, places))]
    for move in moves:
        move.start()
    return moves


def pre_kernel(paired, f_hbm, c_hbm, f_own, c_own, first, second, *rest):
    f_ref, c_ref, sems = rest[-3:]
    nb = f_own.shape[0]
    moves = fetch((f_hbm, c_hbm), (f_ref, c_ref), sems)
    for move, ref, own in zip(moves, (f_ref, c_ref), (f_own, c_own)):
        move.wait()
        ch, _, cells = ref.shape
        swapped = jnp.swapaxes(ref[...].astype(F32), 0, 1)
        for j in range(nb):
            own[j] = swapped[PB * j : PB * (j + 1)].reshape(PB * ch, cells).T.astype(BF)
    e = lax.axis_index("eta") if paired else 1
    for rim, low in ((first, e), (second, 1 - e)):
        for j in range(2):
            rim[j] = f_own[(nb - 2) * (1 - low) + j]
        rim[2] = c_own[(nb - 1) * (1 - low)]
    if paired:
        partner = rest[0]
        for j in range(partner.shape[0]):
            partner[j] = c_own[(1 - e) * (nb // 2 - 1) + j]


def copies(size, times):
    shape = (size, size * times)
    return jnp.where(iota(shape, 0) == iota(shape, 1) % size, 1.0, 0.0).astype(BF)


def weights_kernel(
    ka_hbm, kbt_hbm, mix_hbm, wa, waf, wb, wbf, mp, mt, pool, up, ta, taf, tb, tbf, ka, kbt, mix, sems
):
    for move in fetch((ka_hbm, kbt_hbm, mix_hbm), (ka, kbt, mix), sems):
        move.wait()
    c1 = ka.shape[1]
    c2 = kbt.shape[2]
    width = PB * c1
    wide = PB * c2

    def flat(block):
        return block.reshape(-1, block.shape[2])

    def turned(ref):
        return jnp.swapaxes(ref[...].astype(F32), 1, 2).astype(BF)

    few = copies(c1, PB)
    many = copies(c2, PB)
    ta[...] = dot(flat(turned(ka)), few)
    taf[...] = dot(flat(ka[...]), few)
    tb[...] = dot(flat(kbt[...]), many)
    tbf[...] = dot(flat(turned(kbt)), few)

    def toeplitz(out, source, order, rows_per, cols_per, row_blocks):
        height = len(row_blocks) * rows_per
        across = PB * cols_per
        place = iota((rows_per, across), 1) // cols_per
        for b in range(3):
            for c in range(3):
                for at, q in enumerate(row_blocks):
                    value = jnp.zeros((rows_per, across), F32)
                    for a in range(3):
                        if 0 <= q + 1 - a < PB:
                            t = order(9 * a + 3 * b + c) * rows_per
                            value = jnp.where(place == q + 1 - a, source[t : t + rows_per], value)
                    first = b * height + at * rows_per
                    out[first : first + rows_per, c * across : (c + 1) * across] = value.astype(BF)

    ring = (0, 1, 2, 3, 4, 100, 100, -1)
    toeplitz(wa, ta, lambda t: t, c1, c1, ring)
    toeplitz(wb, tb, lambda t: t, c1, c2, ring)
    toeplitz(wbf, tbf, lambda t: 26 - t, c2, c1, (0, 1, 2, 3, 4, -1))
    toeplitz(waf, taf, lambda t: 26 - t, c1, c1, ring)
    mixing = mix[...]
    spread = dot(mixing, many)
    spread_t = dot(mixing.astype(F32).T.astype(BF), few)
    for p in range(PB):
        inside = iota((c1, wide), 1) // c2 == p
        mt[p * c1 : (p + 1) * c1] = jnp.where(inside, spread, 0.0).astype(BF)
        inside = iota((c2, width), 1) // c1 == p
        mp[p * c2 : (p + 1) * c2] = jnp.where(inside, spread_t, 0.0).astype(BF)
    r = iota(pool.shape, 0)
    l = iota(pool.shape, 1)
    hit = (r % c1 == l % c1) & (r // (2 * width) * 2 + r % width // c1 // 2 == l // c1)
    pool[...] = jnp.where(hit, 1.0, 0.0).astype(BF)
    r = iota(up.shape, 0)
    l = iota(up.shape, 1)
    hit = (r % c1 == l % c1) & (l // width * 2 + l % width // c1 // 2 == r // c1)
    up[...] = jnp.where(hit, 1.0, 0.0).astype(BF)


def combine(summed, width):
    rows = summed.shape[0]
    layer = iota((rows, width), 0) % LAYERS
    below = pltpu.roll(summed[:, :width], 1, 0)
    above = pltpu.roll(summed[:, 2 * width :], rows - 1, 0)
    return (
        summed[:, width : 2 * width]
        + jnp.where(layer == 0, 0.0, below)
        + jnp.where(layer == LAYERS - 1, 0.0, above)
    )


def layer_shifts(block):
    rows, width = block.shape
    layer = iota((rows, width), 0) % LAYERS
    wide = block.astype(F32)
    first = jnp.where(layer == LAYERS - 1, 0.0, pltpu.roll(wide, rows - 1, 0))
    last = jnp.where(layer == 0, 0.0, pltpu.roll(wide, 1, 0))
    return jnp.concatenate([first.astype(BF), block, last.astype(BF)], axis=1)


def taps(ref, j, start, rows):
    parts = []
    for b in range(3):
        at = start + b * LAYERS
        if not isinstance(at, int):
            at = pl.multiple_of(at, LAYERS)
        parts.append(ref[j, pl.ds(at, rows), :])
    return jnp.concatenate(parts, axis=1)


def every_other(block, which):
    count = block.shape[0] // (2 * LAYERS)
    return [block[(2 * i + which) * LAYERS : (2 * i + which + 1) * LAYERS] for i in range(count)]


def paired_rows(first, second):
    parts = []
    for block in (first, second):
        for which in range(2):
            parts.append(jnp.concatenate(every_other(block, which), axis=0))
    return jnp.concatenate(parts, axis=1)


def widen_rows(block):
    parts = []
    for i in range(block.shape[0] // LAYERS):
        part = block[i * LAYERS : (i + 1) * LAYERS]
        parts += [part, part]
    return jnp.concatenate(parts, axis=0)


def sigmoid(v):
    return 1.0 / (1.0 + jnp.exp(-v))


def edges(ref, first, last, inner, width, split):
    lane = iota((inner, width), 1)
    at = slice(LAYERS, LAYERS + inner)
    main = ref.shape[2] - width
    for j in range(first, last):
        nxt = ref[j + 1, at, :width] if j + 1 < ref.shape[0] else jnp.zeros((inner, width), BF)
        prv = ref[j - 1, at, main - width : main] if j > 0 else jnp.zeros((inner, width), BF)
        ref[j, at, main:] = jnp.where(lane < split, nxt, prv)


def blank_rims(ref):
    pad = jnp.zeros((LAYERS, ref.shape[2]), BF)
    for j in range(ref.shape[0]):
        ref[j, :LAYERS, :] = pad
        ref[j, ref.shape[1] - LAYERS :, :] = pad


def keep_inside(meta, shards_seen, value, scale):
    if meta is None or shards_seen == 1:
        return value
    r = iota(value.shape, 0)
    inside = (r >= meta[shards_seen] // scale) & (r < meta[shards_seen + 1] // scale)
    return jnp.where(inside, value, jnp.zeros_like(value))


def forward_kernel(paired, count, *refs):
    meta = None
    if not paired:
        meta, refs = refs[0], refs[1:]
    pieces, refs = refs[:count], refs[count:]
    wa, wb, mp, pool = refs[:4]
    fz, hid, slope, cz, gat, slope_b, proj = refs[4:]
    nbx = fz.shape[0]
    nc = gat.shape[0]
    rows = hid.shape[1]
    rows_c = rows // 2
    width = hid.shape[2]
    c1 = width // PB
    wide = gat.shape[2]
    blank_rims(fz)
    blank_rims(cz)
    cells = pieces[0].shape[1]
    if paired:
        own, partner, near, far = pieces
        nb = own.shape[0]
        e = lax.axis_index("eta")
        for chunk, rim, shard in ((own, near, e), (partner, far, 1 - e)):
            at = pl.multiple_of(LAYERS + shard * cells, LAYERS)
            for j in range(nb // 2 + 2):
                fz[j + 2 * (1 - e), pl.ds(at, cells), :width] = chunk[j + e * (nb // 2 - 2)]
            for j in range(2):
                fz[e * (nbx - 2) + j, pl.ds(at, cells), :width] = rim[j]
    else:
        for s in range(count // 3):
            middle, before, after = pieces[3 * s : 3 * s + 3]
            at = pl.multiple_of(LAYERS + meta[s] * cells, LAYERS)
            for j in range(2):
                fz[j, pl.ds(at, cells), :width] = before[j]
                fz[nbx - 2 + j, pl.ds(at, cells), :width] = after[j]
            for j in range(nbx - 4):
                fz[2 + j, pl.ds(at, cells), :width] = middle[j]
    edges(fz, 0, nbx, rows, width, 3 * c1)
    for j in range(nbx):
        linear = combine(dot(taps(fz, j, 0, rows), wa[...]), width)
        logistic = sigmoid(linear)
        hid[j] = (linear * logistic).astype(BF)
        slope[j] = logistic * (1.0 + linear * (1.0 - logistic))
    for j in range(nc + 2):
        first, second = max(2 * j - 1, 0), min(2 * j, nbx - 1)
        pooled = dot(paired_rows(hid[first], hid[second]), pool[...]) * 0.25
        cz[j, LAYERS : LAYERS + rows_c, :width] = keep_inside(meta, count // 3, pooled.astype(BF), 2)
    edges(cz, 1, nc + 1, rows_c, width, 3 * c1)
    for j in range(nc):
        linear = combine(dot(taps(cz, j + 1, 0, rows_c), wb[...]), wide)
        logistic = sigmoid(linear)
        gated = (linear * logistic).astype(BF)
        gat[j] = gated
        slope_b[j] = logistic * (1.0 + linear * (1.0 - logistic))
        proj[j] = dot(gated, mp[...]).astype(BF)


def backward_kernel(paired, count, *refs):
    meta = None
    if not paired:
        meta, refs = refs[0], refs[1:]
    pieces, refs = refs[:count], refs[count:]
    fz, slope, cz, gat, slope_b, wbf, mt, pool, up = refs[:9]
    gz, pk_ref = refs[9:11]
    cot, gb, fold, acc_a, acc_b, packed = refs[11:]
    nbx = fz.shape[0]
    nb = nbx - 4
    nc = gat.shape[0]
    rows = cot.shape[1]
    rows_c = rows // 2
    width = cot.shape[2]
    wide = gat.shape[2]
    c1 = width // PB
    c2 = wide // PB
    cells = pieces[0].shape[1]
    blank_rims(gz)
    blank_rims(gb)
    if paired:
        own, partner, near, far = pieces
        e = lax.axis_index("eta")
        for rim, shard in ((near, e), (far, 1 - e)):
            at = pl.multiple_of(shard * cells, cells)
            cot[1 + e * (nbx - 3), pl.ds(at, cells), :] = rim[2]
            for j in range(partner.shape[0]):
                if rim is near:
                    block = own[j + e * (own.shape[0] // 2 - 1)]
                else:
                    block = partner[j]
                cot[j + 2 - e, pl.ds(at, cells), :] = block
        own, own_at, own_at_c = rows, 0, 0
    else:
        for s in range(count // 3):
            middle, before, after = pieces[3 * s : 3 * s + 3]
            at = pl.multiple_of(meta[s] * cells, cells)
            cot[1, pl.ds(at, cells), :] = before[2]
            cot[nbx - 2, pl.ds(at, cells), :] = after[2]
            for j in range(nb):
                cot[2 + j, pl.ds(at, cells), :] = middle[j]
        own = cells
        own_at = pl.multiple_of(meta[0] * own, own)
        own_at_c = pl.multiple_of(meta[0] * (own // 2), own // 2)
    own_c = own // 2

    for j in range(nc):
        fold[j] = dot(paired_rows(cot[2 * j + 1], cot[2 * j + 2]), pool[...]).astype(BF)
        grad = dot(fold[j], mt[...]) * slope_b[j]
        gb[j, LAYERS : LAYERS + rows_c, :wide] = keep_inside(meta, count // 3, grad.astype(BF), 2)
    edges(gb, 0, nc, rows_c, width, c2)
    for j in range(nc):
        grad = combine(dot(taps(gb, j, 0, rows_c), wbf[...]), width).astype(BF)
        spread = 0.25 * dot(grad, up[...])
        for k in range(2):
            f = 2 * j + 1 + k
            total = cot[f].astype(F32) + widen_rows(spread[:, k * width : (k + 1) * width])
            value = (total * slope[f]).astype(BF)
            gz[f, LAYERS : LAYERS + rows, :width] = keep_inside(meta, count // 3, value, 1)
    edges(gz, 2, nbx - 2, rows, width, 3 * c1)

    def own_half(value, j):
        p = iota(value.shape, 1) // (value.shape[1] // PB)
        if j == 0:
            value = jnp.where(p >= PB // 2, value, jnp.zeros_like(value))
        if j == nc - 1:
            value = jnp.where(p < PB // 2, value, jnp.zeros_like(value))
        return value

    lhs = jnp.concatenate(
        [layer_shifts(gz[2 + j, pl.ds(LAYERS + own_at, own), :width]) for j in range(nb)], axis=0
    )
    rhs = jnp.concatenate([taps(fz, 2 + j, own_at, own) for j in range(nb)], axis=0)
    acc_a[...] = dot_rows(lhs, rhs)
    lhs = jnp.concatenate(
        [layer_shifts(own_half(gb[j, pl.ds(LAYERS + own_at_c, own_c), :wide], j)) for j in range(nc)], axis=0
    )
    rhs = jnp.concatenate([taps(cz, j + 1, own_at_c, own_c) for j in range(nc)], axis=0)
    acc_b[...] = dot_rows(lhs, rhs)
    lhs = jnp.concatenate([gat[j, pl.ds(own_at_c, own_c), :] for j in range(nc)], axis=0)
    rhs = jnp.concatenate([own_half(fold[j, pl.ds(own_at_c, own_c), :], j) for j in range(nc)], axis=0)
    mixed = dot_rows(lhs, rhs)
    mix_sum = mixed[:c2, :c1]
    for p in range(1, PB):
        mix_sum = mix_sum + mixed[p * c2 : (p + 1) * c2, p * c1 : (p + 1) * c1]
    packed[c1:, 27 * c1 : 28 * c1] = mix_sum
    packed[:c1, 27 * c1 : 28 * c1] = jnp.zeros((c1, c1), F32)
    span = 2 * width
    for acc, outs, first in ((acc_a, c1, 0), (acc_b, c2, c1)):
        for b in range(3):
            for c in range(3):
                total = None
                for p in range(PB):
                    at = (c * PB + p) * outs
                    part = acc[at : at + outs, b * span : (b + 1) * span]
                    part = pltpu.roll(part, (span - (p - 1) * c1) % span, 1)
                    total = part if total is None else total + part
                for a in range(3):
                    t = 9 * a + 3 * b + c
                    packed[first : first + outs, t * c1 : (t + 1) * c1] = total[:, a * c1 : (a + 1) * c1]
    chunk = pk_ref.shape[1]
    per = packed.shape[0] // chunk
    used = packed.shape[1] // 128 * per
    for v in range(packed.shape[1] // 128):
        for r in range(per):
            pk_ref[v * per + r] = packed[r * chunk : (r + 1) * chunk, v * 128 : (v + 1) * 128].astype(BF)
    for v in range(used, pk_ref.shape[0]):
        pk_ref[v] = jnp.zeros(pk_ref.shape[1:], BF)


def finish_kernel(paired, *refs):
    meta = None
    if not paired:
        meta, refs = refs[0], refs[1:]
    gz, hid, proj, waf, up = refs[:5]
    outs = refs[5:-1]
    buf = refs[-1]
    nb = gz.shape[0] - 4
    width = hid.shape[2]
    cells = outs[0].shape[2]
    if paired:
        own, own_at, own_at_c = hid.shape[1], 0, 0
        e = lax.axis_index("eta")
        starts = [pl.multiple_of(e * cells, cells), pl.multiple_of((1 - e) * cells, cells)]
    else:
        own = cells
        own_at = pl.multiple_of(meta[0] * own, own)
        own_at_c = pl.multiple_of(meta[0] * (own // 2), own // 2)
        starts = [0]

    def write(value, place):
        buf[place] = value
        for out, start in zip(outs, starts):
            out[place] = buf[place, pl.ds(start, cells), :].T.astype(BF)

    for j in range(nb):
        grad = combine(dot(taps(gz, 2 + j, own_at, own), waf[...]), width)
        write(grad, nb + j)
    for j in range(nb):
        k = (j + 1) % 2
        spread = dot(proj[(j + 1) // 2, pl.ds(own_at_c, own // 2), :], up[:, k * width : (k + 1) * width])
        write(hid[2 + j, pl.ds(own_at, own), :].astype(F32) + widen_rows(spread), j)


def restore_kernel(kept, received, out_ref, gin_ref):
    ch, rows, cells = out_ref.shape
    half = rows // 2
    e = lax.axis_index("eta")
    for k, ref in enumerate((out_ref, gin_ref)):
        at = k * half // PB
        mine = kept[at : at + half // PB].astype(F32)
        other = received[at : at + half // PB].astype(F32)
        first = jnp.where(e == 0, mine, other).reshape(half, ch, cells)
        second = jnp.where(e == 0, other, mine).reshape(half, ch, cells)
        ref[...] = jnp.swapaxes(jnp.concatenate([first, second], axis=0), 0, 1).astype(BF)


def sum_kernel(x_ref, o_ref):
    total = jnp.sum(x_ref[...].astype(F32), axis=0).astype(BF)
    o_ref[...] = jnp.broadcast_to(total[None], o_ref.shape)


def post_kernel(factor, x_ref, ga_ref, gb_ref, gm_ref, buf):
    chunk = x_ref.shape[1]
    per = buf.shape[0] // chunk
    c1 = ga_ref.shape[1]
    for v in range(buf.shape[1] // 128):
        for r in range(per):
            buf[r * chunk : (r + 1) * chunk, v * 128 : (v + 1) * 128] = x_ref[v * per + r].astype(F32) * factor
    for t in range(27):
        ga_ref[t] = buf[:c1, t * c1 : (t + 1) * c1]
        gb_ref[t] = buf[c1:, t * c1 : (t + 1) * c1].T
    gm_ref[...] = buf[c1:, 27 * c1 : 28 * c1].T


def call(kernel, outs, *args, scratch=(), smem=0, near=(), far=()):
    args = list(args)
    specs = []
    for place in range(len(args)):
        if place < smem:
            specs.append(pl.BlockSpec(memory_space=pltpu.SMEM))
        elif place in far:
            specs.append(pl.BlockSpec(memory_space=pl.ANY))
            args[place] = pltpu.with_memory_space_constraint(args[place], pltpu.HBM)
        else:
            specs.append(pl.BlockSpec(memory_space=pltpu.VMEM))
            if place in near:
                args[place] = pltpu.with_memory_space_constraint(args[place], pltpu.VMEM)
    return pl.pallas_call(
        kernel,
        out_shape=outs,
        in_specs=specs,
        out_specs=tuple(pl.BlockSpec(memory_space=pltpu.VMEM) for _ in outs),
        scratch_shapes=list(scratch),
        compiler_params=pltpu.CompilerParams(vmem_limit_bytes=32 * 1024 * 1024),
    )(*args)


def shape(dims, dtype=BF):
    return jax.ShapeDtypeStruct(tuple(dims), dtype)


AXES = ("phi", "eta")


def moves(n_phi, n_eta, rule):
    found = []
    for p in range(n_phi):
        for s in range(n_eta):
            step, t = rule(p, s)
            if 0 <= t < n_eta:
                found.append((p * n_eta + s, (p + step) % n_phi * n_eta + t))
    return found


def gather_pair(f_own, c_own, c_sent, near, far):
    n_phi = lax.axis_size("phi")

    def send(value, rule):
        return lax.ppermute(value, AXES, moves(n_phi, 2, rule))

    far = send(far, lambda p, s: (2 * s - 1, 1 - s))
    near = send(near, lambda p, s: (1 - 2 * s, s))
    f_other = send(f_own, lambda p, s: (0, 1 - s))
    c_other = send(c_sent, lambda p, s: (0, 1 - s))
    return [f_own, f_other, near, far], [c_own, c_other, near, far]


def gather_window(f_own, c_own, low, high):
    n_phi = lax.axis_size("phi")
    n_eta = lax.axis_size("eta")
    f_pieces = []
    c_pieces = []
    for step in window_steps(n_eta):
        send = lambda value, move: lax.ppermute(value, AXES, moves(n_phi, n_eta, lambda p, s: (move, s - step)))
        rims = [send(high, 1), send(low, -1)]
        f_pieces += [f_own if step == 0 else send(f_own, 0)] + rims
        c_pieces += [c_own if step == 0 else send(c_own, 0)] + rims
    return f_pieces, c_pieces


def window_steps(n_eta):
    return [0] if n_eta == 1 else [0, -1, 1, -2, 2]


def window_meta(n_eta, cells):
    e = lax.axis_index("eta")
    steps = window_steps(n_eta)
    middle = len(steps) // 2
    values = [middle + step for step in steps]
    values += [jnp.maximum(0, middle - e) * cells, jnp.minimum(len(steps), n_eta + middle - e) * cells]
    return jnp.stack([jnp.asarray(v, jnp.int32) for v in values])


def shards(features, cotangent, kernel_a, kernel_b, mixing):
    c1, n_rows, cells = features.shape
    c2 = kernel_b.shape[1]
    nb = n_rows // PB
    width = PB * c1
    n_eta = lax.axis_size("eta")
    paired = n_eta == 2 and nb % 4 == 0
    block = (cells, width)
    f_own, c_own, first, second, *c_sent = call(
        functools.partial(pre_kernel, paired),
        tuple(shape((n,) + block) for n in (nb, nb, 3, 3) + ((nb // 2 + 1,) if paired else ())),
        features,
        cotangent,
        scratch=(
            pltpu.VMEM(features.shape, BF),
            pltpu.VMEM(features.shape, BF),
            pltpu.SemaphoreType.DMA((2,)),
        ),
        far=(0, 1),
    )
    if paired:
        f_pieces, c_pieces = gather_pair(f_own, c_own, c_sent[0], first, second)
        meta = []
        nbx = nb // 2 + 4
        rows = 2 * cells
    else:
        f_pieces, c_pieces = gather_window(f_own, c_own, first, second)
        meta = [window_meta(n_eta, cells)]
        nbx = nb + 4
        rows = len(window_steps(n_eta)) * cells
    wa, waf, wb, wbf, mp, mt, pool, up = call(
        weights_kernel,
        (
            pltpu.VMEM((3 * 2 * width, 3 * width), BF),
            pltpu.VMEM((3 * 2 * width, 3 * width), BF),
            pltpu.VMEM((3 * 2 * width, 3 * PB * c2), BF),
            pltpu.VMEM((3 * 6 * c2, 3 * width), BF),
            pltpu.VMEM((PB * c2, width), BF),
            pltpu.VMEM((width, PB * c2), BF),
            pltpu.VMEM((4 * width, width), BF),
            pltpu.VMEM((width, 2 * width), BF),
        ),
        kernel_a,
        jnp.swapaxes(kernel_b, 1, 2),
        mixing,
        scratch=(
            pltpu.VMEM((27 * c1, width), F32),
            pltpu.VMEM((27 * c1, width), F32),
            pltpu.VMEM((27 * c1, PB * c2), F32),
            pltpu.VMEM((27 * c2, width), F32),
            pltpu.VMEM(kernel_a.shape, BF),
            pltpu.VMEM((27, c1, c2), BF),
            pltpu.VMEM(mixing.shape, BF),
            pltpu.SemaphoreType.DMA((3,)),
        ),
        far=(0, 1, 2),
    )
    nc = nbx // 2 - 1
    rows_c = rows // 2
    devices = lax.axis_size("phi") * n_eta
    lanes = 28 * c1
    total_rows = (c1 + c2) * lanes // 128
    chunk = next(d for d in range(8, c1 + c2 + 1, 8) if (c1 + c2) % d == 0 and total_rows <= d * devices)
    tall = rows + 2 * LAYERS
    tall_c = rows_c + 2 * LAYERS
    skip = len(meta)
    count = len(f_pieces)
    matrices = (wa, wb, mp, pool)
    fz, hid, slope, cz, gat, slope_b, proj = call(
        functools.partial(forward_kernel, paired, count),
        (
            pltpu.VMEM((nbx, tall, 2 * width), BF),
            pltpu.VMEM((nbx, rows, width), BF),
            pltpu.VMEM((nbx, rows, width), F32),
            pltpu.VMEM((nc + 2, tall_c, 2 * width), BF),
            pltpu.VMEM((nc, rows_c, PB * c2), BF),
            pltpu.VMEM((nc, rows_c, PB * c2), F32),
            pltpu.VMEM((nc, rows_c, width), BF),
        ),
        *meta,
        *f_pieces,
        *matrices,
        smem=skip,
        near=range(skip + 1, skip + count + len(matrices)),
    )
    inner = (fz, slope, cz, gat, slope_b, wbf, mt, pool, up)
    gz, terms = call(
        functools.partial(backward_kernel, paired, count),
        (pltpu.VMEM((nbx, tall, 2 * width), BF), shape((devices, chunk, 128))),
        *meta,
        *c_pieces,
        *inner,
        scratch=(
            pltpu.VMEM((nbx, rows, width), BF),
            pltpu.VMEM((nc, tall_c, PB * c2 + width), BF),
            pltpu.VMEM((nc, rows_c, width), BF),
            pltpu.VMEM((3 * width, 6 * width), F32),
            pltpu.VMEM((3 * PB * c2, 6 * width), F32),
            pltpu.VMEM((c1 + c2, lanes), F32),
        ),
        smem=skip,
        near=range(skip + 1, skip + count + len(inner)),
    )
    terms = lax.all_to_all(terms, AXES, 0, 0, tiled=True)
    blocks = 2 * (nbx - 4)
    results = call(
        functools.partial(finish_kernel, paired),
        (shape((blocks, width, cells)),) * (2 if paired else 1),
        *meta,
        gz,
        hid,
        proj,
        waf,
        up,
        scratch=(pltpu.VMEM((blocks, rows if paired else cells, width), F32),),
        smem=skip,
        near=range(skip, skip + 5),
    )
    if paired:
        kept, sent = results
        received = lax.ppermute(sent, AXES, moves(lax.axis_size("phi"), 2, lambda p, s: (0, 1 - s)))
        terms, kept = lax.optimization_barrier((terms, kept))
        output, grad_input = call(restore_kernel, (shape(features.shape), shape(features.shape)), kept, received)
    else:
        output, grad_input = (
            jnp.transpose(part.reshape(n_rows, c1, cells), (1, 0, 2)) for part in (results[0][:nb], results[0][nb:])
        )
    (sums,) = call(sum_kernel, (shape(terms.shape),), terms)
    sums = lax.all_to_all(sums, AXES, 0, 0, tiled=True)
    cell_count = n_rows * cells * devices
    grad_a, grad_b, grad_mix = call(
        functools.partial(post_kernel, 1.0 / math.sqrt(cell_count)),
        (shape((27, c1, c1), F32), shape((27, c1, c2), F32), shape((c1, c2), F32)),
        sums,
        scratch=(pltpu.VMEM((c1 + c2, lanes), F32),),
    )
    return output, grad_input, grad_a, jnp.swapaxes(grad_b, 1, 2), grad_mix


def solution(mesh):
    in_specs = (P(None, "phi", "eta"), P(None, "phi", "eta"), P(), P(), P())
    out_specs = (P(None, "phi", "eta"), P(None, "phi", "eta"), P(), P(), P())

    return jax.shard_map(shards, mesh=mesh, in_specs=in_specs, out_specs=out_specs, check_vma=False)
```

```python
import functools
import math

import jax
import jax.numpy as jnp
from jax import lax
from jax.experimental import pallas as pl
from jax.experimental.pallas import tpu as pltpu
from jax.sharding import PartitionSpec as P


LAYERS = 32
PB = 4
BF = jnp.bfloat16
F32 = jnp.float32


def iota(shape, dim):
    return lax.broadcasted_iota(jnp.int32, shape, dim)


def dot(a, b):
    return jnp.dot(a, b, preferred_element_type=F32)


def dot_rows(a, b):
    return lax.dot_general(a, b, (((0,), (0,)), ((), ())), preferred_element_type=F32)


def fetch(sources, places, sems):
    moves = [pltpu.make_async_copy(src, dst, sems.at[i]) for i, (src, dst) in enumerate(zip(sources, places))]
    for move in moves:
        move.start()
    return moves


def pre_kernel(paired, f_hbm, c_hbm, f_own, c_own, first, second, *rest):
    f_ref, c_ref, sems = rest[-3:]
    nb = f_own.shape[0]
    moves = fetch((f_hbm, c_hbm), (f_ref, c_ref), sems)
    for move, ref, own in zip(moves, (f_ref, c_ref), (f_own, c_own)):
        move.wait()
        ch, _, cells = ref.shape
        swapped = jnp.swapaxes(ref[...].astype(F32), 0, 1)
        for j in range(nb):
            own[j] = swapped[PB * j : PB * (j + 1)].reshape(PB * ch, cells).T.astype(BF)
    e = lax.axis_index("eta") if paired else 1
    for rim, low in ((first, e), (second, 1 - e)):
        for j in range(2):
            rim[j] = f_own[(nb - 2) * (1 - low) + j]
        rim[2] = c_own[(nb - 1) * (1 - low)]
    if paired:
        partner = rest[0]
        for j in range(partner.shape[0]):
            partner[j] = c_own[(1 - e) * (nb // 2 - 1) + j]


def copies(size, times):
    shape = (size, size * times)
    return jnp.where(iota(shape, 0) == iota(shape, 1) % size, 1.0, 0.0).astype(BF)


def weights_kernel(
    ka_hbm, kbt_hbm, mix_hbm, wa, waf, wb, wbf, mp, mt, pool, up, ta, taf, tb, tbf, ka, kbt, mix, sems
):
    for move in fetch((ka_hbm, kbt_hbm, mix_hbm), (ka, kbt, mix), sems):
        move.wait()
    c1 = ka.shape[1]
    c2 = kbt.shape[2]
    width = PB * c1
    wide = PB * c2

    def flat(block):
        return block.reshape(-1, block.shape[2])

    def turned(ref):
        return jnp.swapaxes(ref[...].astype(F32), 1, 2).astype(BF)

    few = copies(c1, PB)
    many = copies(c2, PB)
    ta[...] = dot(flat(turned(ka)), few)
    taf[...] = dot(flat(ka[...]), few)
    tb[...] = dot(flat(kbt[...]), many)
    tbf[...] = dot(flat(turned(kbt)), few)

    def toeplitz(out, source, order, rows_per, cols_per, row_blocks):
        height = len(row_blocks) * rows_per
        across = PB * cols_per
        place = iota((rows_per, across), 1) // cols_per
        for b in range(3):
            for c in range(3):
                for at, q in enumerate(row_blocks):
                    value = jnp.zeros((rows_per, across), F32)
                    for a in range(3):
                        if 0 <= q + 1 - a < PB:
                            t = order(9 * a + 3 * b + c) * rows_per
                            value = jnp.where(place == q + 1 - a, source[t : t + rows_per], value)
                    first = b * height + at * rows_per
                    out[first : first + rows_per, c * across : (c + 1) * across] = value.astype(BF)

    ring = (0, 1, 2, 3, 4, 100, 100, -1)
    toeplitz(wa, ta, lambda t: t, c1, c1, ring)
    toeplitz(wb, tb, lambda t: t, c1, c2, ring)
    toeplitz(wbf, tbf, lambda t: 26 - t, c2, c1, (0, 1, 2, 3, 4, -1))
    toeplitz(waf, taf, lambda t: 26 - t, c1, c1, ring)
    mixing = mix[...]
    spread = dot(mixing, many)
    spread_t = dot(mixing.astype(F32).T.astype(BF), few)
    for p in range(PB):
        inside = iota((c1, wide), 1) // c2 == p
        mt[p * c1 : (p + 1) * c1] = jnp.where(inside, spread, 0.0).astype(BF)
        inside = iota((c2, width), 1) // c1 == p
        mp[p * c2 : (p + 1) * c2] = jnp.where(inside, spread_t, 0.0).astype(BF)
    r = iota(pool.shape, 0)
    l = iota(pool.shape, 1)
    hit = (r % c1 == l % c1) & (r // (2 * width) * 2 + r % width // c1 // 2 == l // c1)
    pool[...] = jnp.where(hit, 1.0, 0.0).astype(BF)
    r = iota(up.shape, 0)
    l = iota(up.shape, 1)
    hit = (r % c1 == l % c1) & (l // width * 2 + l % width // c1 // 2 == r // c1)
    up[...] = jnp.where(hit, 1.0, 0.0).astype(BF)


def combine(summed, width):
    rows = summed.shape[0]
    layer = iota((rows, width), 0) % LAYERS
    below = pltpu.roll(summed[:, :width], 1, 0)
    above = pltpu.roll(summed[:, 2 * width :], rows - 1, 0)
    return (
        summed[:, width : 2 * width]
        + jnp.where(layer == 0, 0.0, below)
        + jnp.where(layer == LAYERS - 1, 0.0, above)
    )


def layer_shifts(block):
    rows, width = block.shape
    layer = iota((rows, width), 0) % LAYERS
    wide = block.astype(F32)
    first = jnp.where(layer == LAYERS - 1, 0.0, pltpu.roll(wide, rows - 1, 0))
    last = jnp.where(layer == 0, 0.0, pltpu.roll(wide, 1, 0))
    return jnp.concatenate([first.astype(BF), block, last.astype(BF)], axis=1)


def taps(ref, j, start, rows):
    parts = []
    for b in range(3):
        at = start + b * LAYERS
        if not isinstance(at, int):
            at = pl.multiple_of(at, LAYERS)
        parts.append(ref[j, pl.ds(at, rows), :])
    return jnp.concatenate(parts, axis=1)


def every_other(block, which):
    count = block.shape[0] // (2 * LAYERS)
    return [block[(2 * i + which) * LAYERS : (2 * i + which + 1) * LAYERS] for i in range(count)]


def paired_rows(first, second):
    parts = []
    for block in (first, second):
        for which in range(2):
            parts.append(jnp.concatenate(every_other(block, which), axis=0))
    return jnp.concatenate(parts, axis=1)


def widen_rows(block):
    parts = []
    for i in range(block.shape[0] // LAYERS):
        part = block[i * LAYERS : (i + 1) * LAYERS]
        parts += [part, part]
    return jnp.concatenate(parts, axis=0)


def sigmoid(v):
    return 1.0 / (1.0 + jnp.exp(-v))


def edges(ref, first, last, inner, width, split):
    lane = iota((inner, width), 1)
    at = slice(LAYERS, LAYERS + inner)
    main = ref.shape[2] - width
    for j in range(first, last):
        nxt = ref[j + 1, at, :width] if j + 1 < ref.shape[0] else jnp.zeros((inner, width), BF)
        prv = ref[j - 1, at, main - width : main] if j > 0 else jnp.zeros((inner, width), BF)
        ref[j, at, main:] = jnp.where(lane < split, nxt, prv)


def blank_rims(ref):
    pad = jnp.zeros((LAYERS, ref.shape[2]), BF)
    for j in range(ref.shape[0]):
        ref[j, :LAYERS, :] = pad
        ref[j, ref.shape[1] - LAYERS :, :] = pad


def keep_inside(meta, shards_seen, value, scale):
    if meta is None or shards_seen == 1:
        return value
    r = iota(value.shape, 0)
    inside = (r >= meta[shards_seen] // scale) & (r < meta[shards_seen + 1] // scale)
    return jnp.where(inside, value, jnp.zeros_like(value))


def clamped_edges(ref, j, inner, width, split):
    lane = iota((inner, width), 1)
    at = slice(LAYERS, LAYERS + inner)
    nxt = ref[jnp.minimum(j + 1, ref.shape[0] - 1), at, :width]
    prv = ref[jnp.maximum(j - 1, 0), at, :width]
    ref[j, at, width:] = jnp.where(lane < split, nxt, prv)


def forward_block(j, fz, hid, slope, wa):
    rows, width = hid.shape[1:]
    linear = combine(dot(taps(fz, j, 0, rows), wa[...]), width)
    logistic = sigmoid(linear)
    hid[j] = (linear * logistic).astype(BF)
    slope[j] = logistic * (1.0 + linear * (1.0 - logistic))


def chunk_kernel(own, partner, wa, fz, hid, slope):
    nbx = fz.shape[0]
    nb, cells, width = own.shape
    rows = hid.shape[1]
    e = lax.axis_index("eta")
    blank_rims(fz)
    for chunk, shard in ((own, e), (partner, 1 - e)):
        at = pl.multiple_of(LAYERS + shard * cells, LAYERS)
        for j in range(nb // 2 + 2):
            fz[j + 2 * (1 - e), pl.ds(at, cells), :width] = chunk[j + e * (nb // 2 - 2)]
    first = 3 * (1 - e)
    for j in range(nbx - 3):
        clamped_edges(fz, first + j, rows, width, 3 * width // PB)
    for j in range(nbx - 3):
        forward_block(first + j, fz, hid, slope, wa)


def forward_kernel(paired, count, *refs):
    meta = None
    if not paired:
        meta, refs = refs[0], refs[1:]
    pieces, refs = refs[:count], refs[count:]
    if paired:
        refs = refs[3:]
    wa, wb, mp, pool = refs[:4]
    fz, hid, slope, cz, gat, slope_b, proj = refs[4:]
    nbx = fz.shape[0]
    nc = gat.shape[0]
    rows = hid.shape[1]
    rows_c = rows // 2
    width = hid.shape[2]
    c1 = width // PB
    wide = gat.shape[2]
    blank_rims(cz)
    cells = pieces[0].shape[1]
    if paired:
        near, far = pieces
        e = lax.axis_index("eta")
        for rim, shard in ((near, e), (far, 1 - e)):
            at = pl.multiple_of(LAYERS + shard * cells, LAYERS)
            for j in range(2):
                fz[e * (nbx - 2) + j, pl.ds(at, cells), :width] = rim[j]
        first = e * (nbx - 3)
        for j in range(3):
            clamped_edges(fz, first + j, rows, width, 3 * c1)
        for j in range(3):
            forward_block(first + j, fz, hid, slope, wa)
    else:
        blank_rims(fz)
        for s in range(count // 3):
            middle, before, after = pieces[3 * s : 3 * s + 3]
            at = pl.multiple_of(LAYERS + meta[s] * cells, LAYERS)
            for j in range(2):
                fz[j, pl.ds(at, cells), :width] = before[j]
                fz[nbx - 2 + j, pl.ds(at, cells), :width] = after[j]
            for j in range(nbx - 4):
                fz[2 + j, pl.ds(at, cells), :width] = middle[j]
        edges(fz, 0, nbx, rows, width, 3 * c1)
        for j in range(nbx):
            forward_block(j, fz, hid, slope, wa)
    for j in range(nc + 2):
        start, end = max(2 * j - 1, 0), min(2 * j, nbx - 1)
        pooled = dot(paired_rows(hid[start], hid[end]), pool[...]) * 0.25
        cz[j, LAYERS : LAYERS + rows_c, :width] = keep_inside(meta, count // 3, pooled.astype(BF), 2)
    edges(cz, 1, nc + 1, rows_c, width, 3 * c1)
    for j in range(nc):
        linear = combine(dot(taps(cz, j + 1, 0, rows_c), wb[...]), wide)
        logistic = sigmoid(linear)
        gated = (linear * logistic).astype(BF)
        gat[j] = gated
        slope_b[j] = logistic * (1.0 + linear * (1.0 - logistic))
        proj[j] = dot(gated, mp[...]).astype(BF)


def backward_kernel(paired, count, *refs):
    meta = None
    if not paired:
        meta, refs = refs[0], refs[1:]
    pieces, refs = refs[:count], refs[count:]
    fz, slope, cz, gat, slope_b, wbf, mt, pool, up = refs[:9]
    gz, pk_ref = refs[9:11]
    cot, gb, fold, acc_a, acc_b, packed = refs[11:]
    nbx = fz.shape[0]
    nb = nbx - 4
    nc = gat.shape[0]
    rows = cot.shape[1]
    rows_c = rows // 2
    width = cot.shape[2]
    wide = gat.shape[2]
    c1 = width // PB
    c2 = wide // PB
    cells = pieces[0].shape[1]
    blank_rims(gz)
    blank_rims(gb)
    if paired:
        own, partner, near, far = pieces
        e = lax.axis_index("eta")
        for rim, shard in ((near, e), (far, 1 - e)):
            at = pl.multiple_of(shard * cells, cells)
            cot[1 + e * (nbx - 3), pl.ds(at, cells), :] = rim[2]
            for j in range(partner.shape[0]):
                if rim is near:
                    block = own[j + e * (own.shape[0] // 2 - 1)]
                else:
                    block = partner[j]
                cot[j + 2 - e, pl.ds(at, cells), :] = block
        own, own_at, own_at_c = rows, 0, 0
    else:
        for s in range(count // 3):
            middle, before, after = pieces[3 * s : 3 * s + 3]
            at = pl.multiple_of(meta[s] * cells, cells)
            cot[1, pl.ds(at, cells), :] = before[2]
            cot[nbx - 2, pl.ds(at, cells), :] = after[2]
            for j in range(nb):
                cot[2 + j, pl.ds(at, cells), :] = middle[j]
        own = cells
        own_at = pl.multiple_of(meta[0] * own, own)
        own_at_c = pl.multiple_of(meta[0] * (own // 2), own // 2)
    own_c = own // 2

    for j in range(nc):
        fold[j] = dot(paired_rows(cot[2 * j + 1], cot[2 * j + 2]), pool[...]).astype(BF)
        grad = dot(fold[j], mt[...]) * slope_b[j]
        gb[j, LAYERS : LAYERS + rows_c, :wide] = keep_inside(meta, count // 3, grad.astype(BF), 2)
    edges(gb, 0, nc, rows_c, width, c2)
    for j in range(nc):
        grad = combine(dot(taps(gb, j, 0, rows_c), wbf[...]), width).astype(BF)
        spread = 0.25 * dot(grad, up[...])
        for k in range(2):
            f = 2 * j + 1 + k
            total = cot[f].astype(F32) + widen_rows(spread[:, k * width : (k + 1) * width])
            value = (total * slope[f]).astype(BF)
            gz[f, LAYERS : LAYERS + rows, :width] = keep_inside(meta, count // 3, value, 1)
    edges(gz, 2, nbx - 2, rows, width, 3 * c1)

    def own_half(value, j):
        p = iota(value.shape, 1) // (value.shape[1] // PB)
        if j == 0:
            value = jnp.where(p >= PB // 2, value, jnp.zeros_like(value))
        if j == nc - 1:
            value = jnp.where(p < PB // 2, value, jnp.zeros_like(value))
        return value

    lhs = jnp.concatenate(
        [layer_shifts(gz[2 + j, pl.ds(LAYERS + own_at, own), :width]) for j in range(nb)], axis=0
    )
    rhs = jnp.concatenate([taps(fz, 2 + j, own_at, own) for j in range(nb)], axis=0)
    acc_a[...] = dot_rows(lhs, rhs)
    lhs = jnp.concatenate(
        [layer_shifts(own_half(gb[j, pl.ds(LAYERS + own_at_c, own_c), :wide], j)) for j in range(nc)], axis=0
    )
    rhs = jnp.concatenate([taps(cz, j + 1, own_at_c, own_c) for j in range(nc)], axis=0)
    acc_b[...] = dot_rows(lhs, rhs)
    lhs = jnp.concatenate([gat[j, pl.ds(own_at_c, own_c), :] for j in range(nc)], axis=0)
    rhs = jnp.concatenate([own_half(fold[j, pl.ds(own_at_c, own_c), :], j) for j in range(nc)], axis=0)
    mixed = dot_rows(lhs, rhs)
    mix_sum = mixed[:c2, :c1]
    for p in range(1, PB):
        mix_sum = mix_sum + mixed[p * c2 : (p + 1) * c2, p * c1 : (p + 1) * c1]
    packed[c1:, 27 * c1 : 28 * c1] = mix_sum
    packed[:c1, 27 * c1 : 28 * c1] = jnp.zeros((c1, c1), F32)
    span = 2 * width
    for acc, outs, first in ((acc_a, c1, 0), (acc_b, c2, c1)):
        for b in range(3):
            for c in range(3):
                total = None
                for p in range(PB):
                    at = (c * PB + p) * outs
                    part = acc[at : at + outs, b * span : (b + 1) * span]
                    part = pltpu.roll(part, (span - (p - 1) * c1) % span, 1)
                    total = part if total is None else total + part
                for a in range(3):
                    t = 9 * a + 3 * b + c
                    packed[first : first + outs, t * c1 : (t + 1) * c1] = total[:, a * c1 : (a + 1) * c1]
    chunk = pk_ref.shape[1]
    per = packed.shape[0] // chunk
    used = packed.shape[1] // 128 * per
    for v in range(packed.shape[1] // 128):
        for r in range(per):
            pk_ref[v * per + r] = packed[r * chunk : (r + 1) * chunk, v * 128 : (v + 1) * 128].astype(BF)
    for v in range(used, pk_ref.shape[0]):
        pk_ref[v] = jnp.zeros(pk_ref.shape[1:], BF)


def finish_kernel(paired, *refs):
    meta = None
    if not paired:
        meta, refs = refs[0], refs[1:]
    gz, hid, proj, waf, up = refs[:5]
    outs = refs[5:-1]
    buf = refs[-1]
    nb = gz.shape[0] - 4
    width = hid.shape[2]
    cells = outs[0].shape[2]
    if paired:
        own, own_at, own_at_c = hid.shape[1], 0, 0
        e = lax.axis_index("eta")
        starts = [pl.multiple_of(e * cells, cells), pl.multiple_of((1 - e) * cells, cells)]
    else:
        own = cells
        own_at = pl.multiple_of(meta[0] * own, own)
        own_at_c = pl.multiple_of(meta[0] * (own // 2), own // 2)
        starts = [0]

    def write(value, place):
        buf[place] = value
        for out, start in zip(outs, starts):
            out[place] = buf[place, pl.ds(start, cells), :].T.astype(BF)

    for j in range(nb):
        grad = combine(dot(taps(gz, 2 + j, own_at, own), waf[...]), width)
        write(grad, nb + j)
    for j in range(nb):
        k = (j + 1) % 2
        spread = dot(proj[(j + 1) // 2, pl.ds(own_at_c, own // 2), :], up[:, k * width : (k + 1) * width])
        write(hid[2 + j, pl.ds(own_at, own), :].astype(F32) + widen_rows(spread), j)


def restore_kernel(kept, received, out_ref, gin_ref):
    ch, rows, cells = out_ref.shape
    half = rows // 2
    e = lax.axis_index("eta")
    for k, ref in enumerate((out_ref, gin_ref)):
        at = k * half // PB
        mine = kept[at : at + half // PB].astype(F32)
        other = received[at : at + half // PB].astype(F32)
        first = jnp.where(e == 0, mine, other).reshape(half, ch, cells)
        second = jnp.where(e == 0, other, mine).reshape(half, ch, cells)
        ref[...] = jnp.swapaxes(jnp.concatenate([first, second], axis=0), 0, 1).astype(BF)


def sum_kernel(x_ref, o_ref):
    total = jnp.sum(x_ref[...].astype(F32), axis=0).astype(BF)
    o_ref[...] = jnp.broadcast_to(total[None], o_ref.shape)


def post_kernel(factor, x_ref, ga_ref, gb_ref, gm_ref, buf):
    chunk = x_ref.shape[1]
    per = buf.shape[0] // chunk
    c1 = ga_ref.shape[1]
    for v in range(buf.shape[1] // 128):
        for r in range(per):
            buf[r * chunk : (r + 1) * chunk, v * 128 : (v + 1) * 128] = x_ref[v * per + r].astype(F32) * factor
    for t in range(27):
        ga_ref[t] = buf[:c1, t * c1 : (t + 1) * c1]
        gb_ref[t] = buf[c1:, t * c1 : (t + 1) * c1].T
    gm_ref[...] = buf[c1:, 27 * c1 : 28 * c1].T


def call(kernel, outs, *args, scratch=(), smem=0, near=(), far=(), aliases={}):
    args = list(args)
    specs = []
    for place in range(len(args)):
        if place < smem:
            specs.append(pl.BlockSpec(memory_space=pltpu.SMEM))
        elif place in far:
            specs.append(pl.BlockSpec(memory_space=pl.ANY))
            args[place] = pltpu.with_memory_space_constraint(args[place], pltpu.HBM)
        else:
            specs.append(pl.BlockSpec(memory_space=pltpu.VMEM))
            if place in near:
                args[place] = pltpu.with_memory_space_constraint(args[place], pltpu.VMEM)
    return pl.pallas_call(
        kernel,
        out_shape=outs,
        in_specs=specs,
        out_specs=tuple(pl.BlockSpec(memory_space=pltpu.VMEM) for _ in outs),
        scratch_shapes=list(scratch),
        input_output_aliases=aliases,
        compiler_params=pltpu.CompilerParams(vmem_limit_bytes=32 * 1024 * 1024),
    )(*args)


def shape(dims, dtype=BF):
    return jax.ShapeDtypeStruct(tuple(dims), dtype)


AXES = ("phi", "eta")


def moves(n_phi, n_eta, rule):
    found = []
    for p in range(n_phi):
        for s in range(n_eta):
            step, t = rule(p, s)
            if 0 <= t < n_eta:
                found.append((p * n_eta + s, (p + step) % n_phi * n_eta + t))
    return found


def gather_pair(f_own, c_own, c_sent, near, far):
    n_phi = lax.axis_size("phi")

    def send(value, rule):
        return lax.ppermute(value, AXES, moves(n_phi, 2, rule))

    far = send(far, lambda p, s: (2 * s - 1, 1 - s))
    near = send(near, lambda p, s: (1 - 2 * s, s))
    f_other = send(f_own, lambda p, s: (0, 1 - s))
    c_other = send(c_sent, lambda p, s: (0, 1 - s))
    return [f_own, f_other, near, far], [c_own, c_other, near, far]


def gather_window(f_own, c_own, low, high):
    n_phi = lax.axis_size("phi")
    n_eta = lax.axis_size("eta")
    f_pieces = []
    c_pieces = []
    for step in window_steps(n_eta):
        send = lambda value, move: lax.ppermute(value, AXES, moves(n_phi, n_eta, lambda p, s: (move, s - step)))
        rims = [send(high, 1), send(low, -1)]
        f_pieces += [f_own if step == 0 else send(f_own, 0)] + rims
        c_pieces += [c_own if step == 0 else send(c_own, 0)] + rims
    return f_pieces, c_pieces


def window_steps(n_eta):
    return [0] if n_eta == 1 else [0, -1, 1, -2, 2]


def window_meta(n_eta, cells):
    e = lax.axis_index("eta")
    steps = window_steps(n_eta)
    middle = len(steps) // 2
    values = [middle + step for step in steps]
    values += [jnp.maximum(0, middle - e) * cells, jnp.minimum(len(steps), n_eta + middle - e) * cells]
    return jnp.stack([jnp.asarray(v, jnp.int32) for v in values])


def shards(features, cotangent, kernel_a, kernel_b, mixing):
    c1, n_rows, cells = features.shape
    c2 = kernel_b.shape[1]
    nb = n_rows // PB
    width = PB * c1
    n_eta = lax.axis_size("eta")
    paired = n_eta == 2 and nb % 4 == 0
    block = (cells, width)
    f_own, c_own, first, second, *c_sent = call(
        functools.partial(pre_kernel, paired),
        tuple(pltpu.VMEM((n,) + block, BF) for n in (nb, nb, 3, 3) + ((nb // 2 + 1,) if paired else ())),
        features,
        cotangent,
        scratch=(
            pltpu.VMEM(features.shape, BF),
            pltpu.VMEM(features.shape, BF),
            pltpu.SemaphoreType.DMA((2,)),
        ),
        far=(0, 1),
    )
    if paired:
        f_pieces, c_pieces = gather_pair(f_own, c_own, c_sent[0], first, second)
        meta = []
        nbx = nb // 2 + 4
        rows = 2 * cells
    else:
        f_pieces, c_pieces = gather_window(f_own, c_own, first, second)
        meta = [window_meta(n_eta, cells)]
        nbx = nb + 4
        rows = len(window_steps(n_eta)) * cells
    wa, waf, wb, wbf, mp, mt, pool, up = call(
        weights_kernel,
        (
            pltpu.VMEM((3 * 2 * width, 3 * width), BF),
            pltpu.VMEM((3 * 2 * width, 3 * width), BF),
            pltpu.VMEM((3 * 2 * width, 3 * PB * c2), BF),
            pltpu.VMEM((3 * 6 * c2, 3 * width), BF),
            pltpu.VMEM((PB * c2, width), BF),
            pltpu.VMEM((width, PB * c2), BF),
            pltpu.VMEM((4 * width, width), BF),
            pltpu.VMEM((width, 2 * width), BF),
        ),
        kernel_a,
        jnp.swapaxes(kernel_b, 1, 2),
        mixing,
        scratch=(
            pltpu.VMEM((27 * c1, width), F32),
            pltpu.VMEM((27 * c1, width), F32),
            pltpu.VMEM((27 * c1, PB * c2), F32),
            pltpu.VMEM((27 * c2, width), F32),
            pltpu.VMEM(kernel_a.shape, BF),
            pltpu.VMEM((27, c1, c2), BF),
            pltpu.VMEM(mixing.shape, BF),
            pltpu.SemaphoreType.DMA((3,)),
        ),
        far=(0, 1, 2),
    )
    nc = nbx // 2 - 1
    rows_c = rows // 2
    devices = lax.axis_size("phi") * n_eta
    lanes = 28 * c1
    total_rows = (c1 + c2) * lanes // 128
    chunk = next(d for d in range(8, c1 + c2 + 1, 8) if (c1 + c2) % d == 0 and total_rows <= d * devices)
    tall = rows + 2 * LAYERS
    tall_c = rows_c + 2 * LAYERS
    skip = len(meta)
    count = len(f_pieces)
    matrices = (wa, wb, mp, pool)
    fine = (
        pltpu.VMEM((nbx, tall, 2 * width), BF),
        pltpu.VMEM((nbx, rows, width), BF),
        pltpu.VMEM((nbx, rows, width), F32),
    )
    pooled = (
        pltpu.VMEM((nc + 2, tall_c, 2 * width), BF),
        pltpu.VMEM((nc, rows_c, PB * c2), BF),
        pltpu.VMEM((nc, rows_c, PB * c2), F32),
        pltpu.VMEM((nc, rows_c, width), BF),
    )
    if paired:
        started = call(chunk_kernel, fine, *f_pieces[:2], wa, near=range(3))
        args = (*f_pieces[2:], *started, *matrices)
        extra = {"near": range(len(args)), "aliases": {2: 0, 3: 1, 4: 2}}
    else:
        args = (*meta, *f_pieces, *matrices)
        extra = {"near": range(skip + 1, len(args)), "smem": skip}
    fz, hid, slope, cz, gat, slope_b, proj = call(
        functools.partial(forward_kernel, paired, 2 if paired else count), fine + pooled, *args, **extra
    )
    inner = (fz, slope, cz, gat, slope_b, wbf, mt, pool, up)
    gz, terms = call(
        functools.partial(backward_kernel, paired, count),
        (pltpu.VMEM((nbx, tall, 2 * width), BF), pltpu.VMEM((devices, chunk, 128), BF)),
        *meta,
        *c_pieces,
        *inner,
        scratch=(
            pltpu.VMEM((nbx, rows, width), BF),
            pltpu.VMEM((nc, tall_c, PB * c2 + width), BF),
            pltpu.VMEM((nc, rows_c, width), BF),
            pltpu.VMEM((3 * width, 6 * width), F32),
            pltpu.VMEM((3 * PB * c2, 6 * width), F32),
            pltpu.VMEM((c1 + c2, lanes), F32),
        ),
        smem=skip,
        near=range(skip + 1, skip + count + len(inner)),
    )
    terms = lax.all_to_all(terms, AXES, 0, 0, tiled=True)
    blocks = 2 * (nbx - 4)
    results = call(
        functools.partial(finish_kernel, paired),
        (pltpu.VMEM((blocks, width, cells), BF),) * (2 if paired else 1),
        *meta,
        gz,
        hid,
        proj,
        waf,
        up,
        scratch=(pltpu.VMEM((blocks, rows if paired else cells, width), F32),),
        smem=skip,
        near=range(skip, skip + 5),
    )
    if paired:
        kept, sent = results
        received = lax.ppermute(sent, AXES, moves(lax.axis_size("phi"), 2, lambda p, s: (0, 1 - s)))
        terms, kept = lax.optimization_barrier((terms, kept))
        output, grad_input = call(
            restore_kernel, (shape(features.shape), shape(features.shape)), kept, received, near=(0, 1)
        )
    else:
        output, grad_input = (
            jnp.transpose(part.reshape(n_rows, c1, cells), (1, 0, 2)) for part in (results[0][:nb], results[0][nb:])
        )
    (sums,) = call(sum_kernel, (pltpu.VMEM(terms.shape, BF),), terms, near=(0,))
    sums = lax.all_to_all(sums, AXES, 0, 0, tiled=True)
    cell_count = n_rows * cells * devices
    grad_a, grad_b, grad_mix = call(
        functools.partial(post_kernel, 1.0 / math.sqrt(cell_count)),
        (shape((27, c1, c1), F32), shape((27, c1, c2), F32), shape((c1, c2), F32)),
        sums,
        scratch=(pltpu.VMEM((c1 + c2, lanes), F32),),
        near=(0,),
    )
    return output, grad_input, grad_a, jnp.swapaxes(grad_b, 1, 2), grad_mix


def solution(mesh):
    in_specs = (P(None, "phi", "eta"), P(None, "phi", "eta"), P(), P(), P())
    out_specs = (P(None, "phi", "eta"), P(None, "phi", "eta"), P(), P(), P())

    return jax.shard_map(shards, mesh=mesh, in_specs=in_specs, out_specs=out_specs, check_vma=False)
```

```python
import functools
import math

import jax
import jax.numpy as jnp
from jax import lax
from jax.experimental import pallas as pl
from jax.experimental.pallas import tpu as pltpu
from jax.sharding import PartitionSpec as P


LAYERS = 32
PB = 4
BF = jnp.bfloat16
F32 = jnp.float32


def iota(shape, dim):
    return lax.broadcasted_iota(jnp.int32, shape, dim)


def dot(a, b):
    return jnp.dot(a, b, preferred_element_type=F32)


def dot_rows(a, b):
    return lax.dot_general(a, b, (((0,), (0,)), ((), ())), preferred_element_type=F32)


def fetch(sources, places, sems):
    moves = [pltpu.make_async_copy(src, dst, sems.at[i]) for i, (src, dst) in enumerate(zip(sources, places))]
    for move in moves:
        move.start()
    return moves


def pre_kernel(paired, f_hbm, c_hbm, f_own, c_own, first, second, *rest):
    f_ref, c_ref, sems = rest[-3:]
    nb = f_own.shape[0]
    moves = fetch((f_hbm, c_hbm), (f_ref, c_ref), sems)
    for move, ref, own in zip(moves, (f_ref, c_ref), (f_own, c_own)):
        move.wait()
        ch, _, cells = ref.shape
        swapped = jnp.swapaxes(ref[...].astype(F32), 0, 1)
        for j in range(nb):
            own[j] = swapped[PB * j : PB * (j + 1)].reshape(PB * ch, cells).T.astype(BF)
    e = lax.axis_index("eta") if paired else 1
    for rim, low in ((first, e), (second, 1 - e)):
        for j in range(2):
            rim[j] = f_own[(nb - 2) * (1 - low) + j]
        rim[2] = c_own[(nb - 1) * (1 - low)]
    if paired:
        partner = rest[0]
        for j in range(partner.shape[0]):
            partner[j] = c_own[(1 - e) * (nb // 2 - 1) + j]


def copies(size, times):
    shape = (size, size * times)
    return jnp.where(iota(shape, 0) == iota(shape, 1) % size, 1.0, 0.0).astype(BF)


def weights_kernel(
    ka_hbm, kbt_hbm, mix_hbm, wa, waf, wb, wbf, mp, mt, pool, up, ta, taf, tb, tbf, ka, kbt, mix, sems
):
    for move in fetch((ka_hbm, kbt_hbm, mix_hbm), (ka, kbt, mix), sems):
        move.wait()
    c1 = ka.shape[1]
    c2 = kbt.shape[2]
    width = PB * c1
    wide = PB * c2

    def flat(block):
        return block.reshape(-1, block.shape[2])

    def turned(ref):
        return jnp.swapaxes(ref[...].astype(F32), 1, 2).astype(BF)

    few = copies(c1, PB)
    many = copies(c2, PB)
    ta[...] = dot(flat(turned(ka)), few)
    taf[...] = dot(flat(ka[...]), few)
    tb[...] = dot(flat(kbt[...]), many)
    tbf[...] = dot(flat(turned(kbt)), few)

    def toeplitz(out, source, order, rows_per, cols_per, row_blocks, turn=0):
        height = len(row_blocks) * rows_per
        across = PB * cols_per
        place = iota((rows_per, across), 1) // cols_per
        for b in range(3):
            for c in range(3):
                for at, q in enumerate(row_blocks):
                    value = jnp.zeros((rows_per, across), F32)
                    for a in range(3):
                        p = q + 1 - a
                        if 0 <= p < PB:
                            t = order(9 * a + 3 * b + c) * rows_per
                            value = jnp.where(place == (p + turn) % PB, source[t : t + rows_per], value)
                    first = b * height + at * rows_per
                    out[first : first + rows_per, c * across : (c + 1) * across] = value.astype(BF)

    ring = (0, 1, 2, 3, 4, 100, 100, -1)
    toeplitz(wa, ta, lambda t: t, c1, c1, (2, 3, 0, 1, 100, -1, 4, 100), PB // 2)
    toeplitz(wb, tb, lambda t: t, c1, c2, ring)
    toeplitz(wbf, tbf, lambda t: 26 - t, c2, c1, (0, 1, 2, 3, 4, -1))
    toeplitz(waf, taf, lambda t: 26 - t, c1, c1, ring)
    mixing = mix[...]
    spread = dot(mixing, many)
    spread_t = dot(mixing.astype(F32).T.astype(BF), few)
    for p in range(PB):
        inside = iota((c1, wide), 1) // c2 == p
        mt[p * c1 : (p + 1) * c1] = jnp.where(inside, spread, 0.0).astype(BF)
        inside = iota((c2, width), 1) // c1 == p
        mp[p * c2 : (p + 1) * c2] = jnp.where(inside, spread_t, 0.0).astype(BF)
    r = iota(pool.shape, 0)
    l = iota(pool.shape, 1)
    hit = (r % c1 == l % c1) & (r // (2 * width) * 2 + r % width // c1 // 2 == l // c1)
    pool[...] = jnp.where(hit, 1.0, 0.0).astype(BF)
    r = iota(up.shape, 0)
    l = iota(up.shape, 1)
    hit = (r % c1 == l % c1) & (l // width * 2 + l % width // c1 // 2 == r // c1)
    up[...] = jnp.where(hit, 1.0, 0.0).astype(BF)


def combine(summed, width):
    rows = summed.shape[0]
    layer = iota((rows, width), 0) % LAYERS
    below = pltpu.roll(summed[:, :width], 1, 0)
    above = pltpu.roll(summed[:, 2 * width :], rows - 1, 0)
    return (
        summed[:, width : 2 * width]
        + jnp.where(layer == 0, 0.0, below)
        + jnp.where(layer == LAYERS - 1, 0.0, above)
    )


def layer_shifts(block):
    rows, width = block.shape
    layer = iota((rows, width), 0) % LAYERS
    wide = block.astype(F32)
    first = jnp.where(layer == LAYERS - 1, 0.0, pltpu.roll(wide, rows - 1, 0))
    last = jnp.where(layer == 0, 0.0, pltpu.roll(wide, 1, 0))
    return jnp.concatenate([first.astype(BF), block, last.astype(BF)], axis=1)


def taps(ref, j, start, rows):
    parts = []
    for b in range(3):
        at = start + b * LAYERS
        if not isinstance(at, int):
            at = pl.multiple_of(at, LAYERS)
        parts.append(ref[j, pl.ds(at, rows), :])
    return jnp.concatenate(parts, axis=1)


def every_other(block, which):
    count = block.shape[0] // (2 * LAYERS)
    return [block[(2 * i + which) * LAYERS : (2 * i + which + 1) * LAYERS] for i in range(count)]


def paired_rows(first, second):
    parts = []
    for block in (first, second):
        for which in range(2):
            parts.append(jnp.concatenate(every_other(block, which), axis=0))
    return jnp.concatenate(parts, axis=1)


def widen_rows(block):
    parts = []
    for i in range(block.shape[0] // LAYERS):
        part = block[i * LAYERS : (i + 1) * LAYERS]
        parts += [part, part]
    return jnp.concatenate(parts, axis=0)


def sigmoid(v):
    return 1.0 / (1.0 + jnp.exp(-v))


def edges(ref, first, last, inner, width, split):
    lane = iota((inner, width), 1)
    at = slice(LAYERS, LAYERS + inner)
    main = ref.shape[2] - width
    for j in range(first, last):
        nxt = ref[j + 1, at, :width] if j + 1 < ref.shape[0] else jnp.zeros((inner, width), BF)
        prv = ref[j - 1, at, main - width : main] if j > 0 else jnp.zeros((inner, width), BF)
        ref[j, at, main:] = jnp.where(lane < split, nxt, prv)


def blank_rims(ref):
    pad = jnp.zeros((LAYERS, ref.shape[2]), BF)
    for j in range(ref.shape[0]):
        ref[j, :LAYERS, :] = pad
        ref[j, ref.shape[1] - LAYERS :, :] = pad


def keep_inside(meta, shards_seen, value, scale):
    if meta is None or shards_seen == 1:
        return value
    r = iota(value.shape, 0)
    inside = (r >= meta[shards_seen] // scale) & (r < meta[shards_seen + 1] // scale)
    return jnp.where(inside, value, jnp.zeros_like(value))


def forward_block(place, j, fz, half_way, hid, slope, wa):
    rows, width = hid.shape[1:]
    half = width // 2
    at = slice(LAYERS, LAYERS + rows)
    left = iota((rows, width), 1) < half
    low, high = fz[j, at, :width], fz[j + 1, at, :width]
    half_way[place, at, :width] = jnp.where(left, high, low)
    half_way[place, at, width:] = jnp.where(left, low, high)
    linear = combine(dot(taps(half_way, place, 0, rows), wa[...]), width)
    logistic = sigmoid(linear)
    hidden = (linear * logistic).astype(BF)
    steep = logistic * (1.0 + linear * (1.0 - logistic))
    for ref, value in ((hid, hidden), (slope, steep)):
        ref[j + 1, :, :half] = value[:, :half]
        ref[j, :, half:] = value[:, half:]


def blank_ends(hid):
    rows, width = hid.shape[1:]
    none = jnp.zeros((rows, width // 2), BF)
    hid[0, :, : width // 2] = none
    hid[hid.shape[0] - 1, :, width // 2 :] = none


def chunk_kernel(own, partner, wa, fz, hid, slope, half_way):
    nbx = fz.shape[0]
    nb, cells, width = own.shape
    e = lax.axis_index("eta")
    blank_rims(fz)
    blank_rims(half_way)
    blank_ends(hid)
    for chunk, shard in ((own, e), (partner, 1 - e)):
        at = pl.multiple_of(LAYERS + shard * cells, LAYERS)
        for j in range(nb // 2 + 2):
            fz[j + 2 * (1 - e), pl.ds(at, cells), :width] = chunk[j + e * (nb // 2 - 2)]
    for j in range(nbx - 3):
        forward_block(j, 2 * (1 - e) + j, fz, half_way, hid, slope, wa)


def forward_kernel(paired, count, *refs):
    meta = None
    if not paired:
        meta, refs = refs[0], refs[1:]
    pieces, refs = refs[:count], refs[count:]
    if paired:
        refs = refs[3:]
    wa, wb, mp, pool = refs[:4]
    fz, hid, slope, cz, gat, slope_b, proj, half_way = refs[4:]
    nbx = fz.shape[0]
    nc = gat.shape[0]
    rows = hid.shape[1]
    rows_c = rows // 2
    width = hid.shape[2]
    c1 = width // PB
    wide = gat.shape[2]
    blank_rims(cz)
    blank_rims(half_way)
    cells = pieces[0].shape[1]
    if paired:
        near, far = pieces
        e = lax.axis_index("eta")
        for rim, shard in ((near, e), (far, 1 - e)):
            at = pl.multiple_of(LAYERS + shard * cells, LAYERS)
            for j in range(2):
                fz[e * (nbx - 2) + j, pl.ds(at, cells), :width] = rim[j]
        for j in range(2):
            forward_block(j, e * (nbx - 3) + j, fz, half_way, hid, slope, wa)
    else:
        blank_rims(fz)
        blank_ends(hid)
        for s in range(count // 3):
            middle, before, after = pieces[3 * s : 3 * s + 3]
            at = pl.multiple_of(LAYERS + meta[s] * cells, LAYERS)
            for j in range(2):
                fz[j, pl.ds(at, cells), :width] = before[j]
                fz[nbx - 2 + j, pl.ds(at, cells), :width] = after[j]
            for j in range(nbx - 4):
                fz[2 + j, pl.ds(at, cells), :width] = middle[j]
        for j in range(nbx - 1):
            forward_block(j, j, fz, half_way, hid, slope, wa)
    edges(fz, 2, nbx - 2, rows, width, 3 * c1)
    for j in range(nc + 2):
        start, end = max(2 * j - 1, 0), min(2 * j, nbx - 1)
        pooled = dot(paired_rows(hid[start], hid[end]), pool[...]) * 0.25
        cz[j, LAYERS : LAYERS + rows_c, :width] = keep_inside(meta, count // 3, pooled.astype(BF), 2)
    edges(cz, 1, nc + 1, rows_c, width, 3 * c1)
    for j in range(nc):
        linear = combine(dot(taps(cz, j + 1, 0, rows_c), wb[...]), wide)
        logistic = sigmoid(linear)
        gated = (linear * logistic).astype(BF)
        gat[j] = gated
        slope_b[j] = logistic * (1.0 + linear * (1.0 - logistic))
        proj[j] = dot(gated, mp[...]).astype(BF)


def backward_kernel(paired, count, *refs):
    meta = None
    if not paired:
        meta, refs = refs[0], refs[1:]
    pieces, refs = refs[:count], refs[count:]
    fz, slope, cz, gat, slope_b, wbf, mt, pool, up = refs[:9]
    gz, pk_ref = refs[9:11]
    cot, gb, fold, acc_a, acc_b, packed = refs[11:]
    nbx = fz.shape[0]
    nb = nbx - 4
    nc = gat.shape[0]
    rows = cot.shape[1]
    rows_c = rows // 2
    width = cot.shape[2]
    wide = gat.shape[2]
    c1 = width // PB
    c2 = wide // PB
    cells = pieces[0].shape[1]
    blank_rims(gz)
    blank_rims(gb)
    if paired:
        own, partner, near, far = pieces
        e = lax.axis_index("eta")
        for rim, shard in ((near, e), (far, 1 - e)):
            at = pl.multiple_of(shard * cells, cells)
            cot[1 + e * (nbx - 3), pl.ds(at, cells), :] = rim[2]
            for j in range(partner.shape[0]):
                if rim is near:
                    block = own[j + e * (own.shape[0] // 2 - 1)]
                else:
                    block = partner[j]
                cot[j + 2 - e, pl.ds(at, cells), :] = block
        own, own_at, own_at_c = rows, 0, 0
    else:
        for s in range(count // 3):
            middle, before, after = pieces[3 * s : 3 * s + 3]
            at = pl.multiple_of(meta[s] * cells, cells)
            cot[1, pl.ds(at, cells), :] = before[2]
            cot[nbx - 2, pl.ds(at, cells), :] = after[2]
            for j in range(nb):
                cot[2 + j, pl.ds(at, cells), :] = middle[j]
        own = cells
        own_at = pl.multiple_of(meta[0] * own, own)
        own_at_c = pl.multiple_of(meta[0] * (own // 2), own // 2)
    own_c = own // 2

    for j in range(nc):
        fold[j] = dot(paired_rows(cot[2 * j + 1], cot[2 * j + 2]), pool[...]).astype(BF)
        grad = dot(fold[j], mt[...]) * slope_b[j]
        gb[j, LAYERS : LAYERS + rows_c, :wide] = keep_inside(meta, count // 3, grad.astype(BF), 2)
    edges(gb, 0, nc, rows_c, width, c2)
    for j in range(nc):
        grad = combine(dot(taps(gb, j, 0, rows_c), wbf[...]), width).astype(BF)
        spread = 0.25 * dot(grad, up[...])
        for k in range(2):
            f = 2 * j + 1 + k
            total = cot[f].astype(F32) + widen_rows(spread[:, k * width : (k + 1) * width])
            value = (total * slope[f]).astype(BF)
            gz[f, LAYERS : LAYERS + rows, :width] = keep_inside(meta, count // 3, value, 1)
    edges(gz, 2, nbx - 2, rows, width, 3 * c1)

    def own_half(value, j):
        p = iota(value.shape, 1) // (value.shape[1] // PB)
        if j == 0:
            value = jnp.where(p >= PB // 2, value, jnp.zeros_like(value))
        if j == nc - 1:
            value = jnp.where(p < PB // 2, value, jnp.zeros_like(value))
        return value

    lhs = jnp.concatenate(
        [layer_shifts(gz[2 + j, pl.ds(LAYERS + own_at, own), :width]) for j in range(nb)], axis=0
    )
    rhs = jnp.concatenate([taps(fz, 2 + j, own_at, own) for j in range(nb)], axis=0)
    acc_a[...] = dot_rows(lhs, rhs)
    lhs = jnp.concatenate(
        [layer_shifts(own_half(gb[j, pl.ds(LAYERS + own_at_c, own_c), :wide], j)) for j in range(nc)], axis=0
    )
    rhs = jnp.concatenate([taps(cz, j + 1, own_at_c, own_c) for j in range(nc)], axis=0)
    acc_b[...] = dot_rows(lhs, rhs)
    lhs = jnp.concatenate([gat[j, pl.ds(own_at_c, own_c), :] for j in range(nc)], axis=0)
    rhs = jnp.concatenate([own_half(fold[j, pl.ds(own_at_c, own_c), :], j) for j in range(nc)], axis=0)
    mixed = dot_rows(lhs, rhs)
    mix_sum = mixed[:c2, :c1]
    for p in range(1, PB):
        mix_sum = mix_sum + mixed[p * c2 : (p + 1) * c2, p * c1 : (p + 1) * c1]
    packed[c1:, 27 * c1 : 28 * c1] = mix_sum
    packed[:c1, 27 * c1 : 28 * c1] = jnp.zeros((c1, c1), F32)
    span = 2 * width
    for acc, outs, first in ((acc_a, c1, 0), (acc_b, c2, c1)):
        for b in range(3):
            for c in range(3):
                total = None
                for p in range(PB):
                    at = (c * PB + p) * outs
                    part = acc[at : at + outs, b * span : (b + 1) * span]
                    part = pltpu.roll(part, (span - (p - 1) * c1) % span, 1)
                    total = part if total is None else total + part
                for a in range(3):
                    t = 9 * a + 3 * b + c
                    packed[first : first + outs, t * c1 : (t + 1) * c1] = total[:, a * c1 : (a + 1) * c1]
    chunk = pk_ref.shape[1]
    per = packed.shape[0] // chunk
    used = packed.shape[1] // 128 * per
    for v in range(packed.shape[1] // 128):
        for r in range(per):
            pk_ref[v * per + r] = packed[r * chunk : (r + 1) * chunk, v * 128 : (v + 1) * 128].astype(BF)
    for v in range(used, pk_ref.shape[0]):
        pk_ref[v] = jnp.zeros(pk_ref.shape[1:], BF)


def finish_kernel(paired, *refs):
    meta = None
    if not paired:
        meta, refs = refs[0], refs[1:]
    gz, hid, proj, waf, up = refs[:5]
    outs = refs[5:-1]
    buf = refs[-1]
    nb = gz.shape[0] - 4
    width = hid.shape[2]
    cells = outs[0].shape[2]
    if paired:
        own, own_at, own_at_c = hid.shape[1], 0, 0
        e = lax.axis_index("eta")
        starts = [pl.multiple_of(e * cells, cells), pl.multiple_of((1 - e) * cells, cells)]
    else:
        own = cells
        own_at = pl.multiple_of(meta[0] * own, own)
        own_at_c = pl.multiple_of(meta[0] * (own // 2), own // 2)
        starts = [0]

    def write(value, place):
        buf[place] = value
        for out, start in zip(outs, starts):
            out[place] = buf[place, pl.ds(start, cells), :].T.astype(BF)

    for j in range(nb):
        grad = combine(dot(taps(gz, 2 + j, own_at, own), waf[...]), width)
        write(grad, nb + j)
    for j in range(nb):
        k = (j + 1) % 2
        spread = dot(proj[(j + 1) // 2, pl.ds(own_at_c, own // 2), :], up[:, k * width : (k + 1) * width])
        write(hid[2 + j, pl.ds(own_at, own), :].astype(F32) + widen_rows(spread), j)


def restore_kernel(kept, received, out_ref, gin_ref):
    ch, rows, cells = out_ref.shape
    half = rows // 2
    e = lax.axis_index("eta")
    for k, ref in enumerate((out_ref, gin_ref)):
        at = k * half // PB
        mine = kept[at : at + half // PB].astype(F32)
        other = received[at : at + half // PB].astype(F32)
        first = jnp.where(e == 0, mine, other).reshape(half, ch, cells)
        second = jnp.where(e == 0, other, mine).reshape(half, ch, cells)
        ref[...] = jnp.swapaxes(jnp.concatenate([first, second], axis=0), 0, 1).astype(BF)


def sum_kernel(x_ref, o_ref):
    total = jnp.sum(x_ref[...].astype(F32), axis=0).astype(BF)
    o_ref[...] = jnp.broadcast_to(total[None], o_ref.shape)


def post_kernel(factor, x_ref, ga_ref, gb_ref, gm_ref, buf):
    chunk = x_ref.shape[1]
    per = buf.shape[0] // chunk
    c1 = ga_ref.shape[1]
    for v in range(buf.shape[1] // 128):
        for r in range(per):
            buf[r * chunk : (r + 1) * chunk, v * 128 : (v + 1) * 128] = x_ref[v * per + r].astype(F32) * factor
    for t in range(27):
        ga_ref[t] = buf[:c1, t * c1 : (t + 1) * c1]
        gb_ref[t] = buf[c1:, t * c1 : (t + 1) * c1].T
    gm_ref[...] = buf[c1:, 27 * c1 : 28 * c1].T


def call(kernel, outs, *args, scratch=(), smem=0, near=(), far=(), aliases={}):
    args = list(args)
    specs = []
    for place in range(len(args)):
        if place < smem:
            specs.append(pl.BlockSpec(memory_space=pltpu.SMEM))
        elif place in far:
            specs.append(pl.BlockSpec(memory_space=pl.ANY))
            args[place] = pltpu.with_memory_space_constraint(args[place], pltpu.HBM)
        else:
            specs.append(pl.BlockSpec(memory_space=pltpu.VMEM))
            if place in near:
                args[place] = pltpu.with_memory_space_constraint(args[place], pltpu.VMEM)
    return pl.pallas_call(
        kernel,
        out_shape=outs,
        in_specs=specs,
        out_specs=tuple(pl.BlockSpec(memory_space=pltpu.VMEM) for _ in outs),
        scratch_shapes=list(scratch),
        input_output_aliases=aliases,
        compiler_params=pltpu.CompilerParams(vmem_limit_bytes=32 * 1024 * 1024),
    )(*args)


def shape(dims, dtype=BF):
    return jax.ShapeDtypeStruct(tuple(dims), dtype)


AXES = ("phi", "eta")


def moves(n_phi, n_eta, rule):
    found = []
    for p in range(n_phi):
        for s in range(n_eta):
            step, t = rule(p, s)
            if 0 <= t < n_eta:
                found.append((p * n_eta + s, (p + step) % n_phi * n_eta + t))
    return found


def gather_pair(f_own, c_own, c_sent, near, far):
    n_phi = lax.axis_size("phi")

    def send(value, rule):
        return lax.ppermute(value, AXES, moves(n_phi, 2, rule))

    far = send(far, lambda p, s: (2 * s - 1, 1 - s))
    near = send(near, lambda p, s: (1 - 2 * s, s))
    f_other = send(f_own, lambda p, s: (0, 1 - s))
    c_other = send(c_sent, lambda p, s: (0, 1 - s))
    return [f_own, f_other, near, far], [c_own, c_other, near, far]


def gather_window(f_own, c_own, low, high):
    n_phi = lax.axis_size("phi")
    n_eta = lax.axis_size("eta")
    f_pieces = []
    c_pieces = []
    for step in window_steps(n_eta):
        send = lambda value, move: lax.ppermute(value, AXES, moves(n_phi, n_eta, lambda p, s: (move, s - step)))
        rims = [send(high, 1), send(low, -1)]
        f_pieces += [f_own if step == 0 else send(f_own, 0)] + rims
        c_pieces += [c_own if step == 0 else send(c_own, 0)] + rims
    return f_pieces, c_pieces


def window_steps(n_eta):
    return [0] if n_eta == 1 else [0, -1, 1, -2, 2]


def window_meta(n_eta, cells):
    e = lax.axis_index("eta")
    steps = window_steps(n_eta)
    middle = len(steps) // 2
    values = [middle + step for step in steps]
    values += [jnp.maximum(0, middle - e) * cells, jnp.minimum(len(steps), n_eta + middle - e) * cells]
    return jnp.stack([jnp.asarray(v, jnp.int32) for v in values])


def shards(features, cotangent, kernel_a, kernel_b, mixing):
    c1, n_rows, cells = features.shape
    c2 = kernel_b.shape[1]
    nb = n_rows // PB
    width = PB * c1
    n_eta = lax.axis_size("eta")
    paired = n_eta == 2 and nb % 4 == 0
    block = (cells, width)
    f_own, c_own, first, second, *c_sent = call(
        functools.partial(pre_kernel, paired),
        tuple(pltpu.VMEM((n,) + block, BF) for n in (nb, nb, 3, 3) + ((nb // 2 + 1,) if paired else ())),
        features,
        cotangent,
        scratch=(
            pltpu.VMEM(features.shape, BF),
            pltpu.VMEM(features.shape, BF),
            pltpu.SemaphoreType.DMA((2,)),
        ),
        far=(0, 1),
    )
    if paired:
        f_pieces, c_pieces = gather_pair(f_own, c_own, c_sent[0], first, second)
        meta = []
        nbx = nb // 2 + 4
        rows = 2 * cells
    else:
        f_pieces, c_pieces = gather_window(f_own, c_own, first, second)
        meta = [window_meta(n_eta, cells)]
        nbx = nb + 4
        rows = len(window_steps(n_eta)) * cells
    wa, waf, wb, wbf, mp, mt, pool, up = call(
        weights_kernel,
        (
            pltpu.VMEM((3 * 2 * width, 3 * width), BF),
            pltpu.VMEM((3 * 2 * width, 3 * width), BF),
            pltpu.VMEM((3 * 2 * width, 3 * PB * c2), BF),
            pltpu.VMEM((3 * 6 * c2, 3 * width), BF),
            pltpu.VMEM((PB * c2, width), BF),
            pltpu.VMEM((width, PB * c2), BF),
            pltpu.VMEM((4 * width, width), BF),
            pltpu.VMEM((width, 2 * width), BF),
        ),
        kernel_a,
        jnp.swapaxes(kernel_b, 1, 2),
        mixing,
        scratch=(
            pltpu.VMEM((27 * c1, width), F32),
            pltpu.VMEM((27 * c1, width), F32),
            pltpu.VMEM((27 * c1, PB * c2), F32),
            pltpu.VMEM((27 * c2, width), F32),
            pltpu.VMEM(kernel_a.shape, BF),
            pltpu.VMEM((27, c1, c2), BF),
            pltpu.VMEM(mixing.shape, BF),
            pltpu.SemaphoreType.DMA((3,)),
        ),
        far=(0, 1, 2),
    )
    nc = nbx // 2 - 1
    rows_c = rows // 2
    devices = lax.axis_size("phi") * n_eta
    lanes = 28 * c1
    total_rows = (c1 + c2) * lanes // 128
    chunk = next(d for d in range(8, c1 + c2 + 1, 8) if (c1 + c2) % d == 0 and total_rows <= d * devices)
    tall = rows + 2 * LAYERS
    tall_c = rows_c + 2 * LAYERS
    skip = len(meta)
    count = len(f_pieces)
    matrices = (wa, wb, mp, pool)
    fine = (
        pltpu.VMEM((nbx, tall, 2 * width), BF),
        pltpu.VMEM((nbx, rows, width), BF),
        pltpu.VMEM((nbx, rows, width), F32),
    )
    pooled = (
        pltpu.VMEM((nc + 2, tall_c, 2 * width), BF),
        pltpu.VMEM((nc, rows_c, PB * c2), BF),
        pltpu.VMEM((nc, rows_c, PB * c2), F32),
        pltpu.VMEM((nc, rows_c, width), BF),
    )
    between = lambda n: (pltpu.VMEM((n, tall, 2 * width), BF),)
    if paired:
        started = call(chunk_kernel, fine, *f_pieces[:2], wa, scratch=between(nbx - 3), near=range(3))
        args = (*f_pieces[2:], *started, *matrices)
        extra = {"near": range(len(args)), "aliases": {2: 0, 3: 1, 4: 2}}
    else:
        args = (*meta, *f_pieces, *matrices)
        extra = {"near": range(skip + 1, len(args)), "smem": skip}
    fz, hid, slope, cz, gat, slope_b, proj = call(
        functools.partial(forward_kernel, paired, 2 if paired else count),
        fine + pooled,
        *args,
        scratch=between(2 if paired else nbx - 1),
        **extra,
    )
    inner = (fz, slope, cz, gat, slope_b, wbf, mt, pool, up)
    gz, terms = call(
        functools.partial(backward_kernel, paired, count),
        (pltpu.VMEM((nbx, tall, 2 * width), BF), pltpu.VMEM((devices, chunk, 128), BF)),
        *meta,
        *c_pieces,
        *inner,
        scratch=(
            pltpu.VMEM((nbx, rows, width), BF),
            pltpu.VMEM((nc, tall_c, PB * c2 + width), BF),
            pltpu.VMEM((nc, rows_c, width), BF),
            pltpu.VMEM((3 * width, 6 * width), F32),
            pltpu.VMEM((3 * PB * c2, 6 * width), F32),
            pltpu.VMEM((c1 + c2, lanes), F32),
        ),
        smem=skip,
        near=range(skip + 1, skip + count + len(inner)),
    )
    terms = lax.all_to_all(terms, AXES, 0, 0, tiled=True)
    blocks = 2 * (nbx - 4)
    results = call(
        functools.partial(finish_kernel, paired),
        (pltpu.VMEM((blocks, width, cells), BF),) * (2 if paired else 1),
        *meta,
        gz,
        hid,
        proj,
        waf,
        up,
        scratch=(pltpu.VMEM((blocks, rows if paired else cells, width), F32),),
        smem=skip,
        near=range(skip, skip + 5),
    )
    if paired:
        kept, sent = results
        received = lax.ppermute(sent, AXES, moves(lax.axis_size("phi"), 2, lambda p, s: (0, 1 - s)))
        terms, kept = lax.optimization_barrier((terms, kept))
        output, grad_input = call(
            restore_kernel, (shape(features.shape), shape(features.shape)), kept, received, near=(0, 1)
        )
    else:
        output, grad_input = (
            jnp.transpose(part.reshape(n_rows, c1, cells), (1, 0, 2)) for part in (results[0][:nb], results[0][nb:])
        )
    (sums,) = call(sum_kernel, (pltpu.VMEM(terms.shape, BF),), terms, near=(0,))
    sums = lax.all_to_all(sums, AXES, 0, 0, tiled=True)
    cell_count = n_rows * cells * devices
    grad_a, grad_b, grad_mix = call(
        functools.partial(post_kernel, 1.0 / math.sqrt(cell_count)),
        (shape((27, c1, c1), F32), shape((27, c1, c2), F32), shape((c1, c2), F32)),
        sums,
        scratch=(pltpu.VMEM((c1 + c2, lanes), F32),),
        near=(0,),
    )
    return output, grad_input, grad_a, jnp.swapaxes(grad_b, 1, 2), grad_mix


def solution(mesh):
    in_specs = (P(None, "phi", "eta"), P(None, "phi", "eta"), P(), P(), P())
    out_specs = (P(None, "phi", "eta"), P(None, "phi", "eta"), P(), P(), P())

    return jax.shard_map(shards, mesh=mesh, in_specs=in_specs, out_specs=out_specs, check_vma=False)
```

```python
import functools
import math

import jax
import jax.numpy as jnp
from jax import lax
from jax.experimental import pallas as pl
from jax.experimental.pallas import tpu as pltpu
from jax.sharding import PartitionSpec as P


LAYERS = 32
PB = 4
BF = jnp.bfloat16
F32 = jnp.float32


def iota(shape, dim):
    return lax.broadcasted_iota(jnp.int32, shape, dim)


def dot(a, b):
    return jnp.dot(a, b, preferred_element_type=F32)


def dot_rows(a, b):
    return lax.dot_general(a, b, (((0,), (0,)), ((), ())), preferred_element_type=F32)


def fetch(sources, places, sems):
    moves = [pltpu.make_async_copy(src, dst, sems.at[i]) for i, (src, dst) in enumerate(zip(sources, places))]
    for move in moves:
        move.start()
    return moves


def pre_kernel(paired, f_hbm, c_hbm, f_own, c_own, first, second, *rest):
    f_ref, c_ref, sems = rest[-3:]
    nb = f_own.shape[0]
    moves = fetch((f_hbm, c_hbm), (f_ref, c_ref), sems)
    for move, ref, own in zip(moves, (f_ref, c_ref), (f_own, c_own)):
        move.wait()
        ch, _, cells = ref.shape
        swapped = jnp.swapaxes(ref[...].astype(F32), 0, 1)
        for j in range(nb):
            own[j] = swapped[PB * j : PB * (j + 1)].reshape(PB * ch, cells).T.astype(BF)
    e = lax.axis_index("eta") if paired else 1
    for rim, low in ((first, e), (second, 1 - e)):
        for j in range(2):
            rim[j] = f_own[(nb - 2) * (1 - low) + j]
        rim[2] = c_own[(nb - 1) * (1 - low)]
    if paired:
        partner = rest[0]
        for j in range(partner.shape[0]):
            partner[j] = c_own[(1 - e) * (nb // 2 - 1) + j]


def copies(size, times):
    shape = (size, size * times)
    return jnp.where(iota(shape, 0) == iota(shape, 1) % size, 1.0, 0.0).astype(BF)


def weights_kernel(
    ka_hbm, kbt_hbm, mix_hbm, wa, waf, wb, wbf, mp, mt, pool, up, ta, taf, tb, tbf, ka, kbt, mix, sems
):
    for move in fetch((ka_hbm, kbt_hbm, mix_hbm), (ka, kbt, mix), sems):
        move.wait()
    c1 = ka.shape[1]
    c2 = kbt.shape[2]
    width = PB * c1
    wide = PB * c2

    def flat(block):
        return block.reshape(-1, block.shape[2])

    def turned(ref):
        return jnp.swapaxes(ref[...].astype(F32), 1, 2).astype(BF)

    few = copies(c1, PB)
    many = copies(c2, PB)
    ta[...] = dot(flat(turned(ka)), few)
    taf[...] = dot(flat(ka[...]), few)
    tb[...] = dot(flat(kbt[...]), many)
    tbf[...] = dot(flat(turned(kbt)), few)

    def toeplitz(out, source, order, rows_per, cols_per, row_blocks, turn=0):
        height = len(row_blocks) * rows_per
        across = PB * cols_per
        place = iota((rows_per, across), 1) // cols_per
        for b in range(3):
            for c in range(3):
                for at, q in enumerate(row_blocks):
                    value = jnp.zeros((rows_per, across), F32)
                    for a in range(3):
                        p = q + 1 - a
                        if 0 <= p < PB:
                            t = order(9 * a + 3 * b + c) * rows_per
                            value = jnp.where(place == (p + turn) % PB, source[t : t + rows_per], value)
                    first = b * height + at * rows_per
                    out[first : first + rows_per, c * across : (c + 1) * across] = value.astype(BF)

    ring = (0, 1, 2, 3, 4, 100, 100, -1)
    toeplitz(wa, ta, lambda t: t, c1, c1, (2, 3, 0, 1, 100, -1, 4, 100), PB // 2)
    toeplitz(wb, tb, lambda t: t, c1, c2, ring)
    toeplitz(wbf, tbf, lambda t: 26 - t, c2, c1, (0, 1, 2, 3, 4, -1))
    toeplitz(waf, taf, lambda t: 26 - t, c1, c1, ring)
    mixing = mix[...]
    spread = dot(mixing, many)
    spread_t = dot(mixing.astype(F32).T.astype(BF), few)
    for p in range(PB):
        inside = iota((c1, wide), 1) // c2 == p
        mt[p * c1 : (p + 1) * c1] = jnp.where(inside, spread, 0.0).astype(BF)
        inside = iota((c2, width), 1) // c1 == p
        mp[p * c2 : (p + 1) * c2] = jnp.where(inside, spread_t, 0.0).astype(BF)
    r = iota(pool.shape, 0)
    l = iota(pool.shape, 1)
    hit = (r % c1 == l % c1) & (r // (2 * width) * 2 + r % width // c1 // 2 == l // c1)
    pool[...] = jnp.where(hit, 1.0, 0.0).astype(BF)
    r = iota(up.shape, 0)
    l = iota(up.shape, 1)
    hit = (r % c1 == l % c1) & (l // width * 2 + l % width // c1 // 2 == r // c1)
    up[...] = jnp.where(hit, 1.0, 0.0).astype(BF)


def combine(summed, width):
    rows = summed.shape[0]
    layer = iota((rows, width), 0) % LAYERS
    below = pltpu.roll(summed[:, :width], 1, 0)
    above = pltpu.roll(summed[:, 2 * width :], rows - 1, 0)
    return (
        summed[:, width : 2 * width]
        + jnp.where(layer == 0, 0.0, below)
        + jnp.where(layer == LAYERS - 1, 0.0, above)
    )


def layer_shifts(block):
    rows, width = block.shape
    layer = iota((rows, width), 0) % LAYERS
    wide = block.astype(F32)
    first = jnp.where(layer == LAYERS - 1, 0.0, pltpu.roll(wide, rows - 1, 0))
    last = jnp.where(layer == 0, 0.0, pltpu.roll(wide, 1, 0))
    return jnp.concatenate([first.astype(BF), block, last.astype(BF)], axis=1)


def taps(ref, j, start, rows):
    parts = []
    for b in range(3):
        at = start + b * LAYERS
        if not isinstance(at, int):
            at = pl.multiple_of(at, LAYERS)
        parts.append(ref[j, pl.ds(at, rows), :])
    return jnp.concatenate(parts, axis=1)


def every_other(block, which):
    count = block.shape[0] // (2 * LAYERS)
    return [block[(2 * i + which) * LAYERS : (2 * i + which + 1) * LAYERS] for i in range(count)]


def paired_rows(first, second):
    parts = []
    for block in (first, second):
        for which in range(2):
            parts.append(jnp.concatenate(every_other(block, which), axis=0))
    return jnp.concatenate(parts, axis=1)


def widen_rows(block):
    parts = []
    for i in range(block.shape[0] // LAYERS):
        part = block[i * LAYERS : (i + 1) * LAYERS]
        parts += [part, part]
    return jnp.concatenate(parts, axis=0)


def sigmoid(v):
    return 1.0 / (1.0 + jnp.exp(-v))


def edges(ref, first, last, inner, width, split):
    lane = iota((inner, width), 1)
    at = slice(LAYERS, LAYERS + inner)
    main = ref.shape[2] - width
    for j in range(first, last):
        nxt = ref[j + 1, at, :width] if j + 1 < ref.shape[0] else jnp.zeros((inner, width), BF)
        prv = ref[j - 1, at, main - width : main] if j > 0 else jnp.zeros((inner, width), BF)
        ref[j, at, main:] = jnp.where(lane < split, nxt, prv)


def blank_rims(ref):
    pad = jnp.zeros((LAYERS, ref.shape[2]), BF)
    for j in range(ref.shape[0]):
        ref[j, :LAYERS, :] = pad
        ref[j, ref.shape[1] - LAYERS :, :] = pad


def keep_inside(meta, shards_seen, value, scale):
    if meta is None or shards_seen == 1:
        return value
    r = iota(value.shape, 0)
    inside = (r >= meta[shards_seen] // scale) & (r < meta[shards_seen + 1] // scale)
    return jnp.where(inside, value, jnp.zeros_like(value))


def forward_block(place, j, fz, half_way, hid, slope, wa):
    rows, width = hid.shape[1:]
    half = width // 2
    at = slice(LAYERS, LAYERS + rows)
    left = iota((rows, width), 1) < half
    low, high = fz[j, at, :width], fz[j + 1, at, :width]
    half_way[place, at, :width] = jnp.where(left, high, low)
    half_way[place, at, width:] = jnp.where(left, low, high)
    linear = combine(dot(taps(half_way, place, 0, rows), wa[...]), width)
    logistic = sigmoid(linear)
    hidden = (linear * logistic).astype(BF)
    steep = logistic * (1.0 + linear * (1.0 - logistic))
    for ref, value in ((hid, hidden), (slope, steep)):
        ref[j + 1, :, :half] = value[:, :half]
        ref[j, :, half:] = value[:, half:]


def blank_ends(hid):
    rows, width = hid.shape[1:]
    none = jnp.zeros((rows, width // 2), BF)
    hid[0, :, : width // 2] = none
    hid[hid.shape[0] - 1, :, width // 2 :] = none


def chunk_kernel(own, partner, wa, fz, hid, slope, half_way):
    nbx = fz.shape[0]
    nb, cells, width = own.shape
    e = lax.axis_index("eta")
    blank_rims(fz)
    blank_rims(half_way)
    blank_ends(hid)
    for chunk, shard in ((own, e), (partner, 1 - e)):
        at = pl.multiple_of(LAYERS + shard * cells, LAYERS)
        for j in range(nb // 2 + 2):
            fz[j + 2 * (1 - e), pl.ds(at, cells), :width] = chunk[j + e * (nb // 2 - 2)]
    for j in range(nbx - 3):
        forward_block(j, 2 * (1 - e) + j, fz, half_way, hid, slope, wa)


def forward_kernel(paired, count, *refs):
    meta = None
    if not paired:
        meta, refs = refs[0], refs[1:]
    pieces, refs = refs[:count], refs[count:]
    if paired:
        refs = refs[3:]
    wa, wb, mp, pool = refs[:4]
    fz, hid, slope, cz, gat, slope_b, proj, half_way = refs[4:]
    nbx = fz.shape[0]
    nc = gat.shape[0]
    rows = hid.shape[1]
    rows_c = rows // 2
    width = hid.shape[2]
    c1 = width // PB
    wide = gat.shape[2]
    blank_rims(cz)
    blank_rims(half_way)
    cells = pieces[0].shape[1]
    if paired:
        near, far = pieces
        e = lax.axis_index("eta")
        for rim, shard in ((near, e), (far, 1 - e)):
            at = pl.multiple_of(LAYERS + shard * cells, LAYERS)
            for j in range(2):
                fz[e * (nbx - 2) + j, pl.ds(at, cells), :width] = rim[j]
        for j in range(2):
            forward_block(j, e * (nbx - 3) + j, fz, half_way, hid, slope, wa)
    else:
        blank_rims(fz)
        blank_ends(hid)
        for s in range(count // 3):
            middle, before, after = pieces[3 * s : 3 * s + 3]
            at = pl.multiple_of(LAYERS + meta[s] * cells, LAYERS)
            for j in range(2):
                fz[j, pl.ds(at, cells), :width] = before[j]
                fz[nbx - 2 + j, pl.ds(at, cells), :width] = after[j]
            for j in range(nbx - 4):
                fz[2 + j, pl.ds(at, cells), :width] = middle[j]
        for j in range(nbx - 1):
            forward_block(j, j, fz, half_way, hid, slope, wa)
    edges(fz, 2, nbx - 2, rows, width, 3 * c1)
    for j in range(nc + 2):
        start, end = max(2 * j - 1, 0), min(2 * j, nbx - 1)
        pooled = dot(paired_rows(hid[start], hid[end]), pool[...]) * 0.25
        cz[j, LAYERS : LAYERS + rows_c, :width] = keep_inside(meta, count // 3, pooled.astype(BF), 2)
    edges(cz, 1, nc + 1, rows_c, width, 3 * c1)
    for j in range(nc):
        linear = combine(dot(taps(cz, j + 1, 0, rows_c), wb[...]), wide)
        logistic = sigmoid(linear)
        gated = (linear * logistic).astype(BF)
        gat[j] = gated
        slope_b[j] = logistic * (1.0 + linear * (1.0 - logistic))
        proj[j] = dot(gated, mp[...]).astype(BF)


def backward_kernel(paired, count, *refs):
    meta = None
    if not paired:
        meta, refs = refs[0], refs[1:]
    pieces, refs = refs[:count], refs[count:]
    fz, slope, cz, gat, slope_b, wbf, mt, pool, up = refs[:9]
    gz, pk_ref = refs[9:11]
    cot, gb, fold, acc_a, acc_b, packed = refs[11:]
    nbx = fz.shape[0]
    nb = nbx - 4
    nc = gat.shape[0]
    rows = cot.shape[1]
    rows_c = rows // 2
    width = cot.shape[2]
    wide = gat.shape[2]
    c1 = width // PB
    c2 = wide // PB
    cells = pieces[0].shape[1]
    blank_rims(gz)
    blank_rims(gb)
    if paired:
        own, partner, near, far = pieces
        e = lax.axis_index("eta")
        for rim, shard in ((near, e), (far, 1 - e)):
            at = pl.multiple_of(shard * cells, cells)
            cot[1 + e * (nbx - 3), pl.ds(at, cells), :] = rim[2]
            for j in range(partner.shape[0]):
                if rim is near:
                    block = own[j + e * (own.shape[0] // 2 - 1)]
                else:
                    block = partner[j]
                cot[j + 2 - e, pl.ds(at, cells), :] = block
        own, own_at, own_at_c = rows, 0, 0
    else:
        for s in range(count // 3):
            middle, before, after = pieces[3 * s : 3 * s + 3]
            at = pl.multiple_of(meta[s] * cells, cells)
            cot[1, pl.ds(at, cells), :] = before[2]
            cot[nbx - 2, pl.ds(at, cells), :] = after[2]
            for j in range(nb):
                cot[2 + j, pl.ds(at, cells), :] = middle[j]
        own = cells
        own_at = pl.multiple_of(meta[0] * own, own)
        own_at_c = pl.multiple_of(meta[0] * (own // 2), own // 2)
    own_c = own // 2

    for j in range(nc):
        fold[j] = dot(paired_rows(cot[2 * j + 1], cot[2 * j + 2]), pool[...]).astype(BF)
        grad = dot(fold[j], mt[...]) * slope_b[j]
        gb[j, LAYERS : LAYERS + rows_c, :wide] = keep_inside(meta, count // 3, grad.astype(BF), 2)
    edges(gb, 0, nc, rows_c, width, c2)
    for j in range(nc):
        grad = combine(dot(taps(gb, j, 0, rows_c), wbf[...]), width).astype(BF)
        spread = 0.25 * dot(grad, up[...])
        for k in range(2):
            f = 2 * j + 1 + k
            total = cot[f].astype(F32) + widen_rows(spread[:, k * width : (k + 1) * width])
            value = (total * slope[f]).astype(BF)
            gz[f, LAYERS : LAYERS + rows, :width] = keep_inside(meta, count // 3, value, 1)
    edges(gz, 2, nbx - 2, rows, width, 3 * c1)

    def own_half(value, j):
        p = iota(value.shape, 1) // (value.shape[1] // PB)
        if j == 0:
            value = jnp.where(p >= PB // 2, value, jnp.zeros_like(value))
        if j == nc - 1:
            value = jnp.where(p < PB // 2, value, jnp.zeros_like(value))
        return value

    lhs = jnp.concatenate(
        [layer_shifts(gz[2 + j, pl.ds(LAYERS + own_at, own), :width]) for j in range(nb)], axis=0
    )
    rhs = jnp.concatenate([taps(fz, 2 + j, own_at, own) for j in range(nb)], axis=0)
    acc_a[...] = dot_rows(lhs, rhs)
    lhs = jnp.concatenate(
        [layer_shifts(own_half(gb[j, pl.ds(LAYERS + own_at_c, own_c), :wide], j)) for j in range(nc)], axis=0
    )
    rhs = jnp.concatenate([taps(cz, j + 1, own_at_c, own_c) for j in range(nc)], axis=0)
    acc_b[...] = dot_rows(rhs, lhs)
    lhs = jnp.concatenate([gat[j, pl.ds(own_at_c, own_c), :] for j in range(nc)], axis=0)
    rhs = jnp.concatenate([own_half(fold[j, pl.ds(own_at_c, own_c), :], j) for j in range(nc)], axis=0)
    mixed = dot_rows(rhs, lhs)
    mix_sum = mixed[:c1, :c2]
    for p in range(1, PB):
        mix_sum = mix_sum + mixed[p * c1 : (p + 1) * c1, p * c2 : (p + 1) * c2]
    first_b, first_mix = places_of(c1, c2)
    packed[:, first_mix : first_mix + c2] = mix_sum
    packed[:, 27 * c1 : first_b] = jnp.zeros((c1, first_b - 27 * c1), F32)
    span = 2 * width
    for b in range(3):
        for c in range(3):
            total = None
            for p in range(PB):
                at = (c * PB + p) * c1
                part = acc_a[at : at + c1, b * span : (b + 1) * span]
                part = pltpu.roll(part, (span - (p - 1) * c1) % span, 1)
                total = part if total is None else total + part
            for a in range(3):
                t = 9 * a + 3 * b + c
                packed[:, t * c1 : (t + 1) * c1] = total[:, a * c1 : (a + 1) * c1]
    for t in range(27):
        a, b, c = t // 9, t // 3 % 3, t % 3
        sides = [None, None]
        for p in range(PB):
            at = b * span + (p + a - 1) % (2 * PB) * c1
            lanes = c * wide + p // 2 * 2 * c2
            part = acc_b[at : at + c1, lanes : lanes + 2 * c2]
            sides[p % 2] = part if sides[p % 2] is None else sides[p % 2] + part
        total = sides[t % 2] + pltpu.roll(sides[1 - t % 2], c2, 1)
        lanes = first_b + t * c2
        packed[:, lanes : lanes + c2] = total[:, t % 2 * c2 : (t % 2 + 1) * c2]
    step = pk_ref.shape[1] // 8
    pieces8 = packed.shape[0] // 8
    used = packed.shape[1] // 128 * pieces8
    for n in range(pk_ref.shape[0] * step):
        at = slice(n % step * 8, n % step * 8 + 8)
        if n < used:
            v, k = n // pieces8, n % pieces8
            pk_ref[n // step, at] = packed[8 * k : 8 * k + 8, v * 128 : (v + 1) * 128].astype(BF)
        else:
            pk_ref[n // step, at] = jnp.zeros((8, 128), BF)


def places_of(c1, c2):
    first_b = -(-27 * c1 // 128) * 128
    return first_b, first_b + 27 * c2


def finish_kernel(paired, *refs):
    meta = None
    if not paired:
        meta, refs = refs[0], refs[1:]
    gz, hid, proj, waf, up = refs[:5]
    outs = refs[5:-1]
    buf = refs[-1]
    nb = gz.shape[0] - 4
    width = hid.shape[2]
    cells = outs[0].shape[2]
    if paired:
        own, own_at, own_at_c = hid.shape[1], 0, 0
        e = lax.axis_index("eta")
        starts = [pl.multiple_of(e * cells, cells), pl.multiple_of((1 - e) * cells, cells)]
    else:
        own = cells
        own_at = pl.multiple_of(meta[0] * own, own)
        own_at_c = pl.multiple_of(meta[0] * (own // 2), own // 2)
        starts = [0]

    def write(value, place):
        buf[place] = value
        for out, start in zip(outs, starts):
            out[place] = buf[place, pl.ds(start, cells), :].T.astype(BF)

    for j in range(nb):
        grad = combine(dot(taps(gz, 2 + j, own_at, own), waf[...]), width)
        write(grad, nb + j)
    for j in range(nb):
        k = (j + 1) % 2
        spread = dot(proj[(j + 1) // 2, pl.ds(own_at_c, own // 2), :], up[:, k * width : (k + 1) * width])
        write(hid[2 + j, pl.ds(own_at, own), :].astype(F32) + widen_rows(spread), j)


def restore_kernel(kept, received, out_ref, gin_ref):
    ch, rows, cells = out_ref.shape
    half = rows // 2
    e = lax.axis_index("eta")
    for k, ref in enumerate((out_ref, gin_ref)):
        at = k * half // PB
        mine = kept[at : at + half // PB].astype(F32)
        other = received[at : at + half // PB].astype(F32)
        first = jnp.where(e == 0, mine, other).reshape(half, ch, cells)
        second = jnp.where(e == 0, other, mine).reshape(half, ch, cells)
        ref[...] = jnp.swapaxes(jnp.concatenate([first, second], axis=0), 0, 1).astype(BF)


def sum_kernel(x_ref, o_ref):
    total = jnp.sum(x_ref[...].astype(F32), axis=0).astype(BF)
    o_ref[...] = jnp.broadcast_to(total[None], o_ref.shape)


def post_kernel(factor, x_ref, ga_ref, gb_ref, gm_ref, buf):
    step = x_ref.shape[1] // 8
    pieces8 = buf.shape[0] // 8
    c1, c2 = gm_ref.shape
    for n in range(buf.shape[1] // 128 * pieces8):
        v, k = n // pieces8, n % pieces8
        part = x_ref[n // step, n % step * 8 : n % step * 8 + 8]
        buf[8 * k : 8 * k + 8, v * 128 : (v + 1) * 128] = part.astype(F32) * factor
    first_b, first_mix = places_of(c1, c2)
    for t in range(27):
        ga_ref[t] = buf[:, t * c1 : (t + 1) * c1]
        gb_ref[t] = buf[:, first_b + t * c2 : first_b + (t + 1) * c2]
    gm_ref[...] = buf[:, first_mix : first_mix + c2]


def call(kernel, outs, *args, scratch=(), smem=0, near=(), far=(), aliases={}):
    args = list(args)
    specs = []
    for place in range(len(args)):
        if place < smem:
            specs.append(pl.BlockSpec(memory_space=pltpu.SMEM))
        elif place in far:
            specs.append(pl.BlockSpec(memory_space=pl.ANY))
            args[place] = pltpu.with_memory_space_constraint(args[place], pltpu.HBM)
        else:
            specs.append(pl.BlockSpec(memory_space=pltpu.VMEM))
            if place in near:
                args[place] = pltpu.with_memory_space_constraint(args[place], pltpu.VMEM)
    return pl.pallas_call(
        kernel,
        out_shape=outs,
        in_specs=specs,
        out_specs=tuple(pl.BlockSpec(memory_space=pltpu.VMEM) for _ in outs),
        scratch_shapes=list(scratch),
        input_output_aliases=aliases,
        compiler_params=pltpu.CompilerParams(vmem_limit_bytes=32 * 1024 * 1024),
    )(*args)


def shape(dims, dtype=BF):
    return jax.ShapeDtypeStruct(tuple(dims), dtype)


AXES = ("phi", "eta")


def moves(n_phi, n_eta, rule):
    found = []
    for p in range(n_phi):
        for s in range(n_eta):
            step, t = rule(p, s)
            if 0 <= t < n_eta:
                found.append((p * n_eta + s, (p + step) % n_phi * n_eta + t))
    return found


def gather_pair(f_own, c_own, c_sent, near, far):
    n_phi = lax.axis_size("phi")

    def send(value, rule):
        return lax.ppermute(value, AXES, moves(n_phi, 2, rule))

    far = send(far, lambda p, s: (2 * s - 1, 1 - s))
    near = send(near, lambda p, s: (1 - 2 * s, s))
    f_other = send(f_own, lambda p, s: (0, 1 - s))
    c_other = send(c_sent, lambda p, s: (0, 1 - s))
    return [f_own, f_other, near, far], [c_own, c_other, near, far]


def gather_window(f_own, c_own, low, high):
    n_phi = lax.axis_size("phi")
    n_eta = lax.axis_size("eta")
    f_pieces = []
    c_pieces = []
    for step in window_steps(n_eta):
        send = lambda value, move: lax.ppermute(value, AXES, moves(n_phi, n_eta, lambda p, s: (move, s - step)))
        rims = [send(high, 1), send(low, -1)]
        f_pieces += [f_own if step == 0 else send(f_own, 0)] + rims
        c_pieces += [c_own if step == 0 else send(c_own, 0)] + rims
    return f_pieces, c_pieces


def window_steps(n_eta):
    return [0] if n_eta == 1 else [0, -1, 1, -2, 2]


def window_meta(n_eta, cells):
    e = lax.axis_index("eta")
    steps = window_steps(n_eta)
    middle = len(steps) // 2
    values = [middle + step for step in steps]
    values += [jnp.maximum(0, middle - e) * cells, jnp.minimum(len(steps), n_eta + middle - e) * cells]
    return jnp.stack([jnp.asarray(v, jnp.int32) for v in values])


def shards(features, cotangent, kernel_a, kernel_b, mixing):
    c1, n_rows, cells = features.shape
    c2 = kernel_b.shape[1]
    nb = n_rows // PB
    width = PB * c1
    n_eta = lax.axis_size("eta")
    paired = n_eta == 2 and nb % 4 == 0
    block = (cells, width)
    f_own, c_own, first, second, *c_sent = call(
        functools.partial(pre_kernel, paired),
        tuple(pltpu.VMEM((n,) + block, BF) for n in (nb, nb, 3, 3) + ((nb // 2 + 1,) if paired else ())),
        features,
        cotangent,
        scratch=(
            pltpu.VMEM(features.shape, BF),
            pltpu.VMEM(features.shape, BF),
            pltpu.SemaphoreType.DMA((2,)),
        ),
        far=(0, 1),
    )
    if paired:
        f_pieces, c_pieces = gather_pair(f_own, c_own, c_sent[0], first, second)
        meta = []
        nbx = nb // 2 + 4
        rows = 2 * cells
    else:
        f_pieces, c_pieces = gather_window(f_own, c_own, first, second)
        meta = [window_meta(n_eta, cells)]
        nbx = nb + 4
        rows = len(window_steps(n_eta)) * cells
    wa, waf, wb, wbf, mp, mt, pool, up = call(
        weights_kernel,
        (
            pltpu.VMEM((3 * 2 * width, 3 * width), BF),
            pltpu.VMEM((3 * 2 * width, 3 * width), BF),
            pltpu.VMEM((3 * 2 * width, 3 * PB * c2), BF),
            pltpu.VMEM((3 * 6 * c2, 3 * width), BF),
            pltpu.VMEM((PB * c2, width), BF),
            pltpu.VMEM((width, PB * c2), BF),
            pltpu.VMEM((4 * width, width), BF),
            pltpu.VMEM((width, 2 * width), BF),
        ),
        kernel_a,
        jnp.swapaxes(kernel_b, 1, 2),
        mixing,
        scratch=(
            pltpu.VMEM((27 * c1, width), F32),
            pltpu.VMEM((27 * c1, width), F32),
            pltpu.VMEM((27 * c1, PB * c2), F32),
            pltpu.VMEM((27 * c2, width), F32),
            pltpu.VMEM(kernel_a.shape, BF),
            pltpu.VMEM((27, c1, c2), BF),
            pltpu.VMEM(mixing.shape, BF),
            pltpu.SemaphoreType.DMA((3,)),
        ),
        far=(0, 1, 2),
    )
    nc = nbx // 2 - 1
    rows_c = rows // 2
    devices = lax.axis_size("phi") * n_eta
    lanes = places_of(c1, c2)[1] + c2
    chunk = 8 * -(-c1 * lanes // (8 * 128 * devices))
    tall = rows + 2 * LAYERS
    tall_c = rows_c + 2 * LAYERS
    skip = len(meta)
    count = len(f_pieces)
    matrices = (wa, wb, mp, pool)
    fine = (
        pltpu.VMEM((nbx, tall, 2 * width), BF),
        pltpu.VMEM((nbx, rows, width), BF),
        pltpu.VMEM((nbx, rows, width), F32),
    )
    pooled = (
        pltpu.VMEM((nc + 2, tall_c, 2 * width), BF),
        pltpu.VMEM((nc, rows_c, PB * c2), BF),
        pltpu.VMEM((nc, rows_c, PB * c2), F32),
        pltpu.VMEM((nc, rows_c, width), BF),
    )
    between = lambda n: (pltpu.VMEM((n, tall, 2 * width), BF),)
    if paired:
        started = call(chunk_kernel, fine, *f_pieces[:2], wa, scratch=between(nbx - 3), near=range(3))
        args = (*f_pieces[2:], *started, *matrices)
        extra = {"near": range(len(args)), "aliases": {2: 0, 3: 1, 4: 2}}
    else:
        args = (*meta, *f_pieces, *matrices)
        extra = {"near": range(skip + 1, len(args)), "smem": skip}
    fz, hid, slope, cz, gat, slope_b, proj = call(
        functools.partial(forward_kernel, paired, 2 if paired else count),
        fine + pooled,
        *args,
        scratch=between(2 if paired else nbx - 1),
        **extra,
    )
    inner = (fz, slope, cz, gat, slope_b, wbf, mt, pool, up)
    gz, terms = call(
        functools.partial(backward_kernel, paired, count),
        (pltpu.VMEM((nbx, tall, 2 * width), BF), pltpu.VMEM((devices, chunk, 128), BF)),
        *meta,
        *c_pieces,
        *inner,
        scratch=(
            pltpu.VMEM((nbx, rows, width), BF),
            pltpu.VMEM((nc, tall_c, PB * c2 + width), BF),
            pltpu.VMEM((nc, rows_c, width), BF),
            pltpu.VMEM((3 * width, 6 * width), F32),
            pltpu.VMEM((3 * PB * c2, 6 * width), F32),
            pltpu.VMEM((c1, lanes), F32),
        ),
        smem=skip,
        near=range(skip + 1, skip + count + len(inner)),
    )
    terms = lax.all_to_all(terms, AXES, 0, 0, tiled=True)
    blocks = 2 * (nbx - 4)
    results = call(
        functools.partial(finish_kernel, paired),
        (pltpu.VMEM((blocks, width, cells), BF),) * (2 if paired else 1),
        *meta,
        gz,
        hid,
        proj,
        waf,
        up,
        scratch=(pltpu.VMEM((blocks, rows if paired else cells, width), F32),),
        smem=skip,
        near=range(skip, skip + 5),
    )
    if paired:
        kept, sent = results
        received = lax.ppermute(sent, AXES, moves(lax.axis_size("phi"), 2, lambda p, s: (0, 1 - s)))
        terms, kept = lax.optimization_barrier((terms, kept))
        output, grad_input = call(
            restore_kernel, (shape(features.shape), shape(features.shape)), kept, received, near=(0, 1)
        )
    else:
        output, grad_input = (
            jnp.transpose(part.reshape(n_rows, c1, cells), (1, 0, 2)) for part in (results[0][:nb], results[0][nb:])
        )
    (sums,) = call(sum_kernel, (pltpu.VMEM(terms.shape, BF),), terms, near=(0,))
    sums = lax.all_to_all(sums, AXES, 0, 0, tiled=True)
    cell_count = n_rows * cells * devices
    grad_a, grad_b, grad_mix = call(
        functools.partial(post_kernel, 1.0 / math.sqrt(cell_count)),
        (shape((27, c1, c1), F32), shape((27, c1, c2), F32), shape((c1, c2), F32)),
        sums,
        scratch=(pltpu.VMEM((c1, lanes), F32),),
        near=(0,),
    )
    return output, grad_input, grad_a, jnp.swapaxes(grad_b, 1, 2), grad_mix


def solution(mesh):
    in_specs = (P(None, "phi", "eta"), P(None, "phi", "eta"), P(), P(), P())
    out_specs = (P(None, "phi", "eta"), P(None, "phi", "eta"), P(), P(), P())

    return jax.shard_map(shards, mesh=mesh, in_specs=in_specs, out_specs=out_specs, check_vma=False)
```

```python
import functools
import math

import jax
import jax.numpy as jnp
from jax import lax
from jax.experimental import pallas as pl
from jax.experimental.pallas import tpu as pltpu
from jax.sharding import PartitionSpec as P


LAYERS = 32
PB = 4
BF = jnp.bfloat16
F32 = jnp.float32


def iota(shape, dim):
    return lax.broadcasted_iota(jnp.int32, shape, dim)


def dot(a, b):
    return jnp.dot(a, b, preferred_element_type=F32)


def dot_rows(a, b):
    return lax.dot_general(a, b, (((0,), (0,)), ((), ())), preferred_element_type=F32)


def fetch(sources, places, sems):
    moves = [pltpu.make_async_copy(src, dst, sems.at[i]) for i, (src, dst) in enumerate(zip(sources, places))]
    for move in moves:
        move.start()
    return moves


def pre_kernel(paired, f_hbm, c_hbm, f_own, c_own, first, second, *rest):
    f_ref, c_ref, sems = rest[-3:]
    nb = f_own.shape[0]
    moves = fetch((f_hbm, c_hbm), (f_ref, c_ref), sems)
    for move, ref, own in zip(moves, (f_ref, c_ref), (f_own, c_own)):
        move.wait()
        ch, _, cells = ref.shape
        swapped = jnp.swapaxes(ref[...].astype(F32), 0, 1)
        for j in range(nb):
            own[j] = swapped[PB * j : PB * (j + 1)].reshape(PB * ch, cells).astype(BF).T
    e = lax.axis_index("eta") if paired else 1
    for rim, low in ((first, e), (second, 1 - e)):
        for j in range(2):
            rim[j] = f_own[(nb - 2) * (1 - low) + j]
        rim[2] = c_own[(nb - 1) * (1 - low)]
    if paired:
        partner = rest[0]
        for j in range(partner.shape[0]):
            partner[j] = c_own[(1 - e) * (nb // 2 - 1) + j]


def copies(size, times):
    shape = (size, size * times)
    return jnp.where(iota(shape, 0) == iota(shape, 1) % size, 1.0, 0.0).astype(BF)


def weights_kernel(
    ka_hbm, kbt_hbm, mix_hbm, wa, waf, wb, wbf, mp, mt, pool, up, ta, taf, tb, tbf, ka, kbt, mix, sems
):
    for move in fetch((ka_hbm, kbt_hbm, mix_hbm), (ka, kbt, mix), sems):
        move.wait()
    c1 = ka.shape[1]
    c2 = kbt.shape[2]
    width = PB * c1
    wide = PB * c2

    def flat(block):
        return block.reshape(-1, block.shape[2])

    def turned(ref):
        return jnp.swapaxes(ref[...].astype(F32), 1, 2).astype(BF)

    few = copies(c1, PB)
    many = copies(c2, PB)
    ta[...] = dot(flat(turned(ka)), few)
    taf[...] = dot(flat(ka[...]), few)
    tb[...] = dot(flat(kbt[...]), many)
    tbf[...] = dot(flat(turned(kbt)), few)

    def toeplitz(out, source, order, rows_per, cols_per, row_blocks, turn=0):
        height = len(row_blocks) * rows_per
        across = PB * cols_per
        place = iota((rows_per, across), 1) // cols_per
        for b in range(3):
            for c in range(3):
                for at, q in enumerate(row_blocks):
                    value = jnp.zeros((rows_per, across), F32)
                    for a in range(3):
                        p = q + 1 - a
                        if 0 <= p < PB:
                            t = order(9 * a + 3 * b + c) * rows_per
                            value = jnp.where(place == (p + turn) % PB, source[t : t + rows_per], value)
                    first = b * height + at * rows_per
                    out[first : first + rows_per, c * across : (c + 1) * across] = value.astype(BF)

    ring = (0, 1, 2, 3, 4, 100, 100, -1)
    toeplitz(wa, ta, lambda t: t, c1, c1, (2, 3, 0, 1, 100, -1, 4, 100), PB // 2)
    toeplitz(wb, tb, lambda t: t, c1, c2, ring)
    toeplitz(wbf, tbf, lambda t: 26 - t, c2, c1, (0, 1, 2, 3, 4, -1))
    toeplitz(waf, taf, lambda t: 26 - t, c1, c1, ring)
    mixing = mix[...]
    spread = dot(mixing, many)
    spread_t = dot(mixing.astype(F32).T.astype(BF), few)
    for p in range(PB):
        inside = iota((c1, wide), 1) // c2 == p
        mt[p * c1 : (p + 1) * c1] = jnp.where(inside, spread, 0.0).astype(BF)
        inside = iota((c2, width), 1) // c1 == p
        mp[p * c2 : (p + 1) * c2] = jnp.where(inside, spread_t, 0.0).astype(BF)
    r = iota(pool.shape, 0)
    l = iota(pool.shape, 1)
    hit = (r % c1 == l % c1) & (r // (2 * width) * 2 + r % width // c1 // 2 == l // c1)
    pool[...] = jnp.where(hit, 1.0, 0.0).astype(BF)
    r = iota(up.shape, 0)
    l = iota(up.shape, 1)
    hit = (r % c1 == l % c1) & (l // width * 2 + l % width // c1 // 2 == r // c1)
    up[...] = jnp.where(hit, 1.0, 0.0).astype(BF)


def combine(summed, width):
    rows = summed.shape[0]
    layer = iota((rows, width), 0) % LAYERS
    below = pltpu.roll(summed[:, :width], 1, 0)
    above = pltpu.roll(summed[:, 2 * width :], rows - 1, 0)
    return (
        summed[:, width : 2 * width]
        + jnp.where(layer == 0, 0.0, below)
        + jnp.where(layer == LAYERS - 1, 0.0, above)
    )


def layer_shifts(block):
    rows, width = block.shape
    layer = iota((rows, width), 0) % LAYERS
    wide = block.astype(F32)
    first = jnp.where(layer == LAYERS - 1, 0.0, pltpu.roll(wide, rows - 1, 0))
    last = jnp.where(layer == 0, 0.0, pltpu.roll(wide, 1, 0))
    return jnp.concatenate([first.astype(BF), block, last.astype(BF)], axis=1)


def taps(ref, j, start, rows):
    parts = []
    for b in range(3):
        at = start + b * LAYERS
        if not isinstance(at, int):
            at = pl.multiple_of(at, LAYERS)
        parts.append(ref[j, pl.ds(at, rows), :])
    return jnp.concatenate(parts, axis=1)


def every_other(block, which):
    count = block.shape[0] // (2 * LAYERS)
    return [block[(2 * i + which) * LAYERS : (2 * i + which + 1) * LAYERS] for i in range(count)]


def paired_rows(first, second):
    parts = []
    for block in (first, second):
        for which in range(2):
            parts.append(jnp.concatenate(every_other(block, which), axis=0))
    return jnp.concatenate(parts, axis=1)


def widen_rows(block):
    parts = []
    for i in range(block.shape[0] // LAYERS):
        part = block[i * LAYERS : (i + 1) * LAYERS]
        parts += [part, part]
    return jnp.concatenate(parts, axis=0)


def sigmoid(v):
    return 1.0 / (1.0 + jnp.exp(-v))


def edges(ref, first, last, inner, width, split):
    lane = iota((inner, width), 1)
    at = slice(LAYERS, LAYERS + inner)
    main = ref.shape[2] - width
    for j in range(first, last):
        nxt = ref[j + 1, at, :width] if j + 1 < ref.shape[0] else jnp.zeros((inner, width), BF)
        prv = ref[j - 1, at, main - width : main] if j > 0 else jnp.zeros((inner, width), BF)
        ref[j, at, main:] = jnp.where(lane < split, nxt, prv)


def blank_rims(ref):
    pad = jnp.zeros((LAYERS, ref.shape[2]), BF)
    for j in range(ref.shape[0]):
        ref[j, :LAYERS, :] = pad
        ref[j, ref.shape[1] - LAYERS :, :] = pad


def keep_inside(meta, shards_seen, value, scale):
    if meta is None or shards_seen == 1:
        return value
    r = iota(value.shape, 0)
    inside = (r >= meta[shards_seen] // scale) & (r < meta[shards_seen + 1] // scale)
    return jnp.where(inside, value, jnp.zeros_like(value))


def forward_block(place, j, fz, half_way, hid, slope, wa):
    rows, width = hid.shape[1:]
    half = width // 2
    at = slice(LAYERS, LAYERS + rows)
    left = iota((rows, width), 1) < half
    low, high = fz[j, at, :width], fz[j + 1, at, :width]
    half_way[place, at, :width] = jnp.where(left, high, low)
    half_way[place, at, width:] = jnp.where(left, low, high)
    linear = combine(dot(taps(half_way, place, 0, rows), wa[...]), width)
    logistic = sigmoid(linear)
    hidden = (linear * logistic).astype(BF)
    steep = logistic * (1.0 + linear * (1.0 - logistic))
    for ref, value in ((hid, hidden), (slope, steep)):
        ref[j + 1, :, :half] = value[:, :half]
        ref[j, :, half:] = value[:, half:]


def blank_ends(hid):
    rows, width = hid.shape[1:]
    none = jnp.zeros((rows, width // 2), BF)
    hid[0, :, : width // 2] = none
    hid[hid.shape[0] - 1, :, width // 2 :] = none


def chunk_kernel(own, partner, wa, fz, hid, slope, half_way):
    nbx = fz.shape[0]
    nb, cells, width = own.shape
    e = lax.axis_index("eta")
    blank_rims(fz)
    blank_rims(half_way)
    blank_ends(hid)
    for chunk, shard in ((own, e), (partner, 1 - e)):
        at = pl.multiple_of(LAYERS + shard * cells, LAYERS)
        for j in range(nb // 2 + 2):
            fz[j + 2 * (1 - e), pl.ds(at, cells), :width] = chunk[j + e * (nb // 2 - 2)]
    for j in range(nbx - 3):
        forward_block(j, 2 * (1 - e) + j, fz, half_way, hid, slope, wa)


def forward_kernel(paired, count, *refs):
    meta = None
    if not paired:
        meta, refs = refs[0], refs[1:]
    pieces, refs = refs[:count], refs[count:]
    if paired:
        refs = refs[3:]
    wa, wb, pool = refs[:3]
    fz, hid, slope, cz, gat, slope_b, half_way = refs[3:]
    nbx = fz.shape[0]
    nc = gat.shape[0]
    rows = hid.shape[1]
    rows_c = rows // 2
    width = hid.shape[2]
    c1 = width // PB
    wide = gat.shape[2]
    blank_rims(cz)
    blank_rims(half_way)
    cells = pieces[0].shape[1]
    if paired:
        near, far = pieces
        e = lax.axis_index("eta")
        for rim, shard in ((near, e), (far, 1 - e)):
            at = pl.multiple_of(LAYERS + shard * cells, LAYERS)
            for j in range(2):
                fz[e * (nbx - 2) + j, pl.ds(at, cells), :width] = rim[j]
        for j in range(2):
            forward_block(j, e * (nbx - 3) + j, fz, half_way, hid, slope, wa)
    else:
        blank_rims(fz)
        blank_ends(hid)
        for s in range(count // 3):
            middle, before, after = pieces[3 * s : 3 * s + 3]
            at = pl.multiple_of(LAYERS + meta[s] * cells, LAYERS)
            for j in range(2):
                fz[j, pl.ds(at, cells), :width] = before[j]
                fz[nbx - 2 + j, pl.ds(at, cells), :width] = after[j]
            for j in range(nbx - 4):
                fz[2 + j, pl.ds(at, cells), :width] = middle[j]
        for j in range(nbx - 1):
            forward_block(j, j, fz, half_way, hid, slope, wa)
    edges(fz, 2, nbx - 2, rows, width, 3 * c1)
    for j in range(nc + 2):
        start, end = max(2 * j - 1, 0), min(2 * j, nbx - 1)
        pooled = dot(paired_rows(hid[start], hid[end]), pool[...]) * 0.25
        cz[j, LAYERS : LAYERS + rows_c, :width] = keep_inside(meta, count // 3, pooled.astype(BF), 2)
    edges(cz, 1, nc + 1, rows_c, width, 3 * c1)
    for j in range(nc):
        linear = combine(dot(taps(cz, j + 1, 0, rows_c), wb[...]), wide)
        logistic = sigmoid(linear)
        gated = (linear * logistic).astype(BF)
        gat[j] = gated
        slope_b[j] = logistic * (1.0 + linear * (1.0 - logistic))


def backward_kernel(paired, count, *refs):
    meta = None
    if not paired:
        meta, refs = refs[0], refs[1:]
    pieces, refs = refs[:count], refs[count:]
    fz, slope, cz, gat, slope_b, wbf, mt, pool, up = refs[:9]
    gz, pk_ref = refs[9:11]
    cot, gb, fold, acc_a, acc_b, packed = refs[11:]
    nbx = fz.shape[0]
    nb = nbx - 4
    nc = gat.shape[0]
    rows = cot.shape[1]
    rows_c = rows // 2
    width = cot.shape[2]
    wide = gat.shape[2]
    c1 = width // PB
    c2 = wide // PB
    cells = pieces[0].shape[1]
    blank_rims(gz)
    blank_rims(gb)
    if paired:
        own, partner, near, far = pieces
        e = lax.axis_index("eta")
        for rim, shard in ((near, e), (far, 1 - e)):
            at = pl.multiple_of(shard * cells, cells)
            cot[1 + e * (nbx - 3), pl.ds(at, cells), :] = rim[2]
            for j in range(partner.shape[0]):
                if rim is near:
                    block = own[j + e * (own.shape[0] // 2 - 1)]
                else:
                    block = partner[j]
                cot[j + 2 - e, pl.ds(at, cells), :] = block
        own, own_at, own_at_c = rows, 0, 0
    else:
        for s in range(count // 3):
            middle, before, after = pieces[3 * s : 3 * s + 3]
            at = pl.multiple_of(meta[s] * cells, cells)
            cot[1, pl.ds(at, cells), :] = before[2]
            cot[nbx - 2, pl.ds(at, cells), :] = after[2]
            for j in range(nb):
                cot[2 + j, pl.ds(at, cells), :] = middle[j]
        own = cells
        own_at = pl.multiple_of(meta[0] * own, own)
        own_at_c = pl.multiple_of(meta[0] * (own // 2), own // 2)
    own_c = own // 2

    for j in range(nc):
        fold[j] = dot(paired_rows(cot[2 * j + 1], cot[2 * j + 2]), pool[...]).astype(BF)
        grad = dot(fold[j], mt[...]) * slope_b[j]
        gb[j, LAYERS : LAYERS + rows_c, :wide] = keep_inside(meta, count // 3, grad.astype(BF), 2)
    edges(gb, 0, nc, rows_c, width, c2)
    for j in range(nc):
        grad = combine(dot(taps(gb, j, 0, rows_c), wbf[...]), width).astype(BF)
        spread = 0.25 * dot(grad, up[...])
        for k in range(2):
            f = 2 * j + 1 + k
            total = cot[f].astype(F32) + widen_rows(spread[:, k * width : (k + 1) * width])
            value = (total * slope[f]).astype(BF)
            gz[f, LAYERS : LAYERS + rows, :width] = keep_inside(meta, count // 3, value, 1)
    edges(gz, 2, nbx - 2, rows, width, 3 * c1)

    def own_half(value, j):
        p = iota(value.shape, 1) // (value.shape[1] // PB)
        if j == 0:
            value = jnp.where(p >= PB // 2, value, jnp.zeros_like(value))
        if j == nc - 1:
            value = jnp.where(p < PB // 2, value, jnp.zeros_like(value))
        return value

    lhs = jnp.concatenate(
        [layer_shifts(gz[2 + j, pl.ds(LAYERS + own_at, own), :width]) for j in range(nb)], axis=0
    )
    rhs = jnp.concatenate([taps(fz, 2 + j, own_at, own) for j in range(nb)], axis=0)
    acc_a[...] = dot_rows(lhs, rhs)
    lhs = jnp.concatenate(
        [layer_shifts(own_half(gb[j, pl.ds(LAYERS + own_at_c, own_c), :wide], j)) for j in range(nc)], axis=0
    )
    rhs = jnp.concatenate([taps(cz, j + 1, own_at_c, own_c) for j in range(nc)], axis=0)
    acc_b[...] = dot_rows(rhs, lhs)
    lhs = jnp.concatenate([gat[j, pl.ds(own_at_c, own_c), :] for j in range(nc)], axis=0)
    rhs = jnp.concatenate([own_half(fold[j, pl.ds(own_at_c, own_c), :], j) for j in range(nc)], axis=0)
    mixed = dot_rows(rhs, lhs)
    mix_sum = mixed[:c1, :c2]
    for p in range(1, PB):
        mix_sum = mix_sum + mixed[p * c1 : (p + 1) * c1, p * c2 : (p + 1) * c2]
    first_b, first_mix = places_of(c1, c2)
    packed[:, first_mix : first_mix + c2] = mix_sum
    packed[:, 27 * c1 : first_b] = jnp.zeros((c1, first_b - 27 * c1), F32)
    span = 2 * width
    for b in range(3):
        for c in range(3):
            total = None
            for p in range(PB):
                at = (c * PB + p) * c1
                part = acc_a[at : at + c1, b * span : (b + 1) * span]
                part = pltpu.roll(part, (span - (p - 1) * c1) % span, 1)
                total = part if total is None else total + part
            for a in range(3):
                t = 9 * a + 3 * b + c
                packed[:, t * c1 : (t + 1) * c1] = total[:, a * c1 : (a + 1) * c1]
    for t in range(27):
        a, b, c = t // 9, t // 3 % 3, t % 3
        sides = [None, None]
        for p in range(PB):
            at = b * span + (p + a - 1) % (2 * PB) * c1
            lanes = c * wide + p // 2 * 2 * c2
            part = acc_b[at : at + c1, lanes : lanes + 2 * c2]
            sides[p % 2] = part if sides[p % 2] is None else sides[p % 2] + part
        total = sides[t % 2] + pltpu.roll(sides[1 - t % 2], c2, 1)
        lanes = first_b + t * c2
        packed[:, lanes : lanes + c2] = total[:, t % 2 * c2 : (t % 2 + 1) * c2]
    step = pk_ref.shape[1] // 8
    pieces8 = packed.shape[0] // 8
    used = packed.shape[1] // 128 * pieces8
    for n in range(pk_ref.shape[0] * step):
        at = slice(n % step * 8, n % step * 8 + 8)
        if n < used:
            v, k = n // pieces8, n % pieces8
            pk_ref[n // step, at] = packed[8 * k : 8 * k + 8, v * 128 : (v + 1) * 128].astype(BF)
        else:
            pk_ref[n // step, at] = jnp.zeros((8, 128), BF)


def places_of(c1, c2):
    first_b = -(-27 * c1 // 128) * 128
    return first_b, first_b + 27 * c2


def finish_kernel(paired, *refs):
    meta = None
    if not paired:
        meta, refs = refs[0], refs[1:]
    gz, hid, gat, waf, mp, up = refs[:6]
    outs = refs[6:-1]
    buf = refs[-1]
    nb = gz.shape[0] - 4
    width = hid.shape[2]
    cells = outs[0].shape[2]
    if paired:
        own, own_at, own_at_c = hid.shape[1], 0, 0
        e = lax.axis_index("eta")
        starts = [pl.multiple_of(e * cells, cells), pl.multiple_of((1 - e) * cells, cells)]
    else:
        own = cells
        own_at = pl.multiple_of(meta[0] * own, own)
        own_at_c = pl.multiple_of(meta[0] * (own // 2), own // 2)
        starts = [0]

    def write(value, place):
        buf[place] = value
        for out, start in zip(outs, starts):
            out[place] = buf[place, pl.ds(start, cells), :].T.astype(BF)

    for j in range(nb):
        grad = combine(dot(taps(gz, 2 + j, own_at, own), waf[...]), width)
        write(grad, nb + j)
    for j in range(nb):
        k = (j + 1) % 2
        projected = dot(gat[(j + 1) // 2, pl.ds(own_at_c, own // 2), :], mp[...]).astype(BF)
        spread = dot(projected, up[:, k * width : (k + 1) * width])
        write(hid[2 + j, pl.ds(own_at, own), :].astype(F32) + widen_rows(spread), j)


def restore_kernel(kept, received, out_ref, gin_ref):
    ch, rows, cells = out_ref.shape
    half = rows // 2
    e = lax.axis_index("eta")
    for k, ref in enumerate((out_ref, gin_ref)):
        at = k * half // PB
        mine = kept[at : at + half // PB].astype(F32)
        other = received[at : at + half // PB].astype(F32)
        first = jnp.where(e == 0, mine, other).reshape(half, ch, cells)
        second = jnp.where(e == 0, other, mine).reshape(half, ch, cells)
        ref[...] = jnp.swapaxes(jnp.concatenate([first, second], axis=0), 0, 1).astype(BF)


def sum_kernel(x_ref, o_ref):
    total = jnp.sum(x_ref[...].astype(F32), axis=0).astype(BF)
    o_ref[...] = jnp.broadcast_to(total[None], o_ref.shape)


def post_kernel(factor, x_ref, ga_ref, gb_ref, gm_ref, buf):
    step = x_ref.shape[1] // 8
    pieces8 = buf.shape[0] // 8
    c1, c2 = gm_ref.shape
    for n in range(buf.shape[1] // 128 * pieces8):
        v, k = n // pieces8, n % pieces8
        part = x_ref[n // step, n % step * 8 : n % step * 8 + 8]
        buf[8 * k : 8 * k + 8, v * 128 : (v + 1) * 128] = part.astype(F32) * factor
    first_b, first_mix = places_of(c1, c2)
    for t in range(27):
        ga_ref[t] = buf[:, t * c1 : (t + 1) * c1]
        gb_ref[t] = buf[:, first_b + t * c2 : first_b + (t + 1) * c2]
    gm_ref[...] = buf[:, first_mix : first_mix + c2]


def call(kernel, outs, *args, scratch=(), smem=0, near=(), far=(), aliases={}):
    args = list(args)
    specs = []
    for place in range(len(args)):
        if place < smem:
            specs.append(pl.BlockSpec(memory_space=pltpu.SMEM))
        elif place in far:
            specs.append(pl.BlockSpec(memory_space=pl.ANY))
            args[place] = pltpu.with_memory_space_constraint(args[place], pltpu.HBM)
        else:
            specs.append(pl.BlockSpec(memory_space=pltpu.VMEM))
            if place in near:
                args[place] = pltpu.with_memory_space_constraint(args[place], pltpu.VMEM)
    return pl.pallas_call(
        kernel,
        out_shape=outs,
        in_specs=specs,
        out_specs=tuple(pl.BlockSpec(memory_space=pltpu.VMEM) for _ in outs),
        scratch_shapes=list(scratch),
        input_output_aliases=aliases,
        compiler_params=pltpu.CompilerParams(vmem_limit_bytes=32 * 1024 * 1024),
    )(*args)


def shape(dims, dtype=BF):
    return jax.ShapeDtypeStruct(tuple(dims), dtype)


AXES = ("phi", "eta")


def moves(n_phi, n_eta, rule):
    found = []
    for p in range(n_phi):
        for s in range(n_eta):
            step, t = rule(p, s)
            if 0 <= t < n_eta:
                found.append((p * n_eta + s, (p + step) % n_phi * n_eta + t))
    return found


def gather_pair(f_own, c_own, c_sent, near, far):
    n_phi = lax.axis_size("phi")

    def send(value, rule):
        return lax.ppermute(value, AXES, moves(n_phi, 2, rule))

    far = send(far, lambda p, s: (2 * s - 1, 1 - s))
    near = send(near, lambda p, s: (1 - 2 * s, s))
    f_other = send(f_own, lambda p, s: (0, 1 - s))
    c_other = send(c_sent, lambda p, s: (0, 1 - s))
    return [f_own, f_other, near, far], [c_own, c_other, near, far]


def gather_window(f_own, c_own, low, high):
    n_phi = lax.axis_size("phi")
    n_eta = lax.axis_size("eta")
    f_pieces = []
    c_pieces = []
    for step in window_steps(n_eta):
        send = lambda value, move: lax.ppermute(value, AXES, moves(n_phi, n_eta, lambda p, s: (move, s - step)))
        rims = [send(high, 1), send(low, -1)]
        f_pieces += [f_own if step == 0 else send(f_own, 0)] + rims
        c_pieces += [c_own if step == 0 else send(c_own, 0)] + rims
    return f_pieces, c_pieces


def window_steps(n_eta):
    return [0] if n_eta == 1 else [0, -1, 1, -2, 2]


def window_meta(n_eta, cells):
    e = lax.axis_index("eta")
    steps = window_steps(n_eta)
    middle = len(steps) // 2
    values = [middle + step for step in steps]
    values += [jnp.maximum(0, middle - e) * cells, jnp.minimum(len(steps), n_eta + middle - e) * cells]
    return jnp.stack([jnp.asarray(v, jnp.int32) for v in values])


def shards(features, cotangent, kernel_a, kernel_b, mixing):
    c1, n_rows, cells = features.shape
    c2 = kernel_b.shape[1]
    nb = n_rows // PB
    width = PB * c1
    n_eta = lax.axis_size("eta")
    paired = n_eta == 2 and nb % 4 == 0
    block = (cells, width)
    f_own, c_own, first, second, *c_sent = call(
        functools.partial(pre_kernel, paired),
        tuple(pltpu.VMEM((n,) + block, BF) for n in (nb, nb, 3, 3) + ((nb // 2 + 1,) if paired else ())),
        features,
        cotangent,
        scratch=(
            pltpu.VMEM(features.shape, BF),
            pltpu.VMEM(features.shape, BF),
            pltpu.SemaphoreType.DMA((2,)),
        ),
        far=(0, 1),
    )
    if paired:
        f_pieces, c_pieces = gather_pair(f_own, c_own, c_sent[0], first, second)
        meta = []
        nbx = nb // 2 + 4
        rows = 2 * cells
    else:
        f_pieces, c_pieces = gather_window(f_own, c_own, first, second)
        meta = [window_meta(n_eta, cells)]
        nbx = nb + 4
        rows = len(window_steps(n_eta)) * cells
    wa, waf, wb, wbf, mp, mt, pool, up = call(
        weights_kernel,
        (
            pltpu.VMEM((3 * 2 * width, 3 * width), BF),
            pltpu.VMEM((3 * 2 * width, 3 * width), BF),
            pltpu.VMEM((3 * 2 * width, 3 * PB * c2), BF),
            pltpu.VMEM((3 * 6 * c2, 3 * width), BF),
            pltpu.VMEM((PB * c2, width), BF),
            pltpu.VMEM((width, PB * c2), BF),
            pltpu.VMEM((4 * width, width), BF),
            pltpu.VMEM((width, 2 * width), BF),
        ),
        kernel_a,
        jnp.swapaxes(kernel_b, 1, 2),
        mixing,
        scratch=(
            pltpu.VMEM((27 * c1, width), F32),
            pltpu.VMEM((27 * c1, width), F32),
            pltpu.VMEM((27 * c1, PB * c2), F32),
            pltpu.VMEM((27 * c2, width), F32),
            pltpu.VMEM(kernel_a.shape, BF),
            pltpu.VMEM((27, c1, c2), BF),
            pltpu.VMEM(mixing.shape, BF),
            pltpu.SemaphoreType.DMA((3,)),
        ),
        far=(0, 1, 2),
    )
    nc = nbx // 2 - 1
    rows_c = rows // 2
    devices = lax.axis_size("phi") * n_eta
    lanes = places_of(c1, c2)[1] + c2
    chunk = 8 * -(-c1 * lanes // (8 * 128 * devices))
    tall = rows + 2 * LAYERS
    tall_c = rows_c + 2 * LAYERS
    skip = len(meta)
    count = len(f_pieces)
    matrices = (wa, wb, pool)
    fine = (
        pltpu.VMEM((nbx, tall, 2 * width), BF),
        pltpu.VMEM((nbx, rows, width), BF),
        pltpu.VMEM((nbx, rows, width), F32),
    )
    pooled = (
        pltpu.VMEM((nc + 2, tall_c, 2 * width), BF),
        pltpu.VMEM((nc, rows_c, PB * c2), BF),
        pltpu.VMEM((nc, rows_c, PB * c2), F32),
    )
    between = lambda n: (pltpu.VMEM((n, tall, 2 * width), BF),)
    if paired:
        started = call(chunk_kernel, fine, *f_pieces[:2], wa, scratch=between(nbx - 3), near=range(3))
        args = (*f_pieces[2:], *started, *matrices)
        extra = {"near": range(len(args)), "aliases": {2: 0, 3: 1, 4: 2}}
    else:
        args = (*meta, *f_pieces, *matrices)
        extra = {"near": range(skip + 1, len(args)), "smem": skip}
    fz, hid, slope, cz, gat, slope_b = call(
        functools.partial(forward_kernel, paired, 2 if paired else count),
        fine + pooled,
        *args,
        scratch=between(2 if paired else nbx - 1),
        **extra,
    )
    inner = (fz, slope, cz, gat, slope_b, wbf, mt, pool, up)
    gz, terms = call(
        functools.partial(backward_kernel, paired, count),
        (pltpu.VMEM((nbx, tall, 2 * width), BF), pltpu.VMEM((devices, chunk, 128), BF)),
        *meta,
        *c_pieces,
        *inner,
        scratch=(
            pltpu.VMEM((nbx, rows, width), BF),
            pltpu.VMEM((nc, tall_c, PB * c2 + width), BF),
            pltpu.VMEM((nc, rows_c, width), BF),
            pltpu.VMEM((3 * width, 6 * width), F32),
            pltpu.VMEM((3 * PB * c2, 6 * width), F32),
            pltpu.VMEM((c1, lanes), F32),
        ),
        smem=skip,
        near=range(skip + 1, skip + count + len(inner)),
    )
    terms = lax.all_to_all(terms, AXES, 0, 0, tiled=True)
    blocks = 2 * (nbx - 4)
    results = call(
        functools.partial(finish_kernel, paired),
        (pltpu.VMEM((blocks, width, cells), BF),) * (2 if paired else 1),
        *meta,
        gz,
        hid,
        gat,
        waf,
        mp,
        up,
        scratch=(pltpu.VMEM((blocks, rows if paired else cells, width), F32),),
        smem=skip,
        near=range(skip, skip + 6),
    )
    if paired:
        kept, sent = results
        received = lax.ppermute(sent, AXES, moves(lax.axis_size("phi"), 2, lambda p, s: (0, 1 - s)))
        terms, kept = lax.optimization_barrier((terms, kept))
        output, grad_input = call(
            restore_kernel, (shape(features.shape), shape(features.shape)), kept, received, near=(0, 1)
        )
    else:
        output, grad_input = (
            jnp.transpose(part.reshape(n_rows, c1, cells), (1, 0, 2)) for part in (results[0][:nb], results[0][nb:])
        )
    (sums,) = call(sum_kernel, (pltpu.VMEM(terms.shape, BF),), terms, near=(0,))
    sums = lax.all_to_all(sums, AXES, 0, 0, tiled=True)
    cell_count = n_rows * cells * devices
    grad_a, grad_b, grad_mix = call(
        functools.partial(post_kernel, 1.0 / math.sqrt(cell_count)),
        (shape((27, c1, c1), F32), shape((27, c1, c2), F32), shape((c1, c2), F32)),
        sums,
        scratch=(pltpu.VMEM((c1, lanes), F32),),
        near=(0,),
    )
    return output, grad_input, grad_a, jnp.swapaxes(grad_b, 1, 2), grad_mix


def solution(mesh):
    in_specs = (P(None, "phi", "eta"), P(None, "phi", "eta"), P(), P(), P())
    out_specs = (P(None, "phi", "eta"), P(None, "phi", "eta"), P(), P(), P())

    return jax.shard_map(shards, mesh=mesh, in_specs=in_specs, out_specs=out_specs, check_vma=False)
```
